32 devices in a mesh: rep: 4 (over y, x), shard: 8 (over z, core).
Axes of the slice: x: 2, y: 2, z: 4, core: 2. Of those that a mesh axis runs over, the one named last changes fastest.
Arguments:
- tokens: bfloat16 [16384, 768], P(('rep', 'shard')), may hold values from -6 to 6
- joined_weight: bfloat16 [768, 2304], P('shard'), may hold values from -0.21875 to 0.21875
- mixing_weight: bfloat16 [768, 768], P('shard'), may hold values from -1.25 to 1.25
- gate_weight: bfloat16 [768, 3072], P('shard'), may hold values from -0.21875 to 0.21875
- up_weight: bfloat16 [768, 3072], P('shard'), may hold values from -0.21875 to 0.21875
- down_weight: bfloat16 [3072, 768], P('shard'), may hold values from -0.15625 to 0.15625
- inner_gain: bfloat16 [768], P('shard'), may hold values from 0.5 to 1.5
- inner_shift: bfloat16 [768], P('shard'), may hold values from -1.5 to 1.5
- outer_gain: bfloat16 [768], P('shard'), may hold values from 0.5 to 1.5
- outer_shift: bfloat16 [768], P('shard'), may hold values from -1.5 to 1.5
- segments: int32 [32, 512], P(('rep', 'shard')), may hold values from 0 to 3, as said below
- positions: int32 [32, 512], P(('rep', 'shard')), may hold values from 0 to 255, as said below
- cotangent: bfloat16 [16384, 768], P(('rep', 'shard')), may hold values from -6 to 6
Outputs:
- layer_output: bfloat16 [16384, 768], P(('rep', 'shard'))
- input_grad: bfloat16 [16384, 768], P(('rep', 'shard'))
- joined_grad: float32 [768, 2304], P('shard')
- mixing_grad: float32 [768, 768], P('shard')
- gate_grad: float32 [768, 3072], P('shard')
- up_grad: float32 [768, 3072], P('shard')
- down_grad: float32 [3072, 768], P('shard')
- innergain_grad: float32 [768], P('shard')
- innershift_grad: float32 [768], P('shard')
- outergain_grad: float32 [768], P('shard')
- outershift_grad: float32 [768], P('shard')
The draws below stay inside these ranges and needn't reach their ends.
Inputs may be any that keep to these rules, and one draw needn't show every extreme that they name: `segments`: each sequence of 512 tokens packs 4 documents in order: segment numbers never fall along a sequence and each appears; each document holds 32 to 256 tokens, and exactly one holds 256. `positions`: A token's position counts the tokens before it in its own document.
All inputs are finite; a program needn't handle non-finite values.
Results may differ from the reference program's by a relative error of at most 0.02.
Values may be sent and summed in bfloat16 or wider, within the bound.
A program may use at most 128 MiB of HBM per device.

```python
import math
import jax
import jax.numpy as jnp
from jax import lax

D = 768
H = 12
HD = 64
FF = 3072
SEQ = 512
DOCS = 4
SEQS = 32
TOKENS = 16384


def document_layout(key):
    layout_key = jax.random.fold_in(key, 7)
    pick_key, first_key, second_key = jax.random.split(layout_key, 3)
    longest = SEQ - SEQ // 2
    shortest = SEQ // 16
    leftover = SEQ // 2 - 3 * shortest
    long_index = jax.random.randint(pick_key, (SEQS, 1), 0, DOCS).astype(jnp.int32)
    first_cut = jax.random.randint(first_key, (SEQS,), 0, leftover + 1).astype(jnp.int32)
    second_cut = jax.random.randint(second_key, (SEQS,), 0, leftover + 1).astype(jnp.int32)
    lower_cut = jnp.minimum(first_cut, second_cut)
    upper_cut = jnp.maximum(first_cut, second_cut)
    others = jnp.stack([shortest + lower_cut, shortest + upper_cut - lower_cut, shortest + leftover - upper_cut], axis=1)
    slots = jnp.arange(DOCS, dtype=jnp.int32)[None, :]
    earlier = jnp.take_along_axis(others, jnp.broadcast_to(jnp.clip(slots, 0, 2), (SEQS, DOCS)), axis=1)
    following = jnp.take_along_axis(others, jnp.broadcast_to(jnp.clip(slots - 1, 0, 2), (SEQS, DOCS)), axis=1)
    lengths = jnp.where(slots < long_index, earlier, jnp.where(slots == long_index, longest, following)).astype(jnp.int32)
    doc_ends = jnp.cumsum(lengths, axis=1).astype(jnp.int32)
    starts = doc_ends - lengths
    places = jnp.arange(SEQ, dtype=jnp.int32)
    segment_of = jnp.sum((places[None, :, None] >= doc_ends[:, None, :DOCS - 1]).astype(jnp.int32), axis=2).astype(jnp.int32)
    offsets = jnp.take_along_axis(starts, segment_of, axis=1)
    return (segment_of, (places[None, :] - offsets).astype(jnp.int32))


def draw_segments(key, part):
    return document_layout(key)[0]


def draw_positions(key, part):
    return document_layout(key)[1]


def block_levels(key, dims, pieces, low, largest):
    def one(axis_at, shards_of):
        draws = jax.random.uniform(jax.random.fold_in(jax.random.fold_in(key, 6), axis_at), (shards_of,), jnp.float32, low / len(pieces), largest / len(pieces))
        return jnp.repeat(jnp.exp(draws), dims[axis_at] // shards_of).reshape((-1,) + (1,) * (len(dims) - axis_at - 1))

    factor_of = one(*pieces[0])
    for cut in pieces[1:]:
        factor_of = factor_of * one(*cut)
    return factor_of


def scatter_about(stream_key, extent, spread, bound, cuts=(), held_as=jnp.bfloat16):
    factor_of = block_levels(stream_key, extent, cuts, -0.22, 0.18) if cuts else 1.0
    values = jax.random.normal(stream_key, extent, jnp.float32) * spread * factor_of
    return jnp.minimum(jnp.maximum(values, -bound), bound).astype(held_as)


def setup_inputs(seed: int = 0) -> dict:
    streams_of = jax.random.split(jax.random.key(seed), 14)
    return {
        "tokens": scatter_about(streams_of[0], (TOKENS, D), 1.0, 6.0, ((0, 32),)),
        "joined_weight": scatter_about(streams_of[1], (D, 3 * D), D ** -0.5, 0.21875, ((0, 8),)),
        "mixing_weight": scatter_about(streams_of[2], (D, D), (D // 32) ** -0.5, 1.25, ((0, 8),)),
        "gate_weight": scatter_about(streams_of[3], (D, FF), D ** -0.5, 0.21875, ((0, 8),)),
        "up_weight": scatter_about(streams_of[4], (D, FF), D ** -0.5, 0.21875, ((0, 8),)),
        "down_weight": scatter_about(streams_of[5], (FF, D), (FF // 2) ** -0.5, 0.15625, ((0, 8),)),
        "inner_gain": jnp.clip(1.0 + 0.1 * jax.random.normal(streams_of[6], (D,), jnp.float32), 0.5, 1.5).astype(jnp.bfloat16),
        "inner_shift": scatter_about(streams_of[7], (D,), 0.3, 1.5, ((0, 8),)),
        "outer_gain": jnp.clip(1.0 + 0.1 * jax.random.normal(streams_of[8], (D,), jnp.float32), 0.5, 1.5).astype(jnp.bfloat16),
        "outer_shift": scatter_about(streams_of[9], (D,), 0.3, 1.5, ((0, 8),)),
        "segments": draw_segments(jax.random.fold_in(streams_of[13], 71), 0),
        "positions": draw_positions(jax.random.fold_in(streams_of[13], 71), 0),
        "cotangent": scatter_about(streams_of[12], (TOKENS, D), 1.0, 6.0, ((0, 32),)),
    }


@jax.custom_vjp
def low(v):
    return lax.optimization_barrier(v.astype(jnp.bfloat16)).astype(jnp.float32)

@jax.custom_vjp
def low_back(v):
    return v

def low_keep(v):
    return (low(v), None)

def low_pass(kept, grad):
    return (grad,)

def back_keep(v):
    return (v, None)

def back_low(kept, grad):
    return (low(grad),)
low.defvjp(low_keep, low_pass)
low_back.defvjp(back_keep, back_low)
HIGHEST = lax.Precision.HIGHEST
EPSILON = 1e-12
NEG_LARGE = -1e+30

def rotation(positions):
    halves = jnp.arange(HD // 2, dtype=jnp.float32)
    inverse = 1000.0 ** (-(2.0 * halves) / HD)
    angles = positions.astype(jnp.float32)[..., None] * inverse
    angles = jnp.concatenate([angles, angles], axis=-1)
    return (jnp.cos(angles), jnp.sin(angles))

def rotate(values, cosine, sine_table):
    half_size = values.shape[-1] // 2
    turned = jnp.concatenate([-values[..., half_size:], values[..., :half_size]], axis=-1)
    return values * cosine[..., None, :] + turned * sine_table[..., None, :]

def layer_norm(values, gain, shift):
    centred = values - lax.optimization_barrier(jnp.mean(values, axis=-1, keepdims=True))
    variance = lax.optimization_barrier(jnp.mean(centred * centred, axis=-1, keepdims=True))
    return centred * lax.rsqrt(variance + EPSILON) * gain + shift

def project(left, right):
    return jnp.einsum('gsd,de->gse', left, right, precision=HIGHEST, preferred_element_type=jnp.float32)

def forward(tokens, joined_weight, mixing_weight, gate_weight, up_weight, down_weight, inner_gain, inner_shift, outer_gain, outer_shift, segments, positions):
    groups, length, model_width = tokens.shape
    score_scale = 1.0 / math.sqrt(HD)
    joined_rows = low_back(project(tokens, joined_weight))
    head_shape = (groups, length, H, HD)
    cosine, sine_table = rotation(positions)
    queries = low(rotate(joined_rows[..., :model_width].reshape(head_shape), cosine, sine_table))
    key_rows = low(rotate(joined_rows[..., model_width:2 * model_width].reshape(head_shape), cosine, sine_table))
    value_rows = low(joined_rows[..., 2 * model_width:].reshape(head_shape))
    scores = low_back(jnp.einsum('gqhd,gkhd->ghqk', queries, key_rows, precision=HIGHEST) * score_scale)
    same_doc = (segments[:, :, None] == segments[:, None, :])[:, None]
    scores = jnp.where(same_doc, scores, NEG_LARGE)
    probability = jax.nn.softmax(scores, axis=-1)
    attended = jnp.einsum('ghqk,gkhd->gqhd', low(probability), value_rows, precision=HIGHEST)
    attended = low(low_back(attended.reshape(groups, length, model_width)))
    branch = low_back(project(attended, mixing_weight))
    normed = layer_norm(tokens + branch, inner_gain, inner_shift)
    normed_low = low(normed)
    gate_rows = low_back(project(normed_low, gate_weight))
    upward = low_back(project(normed_low, up_weight))
    active = low(jax.nn.silu(gate_rows) * upward)
    result = low_back(project(active, down_weight))
    return layer_norm(normed + result, outer_gain, outer_shift)

def reference(tokens, joined_weight, mixing_weight, gate_weight, up_weight, down_weight, inner_gain, inner_shift, outer_gain, outer_shift, segments, positions, cotangent):
    batch = 4 if SEQS % 4 == 0 else 1
    rounds = SEQS // batch
    params = tuple((tensor.astype(jnp.float32) for tensor in (joined_weight, mixing_weight, gate_weight, up_weight, down_weight, inner_gain, inner_shift, outer_gain, outer_shift)))
    inputs = tokens.astype(jnp.float32).reshape(rounds, batch, SEQ, D)
    seeds = cotangent.astype(jnp.float32).reshape(rounds, batch, SEQ, D)
    segment_blocks = segments.astype(jnp.int32).reshape(rounds, batch, SEQ)
    position_blocks = positions.astype(jnp.int32).reshape(rounds, batch, SEQ)

    def advance(running, item):
        block_tokens, block_seed, block_segments, block_positions = item

        def apply(block_in, *weights):
            return forward(block_in, *weights, block_segments, block_positions)
        outcome, pullback = jax.vjp(apply, block_tokens, *params)
        grads = pullback(block_seed)
        running = tuple((total + update for total, update in zip(running, grads[1:])))
        return (running, (outcome.astype(jnp.bfloat16), grads[0].astype(jnp.bfloat16)))
    zeros = tuple((jnp.zeros_like(tensor) for tensor in params))
    running, (outputs, input_grads) = lax.scan(advance, zeros, (inputs, seeds, segment_blocks, position_blocks))
    return (outputs.reshape(TOKENS, D), input_grads.reshape(TOKENS, D), running[0], running[1], running[2], running[3], running[4], running[5], running[6], running[7], running[8])
```

```python
import functools
import math

import jax
import jax.numpy as jnp
from jax import lax
from jax.experimental import pallas as pl
from jax.experimental.pallas import tpu as pltpu
from jax.sharding import PartitionSpec as P

H = 12
HD = 64

EPSILON = 1e-12
NEG_LARGE = -1e30
LANES = 128
MESH = pl.DeviceIdType.MESH
VMEM_LIMIT = 62 * 1024 * 1024


class Plan:
    def __init__(self, width, replicas, shards):
        self.replicas, self.shards = replicas, shards
        self.chips = shards // 2
        self.levels = replicas.bit_length() - 1
        self.orders = 2 if self.levels > 1 and width % (2 * replicas * LANES) == 0 else 1
        self.ways = (tuple(range(self.levels)), tuple(reversed(range(self.levels))))[: self.orders]
        self.piece = width // (replicas * self.orders)
        self.width = width

    def flip(self, rep, bit):
        return rep + (1 << bit) * (1 - 2 * lax.rem(lax.div(rep, 1 << bit), 2))

    def with_bits(self, rep, bits, number):
        for at, bit in enumerate(bits):
            had = lax.rem(lax.div(rep, 1 << bit), 2)
            rep = rep + (1 << bit) * (((number >> at) & 1) - had)
        return rep

    def column(self, rep, order):
        return pl.multiple_of((rep * self.orders + order) * self.piece, LANES)

    def grow(self, rep, order, step):
        bits = self.ways[order][:step]
        return [self.with_bits(rep, bits, number) for number in range(1 << step)]

    def grow_at(self, step):
        return (1 << step) - 1

    def halve(self, rep, order, step):
        bits = self.ways[order][step + 1 :]
        return [self.with_bits(rep, bits, number) for number in range(1 << len(bits))]

    def halve_at(self, step):
        return sum(1 << (self.levels - 1 - at) for at in range(step))


def peer(rep, shard):
    return {"rep": rep, "shard": shard}


def remote(src, dst, send, recv, rep, shard):
    return pltpu.make_async_remote_copy(
        src_ref=src,
        dst_ref=dst,
        send_sem=send,
        recv_sem=recv,
        device_id=peer(rep, shard),
        device_id_type=MESH,
    )


def greet_all(plan, rep, shard):
    barrier = pltpu.get_barrier_semaphore()
    total = plan.replicas * plan.shards

    def hello(step, carry):
        other = lax.rem(rep * plan.shards + shard + step, total)
        pl.semaphore_signal(
            barrier,
            inc=1,
            device_id=peer(lax.div(other, plan.shards), lax.rem(other, plan.shards)),
            device_id_type=MESH,
        )
        return carry

    lax.fori_loop(1, total, hello, 0)
    pl.semaphore_wait(barrier, total - 1)


def greet_near(plan, rep, shard):
    barrier = pltpu.get_barrier_semaphore()
    for step in range(1, plan.shards):
        pl.semaphore_signal(
            barrier,
            inc=1,
            device_id=peer(rep, lax.rem(shard + step, plan.shards)),
            device_id_type=MESH,
        )
    for bit in range(plan.levels):
        pl.semaphore_signal(
            barrier, inc=1, device_id=peer(plan.flip(rep, bit), shard), device_id_type=MESH
        )
    pl.semaphore_wait(barrier, plan.shards - 1 + plan.levels)


def gather_kernel(plan, *refs):
    own, small = refs[:4], refs[4]
    full, small_all = refs[5:9], refs[9]
    stages = refs[10:14]
    (load_sem, store_sem, small_send, small_recv, z_send, z_recv, rep_send, rep_recv, core_send,
     core_recv) = refs[14:]
    rep, shard = lax.axis_index("rep"), lax.axis_index("shard")
    chips, piece = plan.chips, plan.piece
    place, core = lax.div(shard, 2), lax.rem(shard, 2)
    mate = place * 2 + (1 - core)
    rows = own[0].shape[0]

    def part(ref, mat, top, section_rep, order):
        if mat < 3:
            return ref.at[
                pl.ds(pl.multiple_of(top, 8), rows),
                pl.ds(plan.column(section_rep, order), piece),
            ]
        per = own[3].shape[1] // piece
        section = section_rep * plan.orders + order
        return ref.at[
            pl.ds(pl.multiple_of(top + lax.div(section, per) * rows, 8), rows),
            pl.ds(pl.multiple_of(lax.rem(section, per) * piece, LANES), piece),
        ]

    def slab_part(mat, slab, section_rep, order):
        return part(full[mat], mat, slab * own[mat].shape[0], section_rep, order)

    def slab_of(mat, slab):
        deep = own[mat].shape[0]
        return full[mat].at[pl.ds(pl.multiple_of(slab * deep, 8), deep), :]

    sent = []

    def launch(copy):
        copy.start()
        sent.append(copy)

    loads = [pltpu.make_async_copy(own[mat], stages[mat], load_sem.at[mat]) for mat in range(4)]
    for load in loads:
        load.start()
    small_all[shard] = small[...]
    greet_near(plan, rep, shard)

    def small_copy(step):
        return remote(
            small, small_all.at[shard], small_send.at[step - 1], small_recv.at[step - 1],
            rep, lax.rem(shard + step, plan.shards),
        )

    for mat in range(4):
        for gap in range(1, chips):
            target = lax.rem(place - gap + chips, chips) * 2 + core
            for order in range(plan.orders):
                launch(remote(
                    part(own[mat], mat, 0, rep, order),
                    slab_part(mat, shard, rep, order),
                    z_send.at[mat, gap - 1, order],
                    z_recv.at[mat, gap - 1, order],
                    rep, target,
                ))
        launch(remote(
            own[mat], slab_of(mat, shard), core_send.at[mat, 0], core_recv.at[mat, 0], rep, mate
        ))
        if mat == 0:
            for step in range(1, plan.shards):
                launch(small_copy(step))

    stores = []
    for mat in range(4):
        loads[mat].wait()
        store = pltpu.make_async_copy(stages[mat], slab_of(mat, shard), store_sem.at[mat])
        store.start()
        stores.append(store)

    def source(gap):
        return lax.rem(place + gap, chips) * 2 + core

    def exchange(mat, gap, order, step):
        slab = source(gap)
        far = plan.flip(rep, plan.ways[order][step])
        at = plan.grow_at(step)
        return [
            remote(
                slab_part(mat, slab, section, order),
                slab_part(mat, slab, section, order),
                rep_send.at[mat, gap - 1, order, at + number],
                rep_recv.at[mat, gap - 1, order, at + number],
                far, shard,
            )
            for number, section in enumerate(plan.grow(rep, order, step))
        ]

    def await_exchange(mat, gap, order, step):
        slab = source(gap)
        far = plan.flip(rep, plan.ways[order][step])
        at = plan.grow_at(step)
        for number, section in enumerate(plan.grow(far, order, step)):
            there = slab_part(mat, slab, section, order)
            remote(
                there, there,
                rep_send.at[mat, gap - 1, order, at + number],
                rep_recv.at[mat, gap - 1, order, at + number],
                far, shard,
            ).wait_recv()

    def relay(mat, gap, step):
        for order in range(plan.orders):
            if step == 0:
                there = slab_part(mat, source(gap), rep, order)
                remote(
                    there, there, z_send.at[mat, gap - 1, order], z_recv.at[mat, gap - 1, order],
                    rep, source(gap),
                ).wait_recv()
            else:
                await_exchange(mat, gap, order, step - 1)
            if step < plan.levels:
                for copy in exchange(mat, gap, order, step):
                    launch(copy)
        if step == plan.levels:
            there = slab_of(mat, source(gap))
            launch(remote(
                there, there, core_send.at[mat, gap], core_recv.at[mat, gap], rep, mate
            ))

    items = [(mat, gap) for mat in range(4) for gap in range(1, chips)]
    for tick in range(len(items) + plan.levels):
        for step in reversed(range(plan.levels + 1)):
            if 0 <= tick - step < len(items):
                relay(*items[tick - step], step)
    for mat in range(4):
        stores[mat].wait()
        for gap in range(chips):
            there = slab_of(mat, lax.rem(place + gap, chips) * 2 + (1 - core))
            remote(
                there, there, core_send.at[mat, gap], core_recv.at[mat, gap], rep, mate
            ).wait_recv()
    for step in range(1, plan.shards):
        small_copy(step).wait_recv()
    for copy in sent:
        copy.wait_send()


def gather_weights(plan, own, small):
    hbm = pl.BlockSpec(memory_space=pl.ANY)
    vmem = pl.BlockSpec(memory_space=pltpu.VMEM)
    dma = pltpu.SemaphoreType.DMA
    shapes = [
        jax.ShapeDtypeStruct((array.shape[0] * plan.shards, array.shape[1]), array.dtype)
        for array in own
    ]
    gaps = plan.chips - 1
    crossing = plan.replicas - 1
    return pl.pallas_call(
        functools.partial(gather_kernel, plan),
        out_shape=shapes + [jax.ShapeDtypeStruct((plan.shards,) + small.shape, small.dtype)],
        in_specs=[hbm] * 4 + [vmem],
        out_specs=[hbm] * 4 + [vmem],
        scratch_shapes=[pltpu.VMEM(array.shape, array.dtype) for array in own]
        + [
            dma((4,)),
            dma((4,)),
            dma((plan.shards - 1,)),
            dma((plan.shards - 1,)),
            dma((4, gaps, plan.orders)),
            dma((4, gaps, plan.orders)),
            dma((4, gaps, plan.orders, crossing)),
            dma((4, gaps, plan.orders, crossing)),
            dma((4, plan.chips)),
            dma((4, plan.chips)),
        ],
        compiler_params=pltpu.CompilerParams(
            collective_id=0, has_side_effects=True, vmem_limit_bytes=VMEM_LIMIT
        ),
        name="gather_weights",
    )(*own, small)


def sum_kernel(plan, order_of, *refs):
    joined, mixing, gate, up, down, small = refs[:6]
    outs, small_out = refs[6:10], refs[10]
    (held, mate_in, rep_in, z_in, final, small_in, load_sem, out_sem, small_sem, mate_send,
     mate_recv, rep_send, rep_recv, z_send, z_recv, last_send, last_recv) = refs[11:]
    rep, shard = lax.axis_index("rep"), lax.axis_index("shard")
    chips, piece = plan.chips, plan.piece
    place, core = lax.div(shard, 2), lax.rem(shard, 2)
    mate = place * 2 + (1 - core)
    rows = held.shape[2]
    total = plan.replicas * plan.shards
    sent = []

    def launch(copy):
        copy.start()
        sent.append(copy)

    def fragments(mat, slab):
        top = pl.multiple_of(slab * rows, 8)
        if mat == 0:
            wide = joined.shape[1]
            return [
                (joined.at[pl.ds(top, rows), :], 0, wide),
                (mixing.at[pl.ds(top, rows), :], wide, mixing.shape[1]),
            ]
        if mat < 3:
            return [((gate, up)[mat - 1].at[pl.ds(top, rows), :], 0, plan.width)]
        wide = down.shape[1]
        return [
            (
                down.at[
                    pl.ds(pl.multiple_of(slab * (rows * (plan.width // wide)) + at * rows, 8), rows),
                    :,
                ],
                at * wide,
                wide,
            )
            for at in range(plan.width // wide)
        ]

    items = [(mat, gap) for mat in order_of for gap in list(range(1, chips)) + [0]]

    def slab_at(gap, which):
        return lax.rem(place + gap, chips) * 2 + which

    for mat, gap in items:
        for ref, left, wide in fragments(mat, slab_at(gap, core)):
            pltpu.make_async_copy(
                ref, held.at[mat, gap, :, pl.ds(left, wide)], load_sem.at[mat, gap]
            ).start()

    greet_all(plan, rep, shard)

    for mat, gap in items:
        for ref, left, wide in fragments(mat, slab_at(gap, 1 - core)):
            remote(
                ref, mate_in.at[mat, gap, :, pl.ds(left, wide)],
                mate_send.at[mat, gap], mate_recv.at[mat, gap], rep, mate,
            ).start()

    def small_go(step, carry):
        other = lax.rem(rep * plan.shards + shard + step, total)
        other_rep, other_shard = lax.div(other, plan.shards), lax.rem(other, plan.shards)
        remote(
            small.at[other_shard], small_in.at[step - 1], small_sem.at[0], small_sem.at[1],
            other_rep, other_shard,
        ).start()
        return carry

    lax.fori_loop(1, total, small_go, 0)

    def whole_mate(mat, gap):
        return remote(
            mate_in.at[mat, gap], mate_in.at[mat, gap],
            mate_send.at[mat, gap], mate_recv.at[mat, gap], rep, mate,
        )

    def cross(mat, gap, order, step):
        far = plan.flip(rep, plan.ways[order][step])
        at = plan.halve_at(step)
        copies = [
            remote(
                held.at[mat, gap, :, pl.ds(plan.column(section, order), piece)],
                rep_in.at[mat, gap, order, at + number],
                rep_send.at[mat, gap, order, at + number],
                rep_recv.at[mat, gap, order, at + number],
                far, shard,
            )
            for number, section in enumerate(plan.halve(far, order, step))
        ]
        return copies, [plan.column(section, order) for section in plan.halve(rep, order, step)]

    def last_piece(ref_at, order=None):
        wide = plan.orders * piece
        return ref_at, pl.ds(pl.multiple_of(rep * wide, LANES), wide)

    def z_copy(mat, gap):
        wide = plan.orders * piece
        return remote(
            held.at[mat, gap, :, pl.ds(pl.multiple_of(rep * wide, LANES), wide)],
            z_in.at[mat, gap - 1],
            z_send.at[mat, gap - 1], z_recv.at[mat, gap - 1],
            rep, slab_at(gap, core),
        )

    def advance(mat, gap, step):
        if step == 0:
            pltpu.make_async_copy(
                held.at[mat, gap], held.at[mat, gap], load_sem.at[mat, gap]
            ).wait()
            whole_mate(mat, gap).wait_recv()

            def add(at, carry):
                span = pl.ds(pl.multiple_of(at * piece, LANES), piece)
                held[mat, gap, :, span] = (
                    held[mat, gap, :, span].astype(jnp.float32)
                    + mate_in[mat, gap, :, span].astype(jnp.float32)
                ).astype(jnp.bfloat16)
                return carry

            lax.fori_loop(0, plan.width // piece, add, 0)
        else:
            for order in range(plan.orders):
                copies, columns = cross(mat, gap, order, step - 1)
                at = plan.halve_at(step - 1)
                for number, (copy, column) in enumerate(zip(copies, columns)):
                    copy.wait_recv()
                    span = pl.ds(column, piece)
                    held[mat, gap, :, span] = (
                        held[mat, gap, :, span].astype(jnp.float32)
                        + rep_in[mat, gap, order, at + number].astype(jnp.float32)
                    ).astype(jnp.bfloat16)
        if step < plan.levels:
            for order in range(plan.orders):
                for copy in cross(mat, gap, order, step)[0]:
                    launch(copy)
        elif gap > 0:
            launch(z_copy(mat, gap))

    def spread(mat, order, step):
        far = plan.flip(rep, plan.ways[order][step])
        at = plan.grow_at(step)
        return [
            remote(
                final.at[mat, :, pl.ds(plan.column(section, order), piece)],
                final.at[mat, :, pl.ds(plan.column(section, order), piece)],
                last_send.at[mat, order, at + number],
                last_recv.at[mat, order, at + number],
                far, shard,
            )
            for number, section in enumerate(plan.grow(rep, order, step))
        ]

    def await_spread(mat, order, step):
        far = plan.flip(rep, plan.ways[order][step])
        at = plan.grow_at(step)
        for number, section in enumerate(plan.grow(far, order, step)):
            there = final.at[mat, :, pl.ds(plan.column(section, order), piece)]
            remote(
                there, there,
                last_send.at[mat, order, at + number],
                last_recv.at[mat, order, at + number],
                far, shard,
            ).wait_recv()

    def finish(mat, step):
        if step == 0:
            for gap in range(1, chips):
                z_copy(mat, gap).wait_recv()
            for order in range(plan.orders):
                span = pl.ds(plan.column(rep, order), piece)
                here = pl.ds(order * piece, piece)
                value = held[mat, 0, :, span].astype(jnp.float32)
                for gap in range(1, chips):
                    value = value + z_in[mat, gap - 1, :, here].astype(jnp.float32)
                final[mat, :, span] = value.astype(jnp.bfloat16)
        else:
            for order in range(plan.orders):
                await_spread(mat, order, step - 1)
        if step < plan.levels:
            for order in range(plan.orders):
                for copy in spread(mat, order, step):
                    launch(copy)
        else:
            pltpu.make_async_copy(final.at[mat], outs[mat], out_sem.at[mat]).start()

    finals = []
    for tick in range(len(items) + plan.levels):
        for step in reversed(range(plan.levels + 1)):
            if 0 <= tick - step < len(items):
                advance(*items[tick - step], step)
                if step == plan.levels and (tick - step) % chips == chips - 1:
                    finals.append((items[tick - step][0], tick))
        for mat, since in finals:
            if tick > since and tick - since - 1 <= plan.levels:
                finish(mat, tick - since - 1)
    end = len(items) + plan.levels
    for tick in range(end, end + plan.levels + 1):
        for mat, since in finals:
            if tick > since and tick - since - 1 <= plan.levels:
                finish(mat, tick - since - 1)

    everything = remote(small_in, small_in, small_sem.at[0], small_sem.at[1], rep, mate)
    everything.wait_recv()

    def gain(at, value):
        return value + small_in[at]

    small_out[...] = lax.fori_loop(0, total - 1, gain, small[shard])
    everything.wait_send()
    for mat, gap in items:
        whole_mate(mat, gap).wait_send()
    for copy in sent:
        copy.wait_send()
    for mat in order_of:
        pltpu.make_async_copy(final.at[mat], outs[mat], out_sem.at[mat]).wait()


def sum_grads(plan, grads, small):
    hbm = pl.BlockSpec(memory_space=pl.ANY)
    vmem = pl.BlockSpec(memory_space=pltpu.VMEM)
    dma = pltpu.SemaphoreType.DMA
    chips, gaps, crossing = plan.chips, plan.chips - 1, plan.replicas - 1
    rows = grads[0].shape[0] // plan.shards
    low = jnp.bfloat16
    total = plan.replicas * plan.shards
    return pl.pallas_call(
        functools.partial(sum_kernel, plan, (3, 1, 2, 0)),
        out_shape=[jax.ShapeDtypeStruct((rows, plan.width), low)] * 4
        + [jax.ShapeDtypeStruct(small.shape[1:], small.dtype)],
        in_specs=[hbm] * 5 + [vmem],
        out_specs=[hbm] * 4 + [vmem],
        scratch_shapes=[
            pltpu.VMEM((4, chips, rows, plan.width), low),
            pltpu.VMEM((4, chips, rows, plan.width), low),
            pltpu.VMEM((4, chips, plan.orders, crossing, rows, plan.piece), low),
            pltpu.VMEM((4, gaps, rows, plan.orders * plan.piece), low),
            pltpu.VMEM((4, rows, plan.width), low),
            pltpu.VMEM((total - 1,) + small.shape[1:], small.dtype),
            dma((4, chips)),
            dma((4,)),
            dma((2,)),
            dma((4, chips)),
            dma((4, chips)),
            dma((4, chips, plan.orders, crossing)),
            dma((4, chips, plan.orders, crossing)),
            dma((4, gaps)),
            dma((4, gaps)),
            dma((4, plan.orders, crossing)),
            dma((4, plan.orders, crossing)),
        ],
        compiler_params=pltpu.CompilerParams(
            collective_id=1, has_side_effects=True, vmem_limit_bytes=VMEM_LIMIT
        ),
        name="sum_grads",
    )(*grads, small)


def rotation(positions):
    halves = jnp.arange(HD // 2, dtype=jnp.float32)
    inverse = 1000.0 ** (-(2.0 * halves) / HD)
    angles = positions.astype(jnp.float32)[..., None] * inverse
    angles = jnp.concatenate([angles, angles], axis=-1)
    return (jnp.cos(angles), jnp.sin(angles))


def rotate(values, cosine, sine_table):
    half_size = values.shape[-1] // 2
    turned = jnp.concatenate([-values[..., half_size:], values[..., :half_size]], axis=-1)
    return values * cosine[..., None, :] + turned * sine_table[..., None, :]


def layer_norm(values, gain, shift):
    centred = values - jnp.mean(values, axis=-1, keepdims=True)
    variance = jnp.mean(centred * centred, axis=-1, keepdims=True)
    return centred * lax.rsqrt(variance + EPSILON) * gain + shift


def transposed_product(left, right):
    return lax.dot_general(
        left, right, (((1,), (1,)), ((), ())), preferred_element_type=jnp.float32
    )


def token_contract(left, right):
    return lax.dot_general(
        left, right, (((0,), (0,)), ((), ())), preferred_element_type=jnp.float32
    )


def to_heads(values, group_size):
    length = values.shape[0]
    per_head = values.reshape(length, H, HD).transpose(1, 0, 2)
    return per_head.reshape(H // group_size, group_size, length, HD)


def from_heads(values):
    length = values.shape[2]
    merged = values.reshape(H, length, HD).transpose(1, 0, 2)
    return merged.reshape(length, H * HD)


def on_device(
    tokens,
    joined_weight,
    mixing_weight,
    gate_weight,
    up_weight,
    down_weight,
    inner_gain,
    inner_shift,
    outer_gain,
    outer_shift,
    segments,
    positions,
    cotangent,
):
    replicas, shards = lax.axis_size("rep"), lax.axis_size("shard")
    plan = Plan(gate_weight.shape[1], replicas, shards)
    part_rows = joined_weight.shape[0]
    own_vectors = jnp.stack([inner_gain, inner_shift, outer_gain, outer_shift]).astype(jnp.float32)
    own_vectors = jnp.pad(own_vectors, ((0, 4), (0, LANES - part_rows)))
    attention_full, gate_full, upward_full, down_full, vectors = gather_weights(
        plan,
        (
            jnp.concatenate([joined_weight, mixing_weight], axis=1),
            gate_weight,
            up_weight,
            down_weight,
        ),
        own_vectors,
    )
    joined_full = attention_full[:, : joined_weight.shape[1]]
    mixing_full = attention_full[:, joined_weight.shape[1] :]
    vectors = vectors[:, :4, :part_rows].transpose(1, 0, 2).reshape(4, shards * part_rows)
    innergain_full, innershift_full, outergain_full, outershift_full = vectors
    length = tokens.shape[0]
    model_width = tokens.shape[1]
    group_size = 4
    score_scale = 1.0 / math.sqrt(HD)
    same_doc = segments[0][:, None] == segments[0][None, :]
    cosine, sine_table = rotation(positions[0])
    joined_rows = jnp.dot(tokens, joined_full, preferred_element_type=jnp.float32)
    pre_query = joined_rows[:, :model_width].reshape(length, H, HD)
    pre_key = joined_rows[:, model_width : 2 * model_width].reshape(length, H, HD)
    rotated_pair, rotate_pull = jax.vjp(
        lambda first, second: (
            rotate(first, cosine, sine_table),
            rotate(second, cosine, sine_table),
        ),
        pre_query,
        pre_key,
    )
    query_heads = to_heads(
        rotated_pair[0].astype(jnp.bfloat16).reshape(length, model_width), group_size
    )
    key_heads = to_heads(
        rotated_pair[1].astype(jnp.bfloat16).reshape(length, model_width), group_size
    )
    value_heads = to_heads(joined_rows[:, 2 * model_width :].astype(jnp.bfloat16), group_size)

    def head_scores(query_block, key_block):
        scores = (
            jnp.einsum("hqd,hkd->hqk", query_block, key_block, preferred_element_type=jnp.float32)
            * score_scale
        )
        return jnp.where(same_doc, scores, NEG_LARGE)

    def head_forward(block):
        query_block, key_block, value_block = block
        scores = head_scores(query_block, key_block)
        highest = jnp.max(scores, axis=-1, keepdims=True)
        shifted = jnp.exp(scores - highest)
        denominator = jnp.sum(shifted, axis=-1, keepdims=True)
        probs_low = (shifted / denominator).astype(jnp.bfloat16)
        attended = jnp.einsum(
            "hqk,hkd->hqd", probs_low, value_block, preferred_element_type=jnp.float32
        )
        return (attended.astype(jnp.bfloat16), highest + jnp.log(denominator))

    attended_heads, logsum = lax.map(head_forward, (query_heads, key_heads, value_heads))
    attended_low = from_heads(attended_heads)
    branch = jnp.dot(attended_low, mixing_full, preferred_element_type=jnp.float32)
    inner_resid = tokens.astype(jnp.float32) + branch
    normed, inner_pull = jax.vjp(
        layer_norm,
        inner_resid,
        innergain_full.astype(jnp.float32),
        innershift_full.astype(jnp.float32),
    )
    normed_low = normed.astype(jnp.bfloat16)
    gate_rows = jnp.dot(normed_low, gate_full, preferred_element_type=jnp.float32)
    upward = jnp.dot(normed_low, upward_full, preferred_element_type=jnp.float32)
    active, silu_pull = jax.vjp(
        lambda first, second: jax.nn.silu(first) * second, gate_rows, upward
    )
    active_low = active.astype(jnp.bfloat16)
    result = jnp.dot(active_low, down_full, preferred_element_type=jnp.float32)
    final, outer_pull = jax.vjp(
        layer_norm,
        normed + result,
        outergain_full.astype(jnp.float32),
        outershift_full.astype(jnp.float32),
    )
    layer_output = final.astype(jnp.bfloat16)
    gate_back, upward_back, down_back = gate_full, upward_full, down_full
    outer_grad, outergain_grad, outershift_grad = outer_pull(cotangent.astype(jnp.float32))
    result_grad = outer_grad.astype(jnp.bfloat16)
    down_grad = token_contract(active_low, result_grad)
    active_grad = transposed_product(result_grad, down_back)
    gate_part, upward_part = silu_pull(active_grad)
    gate_low = gate_part.astype(jnp.bfloat16)
    upward_low = upward_part.astype(jnp.bfloat16)
    gate_grad = token_contract(normed_low, gate_low)
    up_grad = token_contract(normed_low, upward_low)
    normed_grad = (
        outer_grad
        + transposed_product(gate_low, gate_back)
        + transposed_product(upward_low, upward_back)
    )
    inner_grad, innergain_grad, innershift_grad = inner_pull(normed_grad)
    joined_back, mixing_back = joined_full, mixing_full
    branch_grad = inner_grad.astype(jnp.bfloat16)
    mixing_grad = token_contract(attended_low, branch_grad)
    attended_grad = transposed_product(branch_grad, mixing_back).astype(jnp.bfloat16)

    def head_backward(block):
        query_block, key_block, value_block, output_block, logsum_block = block
        probability = jnp.exp(head_scores(query_block, key_block) - logsum_block)
        prob_grad = jnp.einsum(
            "hqd,hkd->hqk", output_block, value_block, preferred_element_type=jnp.float32
        )
        value_grad = jnp.einsum(
            "hqk,hqd->hkd",
            probability.astype(jnp.bfloat16),
            output_block,
            preferred_element_type=jnp.float32,
        )
        row_dot = jnp.sum(probability * prob_grad, axis=-1, keepdims=True)
        score_grad = (probability * (prob_grad - row_dot)).astype(jnp.bfloat16)
        query_grad = (
            jnp.einsum("hqk,hkd->hqd", score_grad, key_block, preferred_element_type=jnp.float32)
            * score_scale
        )
        key_grad = (
            jnp.einsum("hqk,hqd->hkd", score_grad, query_block, preferred_element_type=jnp.float32)
            * score_scale
        )
        return (query_grad, key_grad, value_grad)

    query_grad, key_grad, value_grad = lax.map(
        head_backward,
        (query_heads, key_heads, value_heads, to_heads(attended_grad, group_size), logsum),
    )
    query_raw, key_raw = rotate_pull(
        (from_heads(query_grad).reshape(length, H, HD), from_heads(key_grad).reshape(length, H, HD))
    )
    joined_low = jnp.concatenate(
        [
            query_raw.reshape(length, model_width),
            key_raw.reshape(length, model_width),
            from_heads(value_grad),
        ],
        axis=1,
    ).astype(jnp.bfloat16)
    input_grad = (inner_grad + transposed_product(joined_low, joined_back)).astype(jnp.bfloat16)
    joined_grad = token_contract(tokens, joined_low)
    small = jnp.stack([innergain_grad, innershift_grad, outergain_grad, outershift_grad])
    small = small.reshape(4, shards, part_rows).transpose(1, 0, 2)
    small = jnp.pad(small, ((0, 0), (0, 4), (0, LANES - part_rows)))
    low = jnp.bfloat16
    attention_sum, gate_sum, up_sum, down_sum, small_sum = sum_grads(
        plan,
        (
            joined_grad.astype(low),
            mixing_grad.astype(low),
            gate_grad.astype(low),
            up_grad.astype(low),
            down_grad.astype(low),
        ),
        small,
    )
    down_sum = down_sum.reshape(part_rows, -1, model_width).transpose(1, 0, 2)
    full = jnp.float32
    return (
        layer_output,
        input_grad,
        attention_sum[:, : joined_weight.shape[1]].astype(full),
        attention_sum[:, joined_weight.shape[1] :].astype(full),
        gate_sum.astype(full),
        up_sum.astype(full),
        down_sum.reshape(down_weight.shape).astype(full),
        small_sum[0, :part_rows],
        small_sum[1, :part_rows],
        small_sum[2, :part_rows],
        small_sum[3, :part_rows],
    )


def solution(mesh):
    placed = (
        P(("rep", "shard"), None),
        P("shard", None),
        P("shard", None),
        P("shard", None),
        P("shard", None),
        P("shard", None),
        P("shard"),
        P("shard"),
        P("shard"),
        P("shard"),
        P(("rep", "shard"), None),
        P(("rep", "shard"), None),
        P(("rep", "shard"), None),
    )
    return jax.shard_map(
        on_device,
        mesh=mesh,
        in_specs=placed,
        out_specs=(
            P(("rep", "shard"), None),
            P(("rep", "shard"), None),
            P("shard", None),
            P("shard", None),
            P("shard", None),
            P("shard", None),
            P("shard", None),
            P("shard"),
            P("shard"),
            P("shard"),
            P("shard"),
        ),
        check_vma=False,
    )
```

```python
import functools
import math

import jax
import jax.numpy as jnp
from jax import lax
from jax.experimental import pallas as pl
from jax.experimental.pallas import tpu as pltpu
from jax.sharding import PartitionSpec as P

H = 12
HD = 64

EPSILON = 1e-12
NEG_LARGE = -1e30
LANES = 128
MESH = pl.DeviceIdType.MESH
VMEM_LIMIT = 62 * 1024 * 1024
SLACK = 2
AHEAD = 3


class Plan:
    def __init__(self, width, replicas, shards):
        self.replicas, self.shards = replicas, shards
        self.chips = shards // 2
        self.levels = replicas.bit_length() - 1
        self.orders = 2 if self.levels > 1 and width % (2 * replicas * LANES) == 0 else 1
        self.ways = (tuple(range(self.levels)), tuple(reversed(range(self.levels))))[: self.orders]
        self.piece = width // (replicas * self.orders)
        self.width = width

    def flip(self, rep, bit):
        return rep + (1 << bit) * (1 - 2 * lax.rem(lax.div(rep, 1 << bit), 2))

    def with_bits(self, rep, bits, number):
        for at, bit in enumerate(bits):
            had = lax.rem(lax.div(rep, 1 << bit), 2)
            rep = rep + (1 << bit) * (((number >> at) & 1) - had)
        return rep

    def column(self, rep, order):
        return pl.multiple_of((rep * self.orders + order) * self.piece, LANES)

    def grow(self, rep, order, step):
        bits = self.ways[order][:step]
        return [self.with_bits(rep, bits, number) for number in range(1 << step)]

    def grow_at(self, step):
        return (1 << step) - 1

    def halve(self, rep, order, step):
        bits = self.ways[order][step + 1 :]
        return [self.with_bits(rep, bits, number) for number in range(1 << len(bits))]

    def halve_at(self, step):
        return sum(1 << (self.levels - 1 - at) for at in range(step))


def peer(rep, shard):
    return {"rep": rep, "shard": shard}


def remote(src, dst, send, recv, rep, shard):
    return pltpu.make_async_remote_copy(
        src_ref=src,
        dst_ref=dst,
        send_sem=send,
        recv_sem=recv,
        device_id=peer(rep, shard),
        device_id_type=MESH,
    )


def greet_all(plan, rep, shard):
    barrier = pltpu.get_barrier_semaphore()
    total = plan.replicas * plan.shards

    def hello(step, carry):
        other = lax.rem(rep * plan.shards + shard + step, total)
        pl.semaphore_signal(
            barrier,
            inc=1,
            device_id=peer(lax.div(other, plan.shards), lax.rem(other, plan.shards)),
            device_id_type=MESH,
        )
        return carry

    lax.fori_loop(1, total, hello, 0)
    pl.semaphore_wait(barrier, total - 1)


def greet_near(plan, rep, shard):
    barrier = pltpu.get_barrier_semaphore()
    for step in range(1, plan.shards):
        pl.semaphore_signal(
            barrier,
            inc=1,
            device_id=peer(rep, lax.rem(shard + step, plan.shards)),
            device_id_type=MESH,
        )
    for bit in range(plan.levels):
        pl.semaphore_signal(
            barrier, inc=1, device_id=peer(plan.flip(rep, bit), shard), device_id_type=MESH
        )
    pl.semaphore_wait(barrier, plan.shards - 1 + plan.levels)


def gather_kernel(plan, *refs):
    own, small = refs[:4], refs[4]
    full, small_all = refs[5:9], refs[9]
    stages = refs[10:14]
    (load_sem, store_sem, small_send, small_recv, z_send, z_recv, rep_send, rep_recv, core_send,
     core_recv) = refs[14:]
    rep, shard = lax.axis_index("rep"), lax.axis_index("shard")
    chips, piece = plan.chips, plan.piece
    place, core = lax.div(shard, 2), lax.rem(shard, 2)
    mate = place * 2 + (1 - core)
    rows = own[0].shape[0]

    def part(ref, mat, top, section_rep, order):
        if mat < 3:
            return ref.at[
                pl.ds(pl.multiple_of(top, 8), rows),
                pl.ds(plan.column(section_rep, order), piece),
            ]
        per = own[3].shape[1] // piece
        section = section_rep * plan.orders + order
        return ref.at[
            pl.ds(pl.multiple_of(top + lax.div(section, per) * rows, 8), rows),
            pl.ds(pl.multiple_of(lax.rem(section, per) * piece, LANES), piece),
        ]

    def slab_part(mat, slab, section_rep, order):
        return part(full[mat], mat, slab * own[mat].shape[0], section_rep, order)

    def slab_of(mat, slab):
        deep = own[mat].shape[0]
        return full[mat].at[pl.ds(pl.multiple_of(slab * deep, 8), deep), :]

    sent = []

    def launch(copy):
        copy.start()
        sent.append(copy)

    loads = [pltpu.make_async_copy(own[mat], stages[mat], load_sem.at[mat]) for mat in range(4)]
    for load in loads:
        load.start()
    small_all[shard] = small[...]
    greet_near(plan, rep, shard)

    def small_copy(step):
        return remote(
            small, small_all.at[shard], small_send.at[step - 1], small_recv.at[step - 1],
            rep, lax.rem(shard + step, plan.shards),
        )

    items = [(mat, gap) for mat in range(4) for gap in range(1, chips)]

    def along(mat, gap):
        target = lax.rem(place - gap + chips, chips) * 2 + core
        for order in range(plan.orders):
            launch(remote(
                part(own[mat], mat, 0, rep, order),
                slab_part(mat, shard, rep, order),
                z_send.at[mat, gap - 1, order],
                z_recv.at[mat, gap - 1, order],
                rep, target,
            ))

    for item in items[:AHEAD]:
        along(*item)
    for step in range(1, plan.shards):
        launch(small_copy(step))
    for mat in range(4):
        launch(remote(
            own[mat], slab_of(mat, shard), core_send.at[mat, 0], core_recv.at[mat, 0], rep, mate
        ))

    stores = []
    for mat in range(4):
        loads[mat].wait()
        store = pltpu.make_async_copy(stages[mat], slab_of(mat, shard), store_sem.at[mat])
        store.start()
        stores.append(store)

    def source(gap):
        return lax.rem(place + gap, chips) * 2 + core

    def exchange(mat, gap, order, step):
        slab = source(gap)
        far = plan.flip(rep, plan.ways[order][step])
        at = plan.grow_at(step)
        return [
            remote(
                slab_part(mat, slab, section, order),
                slab_part(mat, slab, section, order),
                rep_send.at[mat, gap - 1, order, at + number],
                rep_recv.at[mat, gap - 1, order, at + number],
                far, shard,
            )
            for number, section in enumerate(plan.grow(rep, order, step))
        ]

    def await_exchange(mat, gap, order, step):
        slab = source(gap)
        far = plan.flip(rep, plan.ways[order][step])
        at = plan.grow_at(step)
        for number, section in enumerate(plan.grow(far, order, step)):
            there = slab_part(mat, slab, section, order)
            remote(
                there, there,
                rep_send.at[mat, gap - 1, order, at + number],
                rep_recv.at[mat, gap - 1, order, at + number],
                far, shard,
            ).wait_recv()

    def relay(mat, gap, step):
        for order in range(plan.orders):
            if step == 0:
                there = slab_part(mat, source(gap), rep, order)
                remote(
                    there, there, z_send.at[mat, gap - 1, order], z_recv.at[mat, gap - 1, order],
                    rep, source(gap),
                ).wait_recv()
            else:
                await_exchange(mat, gap, order, step - 1)
            if step < plan.levels:
                for copy in exchange(mat, gap, order, step):
                    launch(copy)
        if step == plan.levels:
            there = slab_of(mat, source(gap))
            launch(remote(
                there, there, core_send.at[mat, gap], core_recv.at[mat, gap], rep, mate
            ))

    events = [
        (at + SLACK * step, -step, item, step)
        for at, item in enumerate(items)
        for step in range(plan.levels + 1)
    ]
    for at, _, item, step in sorted(events):
        relay(*item, step)
        if step == 0 and at + AHEAD < len(items):
            along(*items[at + AHEAD])
    for mat in range(4):
        stores[mat].wait()
        for gap in range(chips):
            there = slab_of(mat, lax.rem(place + gap, chips) * 2 + (1 - core))
            remote(
                there, there, core_send.at[mat, gap], core_recv.at[mat, gap], rep, mate
            ).wait_recv()
    for step in range(1, plan.shards):
        small_copy(step).wait_recv()
    for copy in sent:
        copy.wait_send()


def gather_weights(plan, own, small):
    hbm = pl.BlockSpec(memory_space=pl.ANY)
    vmem = pl.BlockSpec(memory_space=pltpu.VMEM)
    dma = pltpu.SemaphoreType.DMA
    shapes = [
        jax.ShapeDtypeStruct((array.shape[0] * plan.shards, array.shape[1]), array.dtype)
        for array in own
    ]
    gaps = plan.chips - 1
    crossing = plan.replicas - 1
    return pl.pallas_call(
        functools.partial(gather_kernel, plan),
        out_shape=shapes + [jax.ShapeDtypeStruct((plan.shards,) + small.shape, small.dtype)],
        in_specs=[hbm] * 4 + [vmem],
        out_specs=[hbm] * 4 + [vmem],
        scratch_shapes=[pltpu.VMEM(array.shape, array.dtype) for array in own]
        + [
            dma((4,)),
            dma((4,)),
            dma((plan.shards - 1,)),
            dma((plan.shards - 1,)),
            dma((4, gaps, plan.orders)),
            dma((4, gaps, plan.orders)),
            dma((4, gaps, plan.orders, crossing)),
            dma((4, gaps, plan.orders, crossing)),
            dma((4, plan.chips)),
            dma((4, plan.chips)),
        ],
        compiler_params=pltpu.CompilerParams(
            collective_id=0, has_side_effects=True, vmem_limit_bytes=VMEM_LIMIT
        ),
        name="gather_weights",
    )(*own, small)


def sum_kernel(plan, order_of, *refs):
    joined, mixing, gate, up, down, small = refs[:6]
    outs, small_out = refs[6:10], refs[10]
    (held, mate_in, rep_in, z_in, final, small_in, load_sem, out_sem, small_sem, mate_send,
     mate_recv, rep_send, rep_recv, z_send, z_recv, last_send, last_recv) = refs[11:]
    rep, shard = lax.axis_index("rep"), lax.axis_index("shard")
    chips, piece = plan.chips, plan.piece
    place, core = lax.div(shard, 2), lax.rem(shard, 2)
    mate = place * 2 + (1 - core)
    rows = held.shape[2]
    total = plan.replicas * plan.shards
    sent = []

    def launch(copy):
        copy.start()
        sent.append(copy)

    def fragments(mat, slab):
        top = pl.multiple_of(slab * rows, 8)
        if mat == 0:
            wide = joined.shape[1]
            return [
                (joined.at[pl.ds(top, rows), :], 0, wide),
                (mixing.at[pl.ds(top, rows), :], wide, mixing.shape[1]),
            ]
        if mat < 3:
            return [((gate, up)[mat - 1].at[pl.ds(top, rows), :], 0, plan.width)]
        wide = down.shape[1]
        return [
            (
                down.at[
                    pl.ds(pl.multiple_of(slab * (rows * (plan.width // wide)) + at * rows, 8), rows),
                    :,
                ],
                at * wide,
                wide,
            )
            for at in range(plan.width // wide)
        ]

    items = [(mat, gap) for mat in order_of for gap in list(range(1, chips)) + [0]]

    def slab_at(gap, which):
        return lax.rem(place + gap, chips) * 2 + which

    for mat, gap in items:
        for ref, left, wide in fragments(mat, slab_at(gap, core)):
            pltpu.make_async_copy(
                ref, held.at[mat, gap, :, pl.ds(left, wide)], load_sem.at[mat, gap]
            ).start()

    greet_all(plan, rep, shard)

    for mat, gap in items:
        for ref, left, wide in fragments(mat, slab_at(gap, 1 - core)):
            remote(
                ref, mate_in.at[mat, gap, :, pl.ds(left, wide)],
                mate_send.at[mat, gap], mate_recv.at[mat, gap], rep, mate,
            ).start()

    def small_go(step, carry):
        other = lax.rem(rep * plan.shards + shard + step, total)
        other_rep, other_shard = lax.div(other, plan.shards), lax.rem(other, plan.shards)
        remote(
            small.at[other_shard], small_in.at[step - 1], small_sem.at[0], small_sem.at[1],
            other_rep, other_shard,
        ).start()
        return carry

    lax.fori_loop(1, total, small_go, 0)

    def whole_mate(mat, gap):
        return remote(
            mate_in.at[mat, gap], mate_in.at[mat, gap],
            mate_send.at[mat, gap], mate_recv.at[mat, gap], rep, mate,
        )

    def cross(mat, gap, order, step):
        far = plan.flip(rep, plan.ways[order][step])
        at = plan.halve_at(step)
        copies = [
            remote(
                held.at[mat, gap, :, pl.ds(plan.column(section, order), piece)],
                rep_in.at[mat, gap, order, at + number],
                rep_send.at[mat, gap, order, at + number],
                rep_recv.at[mat, gap, order, at + number],
                far, shard,
            )
            for number, section in enumerate(plan.halve(far, order, step))
        ]
        return copies, [plan.column(section, order) for section in plan.halve(rep, order, step)]

    def last_piece(ref_at, order=None):
        wide = plan.orders * piece
        return ref_at, pl.ds(pl.multiple_of(rep * wide, LANES), wide)

    def z_copy(mat, gap):
        wide = plan.orders * piece
        return remote(
            held.at[mat, gap, :, pl.ds(pl.multiple_of(rep * wide, LANES), wide)],
            z_in.at[mat, gap - 1],
            z_send.at[mat, gap - 1], z_recv.at[mat, gap - 1],
            rep, slab_at(gap, core),
        )

    def advance(mat, gap, step):
        if step == 0:
            pltpu.make_async_copy(
                held.at[mat, gap], held.at[mat, gap], load_sem.at[mat, gap]
            ).wait()
            whole_mate(mat, gap).wait_recv()

            def add(at, carry):
                span = pl.ds(pl.multiple_of(at * piece, LANES), piece)
                held[mat, gap, :, span] = (
                    held[mat, gap, :, span].astype(jnp.float32)
                    + mate_in[mat, gap, :, span].astype(jnp.float32)
                ).astype(jnp.bfloat16)
                return carry

            lax.fori_loop(0, plan.width // piece, add, 0)
        else:
            for order in range(plan.orders):
                copies, columns = cross(mat, gap, order, step - 1)
                at = plan.halve_at(step - 1)
                for number, (copy, column) in enumerate(zip(copies, columns)):
                    copy.wait_recv()
                    span = pl.ds(column, piece)
                    held[mat, gap, :, span] = (
                        held[mat, gap, :, span].astype(jnp.float32)
                        + rep_in[mat, gap, order, at + number].astype(jnp.float32)
                    ).astype(jnp.bfloat16)
        if step < plan.levels:
            for order in range(plan.orders):
                for copy in cross(mat, gap, order, step)[0]:
                    launch(copy)
        elif gap > 0:
            launch(z_copy(mat, gap))

    def spread(mat, order, step):
        far = plan.flip(rep, plan.ways[order][step])
        at = plan.grow_at(step)
        return [
            remote(
                final.at[mat, :, pl.ds(plan.column(section, order), piece)],
                final.at[mat, :, pl.ds(plan.column(section, order), piece)],
                last_send.at[mat, order, at + number],
                last_recv.at[mat, order, at + number],
                far, shard,
            )
            for number, section in enumerate(plan.grow(rep, order, step))
        ]

    def await_spread(mat, order, step):
        far = plan.flip(rep, plan.ways[order][step])
        at = plan.grow_at(step)
        for number, section in enumerate(plan.grow(far, order, step)):
            there = final.at[mat, :, pl.ds(plan.column(section, order), piece)]
            remote(
                there, there,
                last_send.at[mat, order, at + number],
                last_recv.at[mat, order, at + number],
                far, shard,
            ).wait_recv()

    def finish(mat, step):
        if step == 0:
            for gap in range(1, chips):
                z_copy(mat, gap).wait_recv()
            for order in range(plan.orders):
                span = pl.ds(plan.column(rep, order), piece)
                here = pl.ds(order * piece, piece)
                value = held[mat, 0, :, span].astype(jnp.float32)
                for gap in range(1, chips):
                    value = value + z_in[mat, gap - 1, :, here].astype(jnp.float32)
                final[mat, :, span] = value.astype(jnp.bfloat16)
        else:
            for order in range(plan.orders):
                await_spread(mat, order, step - 1)
        if step < plan.levels:
            for order in range(plan.orders):
                for copy in spread(mat, order, step):
                    launch(copy)
        else:
            pltpu.make_async_copy(final.at[mat], outs[mat], out_sem.at[mat]).start()

    events = []
    for at, item in enumerate(items):
        for step in range(plan.levels + 1):
            events.append((at + SLACK * step, -step, item[0], item[1], step))
    for number, mat in enumerate(order_of):
        since = (number + 1) * chips - 1 + SLACK * plan.levels
        for step in range(plan.levels + 1):
            events.append((since + SLACK * (step + 1), -plan.levels - 1 - step, mat, -1, step))
    for _, _, mat, gap, step in sorted(events):
        if gap < 0:
            finish(mat, step)
        else:
            advance(mat, gap, step)

    everything = remote(small_in, small_in, small_sem.at[0], small_sem.at[1], rep, mate)
    everything.wait_recv()

    def gain(at, value):
        return value + small_in[at]

    small_out[...] = lax.fori_loop(0, total - 1, gain, small[shard])
    everything.wait_send()
    for mat, gap in items:
        whole_mate(mat, gap).wait_send()
    for copy in sent:
        copy.wait_send()
    for mat in order_of:
        pltpu.make_async_copy(final.at[mat], outs[mat], out_sem.at[mat]).wait()


def sum_grads(plan, grads, small):
    hbm = pl.BlockSpec(memory_space=pl.ANY)
    vmem = pl.BlockSpec(memory_space=pltpu.VMEM)
    dma = pltpu.SemaphoreType.DMA
    chips, gaps, crossing = plan.chips, plan.chips - 1, plan.replicas - 1
    rows = grads[0].shape[0] // plan.shards
    low = jnp.bfloat16
    total = plan.replicas * plan.shards
    return pl.pallas_call(
        functools.partial(sum_kernel, plan, (3, 1, 2, 0)),
        out_shape=[jax.ShapeDtypeStruct((rows, plan.width), low)] * 4
        + [jax.ShapeDtypeStruct(small.shape[1:], small.dtype)],
        in_specs=[hbm] * 5 + [vmem],
        out_specs=[hbm] * 4 + [vmem],
        scratch_shapes=[
            pltpu.VMEM((4, chips, rows, plan.width), low),
            pltpu.VMEM((4, chips, rows, plan.width), low),
            pltpu.VMEM((4, chips, plan.orders, crossing, rows, plan.piece), low),
            pltpu.VMEM((4, gaps, rows, plan.orders * plan.piece), low),
            pltpu.VMEM((4, rows, plan.width), low),
            pltpu.VMEM((total - 1,) + small.shape[1:], small.dtype),
            dma((4, chips)),
            dma((4,)),
            dma((2,)),
            dma((4, chips)),
            dma((4, chips)),
            dma((4, chips, plan.orders, crossing)),
            dma((4, chips, plan.orders, crossing)),
            dma((4, gaps)),
            dma((4, gaps)),
            dma((4, plan.orders, crossing)),
            dma((4, plan.orders, crossing)),
        ],
        compiler_params=pltpu.CompilerParams(
            collective_id=1, has_side_effects=True, vmem_limit_bytes=VMEM_LIMIT
        ),
        name="sum_grads",
    )(*grads, small)


def rotation(positions):
    halves = jnp.arange(HD // 2, dtype=jnp.float32)
    inverse = 1000.0 ** (-(2.0 * halves) / HD)
    angles = positions.astype(jnp.float32)[..., None] * inverse
    angles = jnp.concatenate([angles, angles], axis=-1)
    return (jnp.cos(angles), jnp.sin(angles))


def rotate(values, cosine, sine_table):
    half_size = values.shape[-1] // 2
    turned = jnp.concatenate([-values[..., half_size:], values[..., :half_size]], axis=-1)
    return values * cosine[..., None, :] + turned * sine_table[..., None, :]


def layer_norm(values, gain, shift):
    centred = values - jnp.mean(values, axis=-1, keepdims=True)
    variance = jnp.mean(centred * centred, axis=-1, keepdims=True)
    return centred * lax.rsqrt(variance + EPSILON) * gain + shift


def transposed_product(left, right):
    return lax.dot_general(
        left, right, (((1,), (1,)), ((), ())), preferred_element_type=jnp.float32
    )


def token_contract(left, right):
    return lax.dot_general(
        left, right, (((0,), (0,)), ((), ())), preferred_element_type=jnp.float32
    )


def to_heads(values, group_size):
    length = values.shape[0]
    per_head = values.reshape(length, H, HD).transpose(1, 0, 2)
    return per_head.reshape(H // group_size, group_size, length, HD)


def from_heads(values):
    length = values.shape[2]
    merged = values.reshape(H, length, HD).transpose(1, 0, 2)
    return merged.reshape(length, H * HD)


def on_device(
    tokens,
    joined_weight,
    mixing_weight,
    gate_weight,
    up_weight,
    down_weight,
    inner_gain,
    inner_shift,
    outer_gain,
    outer_shift,
    segments,
    positions,
    cotangent,
):
    replicas, shards = lax.axis_size("rep"), lax.axis_size("shard")
    plan = Plan(gate_weight.shape[1], replicas, shards)
    part_rows = joined_weight.shape[0]
    own_vectors = jnp.stack([inner_gain, inner_shift, outer_gain, outer_shift]).astype(jnp.float32)
    own_vectors = jnp.pad(own_vectors, ((0, 4), (0, LANES - part_rows)))
    attention_full, gate_full, upward_full, down_full, vectors = gather_weights(
        plan,
        (
            jnp.concatenate([joined_weight, mixing_weight], axis=1),
            gate_weight,
            up_weight,
            down_weight,
        ),
        own_vectors,
    )
    joined_full = attention_full[:, : joined_weight.shape[1]]
    mixing_full = attention_full[:, joined_weight.shape[1] :]
    vectors = vectors[:, :4, :part_rows].transpose(1, 0, 2).reshape(4, shards * part_rows)
    innergain_full, innershift_full, outergain_full, outershift_full = vectors
    length = tokens.shape[0]
    model_width = tokens.shape[1]
    group_size = 4
    score_scale = 1.0 / math.sqrt(HD)
    same_doc = segments[0][:, None] == segments[0][None, :]
    cosine, sine_table = rotation(positions[0])
    joined_rows = jnp.dot(tokens, joined_full, preferred_element_type=jnp.float32)
    pre_query = joined_rows[:, :model_width].reshape(length, H, HD)
    pre_key = joined_rows[:, model_width : 2 * model_width].reshape(length, H, HD)
    rotated_pair, rotate_pull = jax.vjp(
        lambda first, second: (
            rotate(first, cosine, sine_table),
            rotate(second, cosine, sine_table),
        ),
        pre_query,
        pre_key,
    )
    query_heads = to_heads(
        rotated_pair[0].astype(jnp.bfloat16).reshape(length, model_width), group_size
    )
    key_heads = to_heads(
        rotated_pair[1].astype(jnp.bfloat16).reshape(length, model_width), group_size
    )
    value_heads = to_heads(joined_rows[:, 2 * model_width :].astype(jnp.bfloat16), group_size)

    def head_scores(query_block, key_block):
        scores = (
            jnp.einsum("hqd,hkd->hqk", query_block, key_block, preferred_element_type=jnp.float32)
            * score_scale
        )
        return jnp.where(same_doc, scores, NEG_LARGE)

    def head_forward(block):
        query_block, key_block, value_block = block
        scores = head_scores(query_block, key_block)
        highest = jnp.max(scores, axis=-1, keepdims=True)
        shifted = jnp.exp(scores - highest)
        denominator = jnp.sum(shifted, axis=-1, keepdims=True)
        probs_low = (shifted / denominator).astype(jnp.bfloat16)
        attended = jnp.einsum(
            "hqk,hkd->hqd", probs_low, value_block, preferred_element_type=jnp.float32
        )
        return (attended.astype(jnp.bfloat16), highest + jnp.log(denominator))

    attended_heads, logsum = lax.map(head_forward, (query_heads, key_heads, value_heads))
    attended_low = from_heads(attended_heads)
    branch = jnp.dot(attended_low, mixing_full, preferred_element_type=jnp.float32)
    inner_resid = tokens.astype(jnp.float32) + branch
    normed, inner_pull = jax.vjp(
        layer_norm,
        inner_resid,
        innergain_full.astype(jnp.float32),
        innershift_full.astype(jnp.float32),
    )
    normed_low = normed.astype(jnp.bfloat16)
    gate_rows = jnp.dot(normed_low, gate_full, preferred_element_type=jnp.float32)
    upward = jnp.dot(normed_low, upward_full, preferred_element_type=jnp.float32)
    active, silu_pull = jax.vjp(
        lambda first, second: jax.nn.silu(first) * second, gate_rows, upward
    )
    active_low = active.astype(jnp.bfloat16)
    result = jnp.dot(active_low, down_full, preferred_element_type=jnp.float32)
    final, outer_pull = jax.vjp(
        layer_norm,
        normed + result,
        outergain_full.astype(jnp.float32),
        outershift_full.astype(jnp.float32),
    )
    layer_output = final.astype(jnp.bfloat16)
    gate_back, upward_back, down_back = gate_full, upward_full, down_full
    outer_grad, outergain_grad, outershift_grad = outer_pull(cotangent.astype(jnp.float32))
    result_grad = outer_grad.astype(jnp.bfloat16)
    down_grad = token_contract(active_low, result_grad)
    active_grad = transposed_product(result_grad, down_back)
    gate_part, upward_part = silu_pull(active_grad)
    gate_low = gate_part.astype(jnp.bfloat16)
    upward_low = upward_part.astype(jnp.bfloat16)
    gate_grad = token_contract(normed_low, gate_low)
    up_grad = token_contract(normed_low, upward_low)
    normed_grad = (
        outer_grad
        + transposed_product(gate_low, gate_back)
        + transposed_product(upward_low, upward_back)
    )
    inner_grad, innergain_grad, innershift_grad = inner_pull(normed_grad)
    joined_back, mixing_back = joined_full, mixing_full
    branch_grad = inner_grad.astype(jnp.bfloat16)
    mixing_grad = token_contract(attended_low, branch_grad)
    attended_grad = transposed_product(branch_grad, mixing_back).astype(jnp.bfloat16)

    def head_backward(block):
        query_block, key_block, value_block, output_block, logsum_block = block
        probability = jnp.exp(head_scores(query_block, key_block) - logsum_block)
        prob_grad = jnp.einsum(
            "hqd,hkd->hqk", output_block, value_block, preferred_element_type=jnp.float32
        )
        value_grad = jnp.einsum(
            "hqk,hqd->hkd",
            probability.astype(jnp.bfloat16),
            output_block,
            preferred_element_type=jnp.float32,
        )
        row_dot = jnp.sum(probability * prob_grad, axis=-1, keepdims=True)
        score_grad = (probability * (prob_grad - row_dot)).astype(jnp.bfloat16)
        query_grad = (
            jnp.einsum("hqk,hkd->hqd", score_grad, key_block, preferred_element_type=jnp.float32)
            * score_scale
        )
        key_grad = (
            jnp.einsum("hqk,hqd->hkd", score_grad, query_block, preferred_element_type=jnp.float32)
            * score_scale
        )
        return (query_grad, key_grad, value_grad)

    query_grad, key_grad, value_grad = lax.map(
        head_backward,
        (query_heads, key_heads, value_heads, to_heads(attended_grad, group_size), logsum),
    )
    query_raw, key_raw = rotate_pull(
        (from_heads(query_grad).reshape(length, H, HD), from_heads(key_grad).reshape(length, H, HD))
    )
    joined_low = jnp.concatenate(
        [
            query_raw.reshape(length, model_width),
            key_raw.reshape(length, model_width),
            from_heads(value_grad),
        ],
        axis=1,
    ).astype(jnp.bfloat16)
    input_grad = (inner_grad + transposed_product(joined_low, joined_back)).astype(jnp.bfloat16)
    joined_grad = token_contract(tokens, joined_low)
    small = jnp.stack([innergain_grad, innershift_grad, outergain_grad, outershift_grad])
    small = small.reshape(4, shards, part_rows).transpose(1, 0, 2)
    small = jnp.pad(small, ((0, 0), (0, 4), (0, LANES - part_rows)))
    low = jnp.bfloat16
    attention_sum, gate_sum, up_sum, down_sum, small_sum = sum_grads(
        plan,
        (
            joined_grad.astype(low),
            mixing_grad.astype(low),
            gate_grad.astype(low),
            up_grad.astype(low),
            down_grad.astype(low),
        ),
        small,
    )
    down_sum = down_sum.reshape(part_rows, -1, model_width).transpose(1, 0, 2)
    full = jnp.float32
    return (
        layer_output,
        input_grad,
        attention_sum[:, : joined_weight.shape[1]].astype(full),
        attention_sum[:, joined_weight.shape[1] :].astype(full),
        gate_sum.astype(full),
        up_sum.astype(full),
        down_sum.reshape(down_weight.shape).astype(full),
        small_sum[0, :part_rows],
        small_sum[1, :part_rows],
        small_sum[2, :part_rows],
        small_sum[3, :part_rows],
    )


def solution(mesh):
    placed = (
        P(("rep", "shard"), None),
        P("shard", None),
        P("shard", None),
        P("shard", None),
        P("shard", None),
        P("shard", None),
        P("shard"),
        P("shard"),
        P("shard"),
        P("shard"),
        P(("rep", "shard"), None),
        P(("rep", "shard"), None),
        P(("rep", "shard"), None),
    )
    return jax.shard_map(
        on_device,
        mesh=mesh,
        in_specs=placed,
        out_specs=(
            P(("rep", "shard"), None),
            P(("rep", "shard"), None),
            P("shard", None),
            P("shard", None),
            P("shard", None),
            P("shard", None),
            P("shard", None),
            P("shard"),
            P("shard"),
            P("shard"),
            P("shard"),
        ),
        check_vma=False,
    )
```

```python
import functools
import math

import jax
import jax.numpy as jnp
from jax import lax
from jax.experimental import pallas as pl
from jax.experimental.pallas import tpu as pltpu
from jax.sharding import PartitionSpec as P

H = 12
HD = 64

EPSILON = 1e-12
NEG_LARGE = -1e30
LANES = 128
MESH = pl.DeviceIdType.MESH
VMEM_LIMIT = 62 * 1024 * 1024
SLACK = 2
AHEAD = 3


class Plan:
    def __init__(self, width, replicas, shards):
        self.replicas, self.shards = replicas, shards
        self.chips = shards // 2
        self.levels = replicas.bit_length() - 1
        self.orders = 2 if self.levels > 1 and width % (2 * replicas * LANES) == 0 else 1
        self.ways = (tuple(range(self.levels)), tuple(reversed(range(self.levels))))[: self.orders]
        self.piece = width // (replicas * self.orders)
        self.width = width

    def flip(self, rep, bit):
        return rep + (1 << bit) * (1 - 2 * lax.rem(lax.div(rep, 1 << bit), 2))

    def with_bits(self, rep, bits, number):
        for at, bit in enumerate(bits):
            had = lax.rem(lax.div(rep, 1 << bit), 2)
            rep = rep + (1 << bit) * (((number >> at) & 1) - had)
        return rep

    def column(self, rep, order):
        return pl.multiple_of((rep * self.orders + order) * self.piece, LANES)

    def grow(self, rep, order, step):
        bits = self.ways[order][:step]
        return [self.with_bits(rep, bits, number) for number in range(1 << step)]

    def grow_at(self, step):
        return (1 << step) - 1

    def halve(self, rep, order, step):
        bits = self.ways[order][step + 1 :]
        return [self.with_bits(rep, bits, number) for number in range(1 << len(bits))]

    def halve_at(self, step):
        return sum(1 << (self.levels - 1 - at) for at in range(step))


def peer(rep, shard):
    return {"rep": rep, "shard": shard}


def remote(src, dst, send, recv, rep, shard):
    return pltpu.make_async_remote_copy(
        src_ref=src,
        dst_ref=dst,
        send_sem=send,
        recv_sem=recv,
        device_id=peer(rep, shard),
        device_id_type=MESH,
    )


def greet_all(plan, rep, shard):
    barrier = pltpu.get_barrier_semaphore()
    total = plan.replicas * plan.shards

    def hello(step, carry):
        other = lax.rem(rep * plan.shards + shard + step, total)
        pl.semaphore_signal(
            barrier,
            inc=1,
            device_id=peer(lax.div(other, plan.shards), lax.rem(other, plan.shards)),
            device_id_type=MESH,
        )
        return carry

    lax.fori_loop(1, total, hello, 0)
    pl.semaphore_wait(barrier, total - 1)


def greet_near(plan, rep, shard):
    barrier = pltpu.get_barrier_semaphore()
    for step in range(1, plan.shards):
        pl.semaphore_signal(
            barrier,
            inc=1,
            device_id=peer(rep, lax.rem(shard + step, plan.shards)),
            device_id_type=MESH,
        )
    for bit in range(plan.levels):
        pl.semaphore_signal(
            barrier, inc=1, device_id=peer(plan.flip(rep, bit), shard), device_id_type=MESH
        )
    pl.semaphore_wait(barrier, plan.shards - 1 + plan.levels)


def gather_kernel(plan, *refs):
    own, small = refs[:4], refs[4]
    full, small_all = refs[5:9], refs[9]
    stages = refs[10:14]
    (load_sem, store_sem, small_send, small_recv, z_send, z_recv, rep_send, rep_recv, core_send,
     core_recv) = refs[14:]
    rep, shard = lax.axis_index("rep"), lax.axis_index("shard")
    chips, piece = plan.chips, plan.piece
    place, core = lax.div(shard, 2), lax.rem(shard, 2)
    mate = place * 2 + (1 - core)
    rows = own[0].shape[0]

    def part(ref, mat, top, section_rep, order):
        if mat < 3:
            return ref.at[
                pl.ds(pl.multiple_of(top, 8), rows),
                pl.ds(plan.column(section_rep, order), piece),
            ]
        per = own[3].shape[1] // piece
        section = section_rep * plan.orders + order
        return ref.at[
            pl.ds(pl.multiple_of(top + lax.div(section, per) * rows, 8), rows),
            pl.ds(pl.multiple_of(lax.rem(section, per) * piece, LANES), piece),
        ]

    def slab_part(mat, slab, section_rep, order):
        return part(full[mat], mat, slab * own[mat].shape[0], section_rep, order)

    def slab_of(mat, slab):
        deep = own[mat].shape[0]
        return full[mat].at[pl.ds(pl.multiple_of(slab * deep, 8), deep), :]

    sent = []

    def launch(copy):
        copy.start()
        sent.append(copy)

    loads = [pltpu.make_async_copy(own[mat], stages[mat], load_sem.at[mat]) for mat in range(4)]
    for load in loads:
        load.start()
    small_all[shard] = small[...]
    greet_near(plan, rep, shard)

    def small_copy(step):
        return remote(
            small, small_all.at[shard], small_send.at[step - 1], small_recv.at[step - 1],
            rep, lax.rem(shard + step, plan.shards),
        )

    items = [(mat, gap) for mat in range(4) for gap in range(1, chips)]

    def along(mat, gap):
        target = lax.rem(place - gap + chips, chips) * 2 + core
        for order in range(plan.orders):
            launch(remote(
                part(own[mat], mat, 0, rep, order),
                slab_part(mat, shard, rep, order),
                z_send.at[mat, gap - 1, order],
                z_recv.at[mat, gap - 1, order],
                rep, target,
            ))

    for item in items[:AHEAD]:
        along(*item)
    for step in range(1, plan.shards):
        launch(small_copy(step))
    for mat in range(4):
        launch(remote(
            own[mat], slab_of(mat, shard), core_send.at[mat, 0], core_recv.at[mat, 0], rep, mate
        ))

    stores = []
    for mat in range(4):
        loads[mat].wait()
        store = pltpu.make_async_copy(stages[mat], slab_of(mat, shard), store_sem.at[mat])
        store.start()
        stores.append(store)

    def source(gap):
        return lax.rem(place + gap, chips) * 2 + core

    def exchange(mat, gap, order, step):
        slab = source(gap)
        far = plan.flip(rep, plan.ways[order][step])
        at = plan.grow_at(step)
        return [
            remote(
                slab_part(mat, slab, section, order),
                slab_part(mat, slab, section, order),
                rep_send.at[mat, gap - 1, order, at + number],
                rep_recv.at[mat, gap - 1, order, at + number],
                far, shard,
            )
            for number, section in enumerate(plan.grow(rep, order, step))
        ]

    def await_exchange(mat, gap, order, step):
        slab = source(gap)
        far = plan.flip(rep, plan.ways[order][step])
        at = plan.grow_at(step)
        for number, section in enumerate(plan.grow(far, order, step)):
            there = slab_part(mat, slab, section, order)
            remote(
                there, there,
                rep_send.at[mat, gap - 1, order, at + number],
                rep_recv.at[mat, gap - 1, order, at + number],
                far, shard,
            ).wait_recv()

    def relay(mat, gap, step):
        for order in range(plan.orders):
            if step == 0:
                there = slab_part(mat, source(gap), rep, order)
                remote(
                    there, there, z_send.at[mat, gap - 1, order], z_recv.at[mat, gap - 1, order],
                    rep, source(gap),
                ).wait_recv()
            else:
                await_exchange(mat, gap, order, step - 1)
            if step < plan.levels:
                for copy in exchange(mat, gap, order, step):
                    launch(copy)
        if step == plan.levels:
            there = slab_of(mat, source(gap))
            launch(remote(
                there, there, core_send.at[mat, gap], core_recv.at[mat, gap], rep, mate
            ))

    events = [
        (at + SLACK * step, -step, item, step)
        for at, item in enumerate(items)
        for step in range(plan.levels + 1)
    ]
    for at, _, item, step in sorted(events):
        relay(*item, step)
        if step == 0 and at + AHEAD < len(items):
            along(*items[at + AHEAD])
    for mat in range(4):
        stores[mat].wait()
        for gap in range(chips):
            there = slab_of(mat, lax.rem(place + gap, chips) * 2 + (1 - core))
            remote(
                there, there, core_send.at[mat, gap], core_recv.at[mat, gap], rep, mate
            ).wait_recv()
    for step in range(1, plan.shards):
        small_copy(step).wait_recv()
    for copy in sent:
        copy.wait_send()


def gather_weights(plan, own, small):
    hbm = pl.BlockSpec(memory_space=pl.ANY)
    vmem = pl.BlockSpec(memory_space=pltpu.VMEM)
    dma = pltpu.SemaphoreType.DMA
    shapes = [
        jax.ShapeDtypeStruct((array.shape[0] * plan.shards, array.shape[1]), array.dtype)
        for array in own
    ]
    gaps = plan.chips - 1
    crossing = plan.replicas - 1
    return pl.pallas_call(
        functools.partial(gather_kernel, plan),
        out_shape=shapes + [jax.ShapeDtypeStruct((plan.shards,) + small.shape, small.dtype)],
        in_specs=[hbm] * 4 + [vmem],
        out_specs=[hbm] * 4 + [vmem],
        scratch_shapes=[pltpu.VMEM(array.shape, array.dtype) for array in own]
        + [
            dma((4,)),
            dma((4,)),
            dma((plan.shards - 1,)),
            dma((plan.shards - 1,)),
            dma((4, gaps, plan.orders)),
            dma((4, gaps, plan.orders)),
            dma((4, gaps, plan.orders, crossing)),
            dma((4, gaps, plan.orders, crossing)),
            dma((4, plan.chips)),
            dma((4, plan.chips)),
        ],
        compiler_params=pltpu.CompilerParams(
            collective_id=0, has_side_effects=True, vmem_limit_bytes=VMEM_LIMIT
        ),
        name="gather_weights",
    )(*own, small)


def turn_tables(cosine, sine):
    first = (jnp.arange(LANES) % HD < HD // 2)[None, :]
    wide = LANES // HD
    cosine, sine = jnp.tile(cosine, (1, wide)), jnp.tile(sine, (1, wide))
    return cosine, jnp.where(first, -sine, 0.0), jnp.where(first, 0.0, sine)


def product(left, right, left_axis, right_axis):
    return lax.dot_general(
        left, right, (((left_axis,), (right_axis,)), ((), ())), preferred_element_type=jnp.float32
    )


def back_pair(pair, query, key, value, upper, logsum, mask_bias, tables, joined_low, width):
    length = query.shape[0]
    block = min(length, 256)
    span = pl.ds(pl.multiple_of(pair * LANES, LANES), LANES)
    lane = lax.broadcasted_iota(jnp.int32, (1, LANES), 1)
    keys, values = key[:, span], value[:, span]
    query_parts = [0.0] * (length // block)
    key_total = value_total = 0.0
    for half in range(LANES // HD):
        pick = jnp.where(lane // HD == half, 1.0, 0.0).astype(jnp.bfloat16)
        scaled = pick * jnp.bfloat16(1.0 / math.sqrt(HD))
        keys_scaled = keys * scaled
        rowsum = logsum[pl.ds(pair * (LANES // HD) + half, 1), :]
        for at in range(length // block):
            rows = slice(at * block, (at + 1) * block)
            queries_scaled = query[rows, span] * scaled
            grads = upper[rows, span] * pick
            scores = product(keys, queries_scaled, 1, 1) + mask_bias[:, rows]
            probs = jnp.exp(scores - rowsum[:, rows])
            dprobs = product(values, grads, 1, 1)
            dots = jnp.sum(probs * dprobs, axis=0, keepdims=True)
            score_grad = (probs * (dprobs - dots)).astype(jnp.bfloat16)
            value_total += product(probs.astype(jnp.bfloat16), grads, 1, 0)
            key_total += product(score_grad, queries_scaled, 1, 0)
            query_parts[at] += product(score_grad, keys_scaled, 0, 0)
    cosine, before, after = tables

    def unrotate(grad, rows):
        return (
            grad * cosine[rows, :]
            - pltpu.roll(grad, LANES - HD // 2, 1) * before[rows, :]
            - pltpu.roll(grad, HD // 2, 1) * after[rows, :]
        ).astype(jnp.bfloat16)

    for at, part in enumerate(query_parts):
        rows = slice(at * block, (at + 1) * block)
        joined_low[rows, span] = unrotate(part, rows)
    everything = slice(0, length)
    joined_low[:, pl.ds(pl.multiple_of(width + pair * LANES, LANES), LANES)] = unrotate(
        key_total, everything
    )
    joined_low[:, pl.ds(pl.multiple_of(2 * width + pair * LANES, LANES), LANES)] = (
        value_total.astype(jnp.bfloat16)
    )


def sum_kernel(plan, *refs):
    mixing, gate, up, down, small = refs[:5]
    carried, weight = refs[5:17], refs[17]
    outs, small_out, input_grad = refs[18:22], refs[22], refs[23]
    (held, mate_in, rep_in, z_in, final, small_in, load_sem, out_sem, small_sem, mate_send,
     mate_recv, rep_send, rep_recv, z_send, z_recv, last_send, last_recv) = refs[24:41]
    here, weight_here = refs[41:53], refs[53]
    joined_low, joined, mask_bias, tokens_across, fetch_sem, result_sem = refs[54:60]
    result_here = refs[60]
    rep, shard = lax.axis_index("rep"), lax.axis_index("shard")
    chips, piece, levels = plan.chips, plan.piece, plan.levels
    place, core = lax.div(shard, 2), lax.rem(shard, 2)
    mate = place * 2 + (1 - core)
    rows = held.shape[2]
    total = plan.replicas * plan.shards
    early = 3 * chips
    count = 4 * chips
    (query, key, value, upper, logsum, segment_down, segment_across, cosine, before, after, tokens,
     inner_grad) = here
    width = query.shape[1]
    pairs = width // LANES

    def fragments(turn, slab):
        top = pl.multiple_of(slab * rows, 8)
        if turn == 3:
            wide = joined.shape[1]
            return [
                (joined.at[pl.ds(top, rows), :], 0, wide),
                (mixing.at[pl.ds(top, rows), :], wide, mixing.shape[1]),
            ]
        if turn > 0:
            return [((gate, up)[turn - 1].at[pl.ds(top, rows), :], 0, plan.width)]
        wide = down.shape[1]
        return [
            (
                down.at[
                    pl.ds(pl.multiple_of(slab * (rows * (plan.width // wide)) + at * rows, 8), rows),
                    :,
                ],
                at * wide,
                wide,
            )
            for at in range(plan.width // wide)
        ]

    gaps = list(range(1, chips)) + [0]

    def slab_at(gap, which):
        return lax.rem(place + gap, chips) * 2 + which

    def load(turn):
        for gap in gaps:
            for ref, left, wide in fragments(turn, slab_at(gap, core)):
                pltpu.make_async_copy(
                    ref, held.at[turn, gap, :, pl.ds(left, wide)], load_sem.at[turn, gap]
                ).start()

    def give(turn):
        for gap in gaps:
            for ref, left, wide in fragments(turn, slab_at(gap, 1 - core)):
                remote(
                    ref, mate_in.at[turn, gap, :, pl.ds(left, wide)],
                    mate_send.at[turn, gap], mate_recv.at[turn, gap], rep, mate,
                ).start()

    for turn in range(3):
        load(turn)
    fetches = [
        pltpu.make_async_copy(far, near, fetch_sem.at[at])
        for at, (far, near) in enumerate(zip(carried, here))
    ]
    fetches.append(
        pltpu.make_async_copy(
            weight.at[:, pl.ds(0, 3 * width)], weight_here, fetch_sem.at[len(carried)]
        )
    )
    for fetch in fetches:
        fetch.start()
    greet_all(plan, rep, shard)
    for turn in range(3):
        give(turn)

    def small_go(step, carry):
        other = lax.rem(rep * plan.shards + shard + step, total)
        other_rep, other_shard = lax.div(other, plan.shards), lax.rem(other, plan.shards)
        remote(
            small.at[other_shard], small_in.at[step - 1], small_sem.at[0], small_sem.at[1],
            other_rep, other_shard,
        ).start()
        return carry

    lax.fori_loop(1, total, small_go, 0)

    def whole_mate(turn, gap):
        return remote(
            mate_in.at[turn, gap], mate_in.at[turn, gap],
            mate_send.at[turn, gap], mate_recv.at[turn, gap], rep, mate,
        )

    def cross(turn, gap, order, step):
        far = plan.flip(rep, plan.ways[order][step])
        at = plan.halve_at(step)
        copies = [
            remote(
                held.at[turn, gap, :, pl.ds(plan.column(section, order), piece)],
                rep_in.at[turn, gap, order, at + number],
                rep_send.at[turn, gap, order, at + number],
                rep_recv.at[turn, gap, order, at + number],
                far, shard,
            )
            for number, section in enumerate(plan.halve(far, order, step))
        ]
        return copies, [plan.column(section, order) for section in plan.halve(rep, order, step)]

    wide_piece = plan.orders * piece
    own_columns = pl.ds(pl.multiple_of(rep * wide_piece, LANES), wide_piece)

    def z_copy(turn, gap):
        return remote(
            held.at[turn, gap, :, own_columns],
            z_in.at[turn, gap - 1],
            z_send.at[turn, gap - 1], z_recv.at[turn, gap - 1],
            rep, slab_at(gap, core),
        )

    def item_of(number):
        return lax.div(number, chips), lax.rem(lax.rem(number, chips) + 1, chips)

    def advance(number, step):
        turn, gap = item_of(number)
        if step == 0:
            pltpu.make_async_copy(
                held.at[turn, gap], held.at[turn, gap], load_sem.at[turn, gap]
            ).wait()
            whole_mate(turn, gap).wait_recv()

            def add(at, carry):
                span = pl.ds(pl.multiple_of(at * piece, LANES), piece)
                held[turn, gap, :, span] = (
                    held[turn, gap, :, span].astype(jnp.float32)
                    + mate_in[turn, gap, :, span].astype(jnp.float32)
                ).astype(jnp.bfloat16)
                return carry

            lax.fori_loop(0, plan.width // piece, add, 0)
        else:
            for order in range(plan.orders):
                copies, columns = cross(turn, gap, order, step - 1)
                at = plan.halve_at(step - 1)
                for index, (copy, column) in enumerate(zip(copies, columns)):
                    copy.wait_recv()
                    span = pl.ds(column, piece)
                    held[turn, gap, :, span] = (
                        held[turn, gap, :, span].astype(jnp.float32)
                        + rep_in[turn, gap, order, at + index].astype(jnp.float32)
                    ).astype(jnp.bfloat16)
        if step < levels:
            for order in range(plan.orders):
                for copy in cross(turn, gap, order, step)[0]:
                    copy.start()
        else:
            @pl.when(gap > 0)
            def _():
                z_copy(turn, gap).start()

    def spread(turn, order, step):
        far = plan.flip(rep, plan.ways[order][step])
        at = plan.grow_at(step)
        return [
            remote(
                final.at[turn, :, pl.ds(plan.column(section, order), piece)],
                final.at[turn, :, pl.ds(plan.column(section, order), piece)],
                last_send.at[turn, order, at + number],
                last_recv.at[turn, order, at + number],
                far, shard,
            )
            for number, section in enumerate(plan.grow(rep, order, step))
        ]

    def await_spread(turn, order, step):
        far = plan.flip(rep, plan.ways[order][step])
        at = plan.grow_at(step)
        for number, section in enumerate(plan.grow(far, order, step)):
            there = final.at[turn, :, pl.ds(plan.column(section, order), piece)]
            remote(
                there, there,
                last_send.at[turn, order, at + number],
                last_recv.at[turn, order, at + number],
                far, shard,
            ).wait_recv()

    def finish(turn, step):
        if step == 0:
            for gap in range(1, chips):
                z_copy(turn, gap).wait_recv()
            for order in range(plan.orders):
                span = pl.ds(plan.column(rep, order), piece)
                part = pl.ds(order * piece, piece)
                value = held[turn, 0, :, span].astype(jnp.float32)
                for gap in range(1, chips):
                    value = value + z_in[turn, gap - 1, :, part].astype(jnp.float32)
                final[turn, :, span] = value.astype(jnp.bfloat16)
        else:
            for order in range(plan.orders):
                await_spread(turn, order, step - 1)
        if step < levels:
            for order in range(plan.orders):
                for copy in spread(turn, order, step):
                    copy.start()

    def tick(now):
        for step in reversed(range(levels + 1)):
            late = now - (SLACK * (levels + step + 1) + chips - 1)

            @pl.when((late >= 0) & (lax.rem(late + chips, chips) == 0) & (late < count))
            def _(late=late, step=step):
                finish(lax.div(late, chips), step)

        for step in reversed(range(levels + 1)):
            number = now - SLACK * step

            @pl.when((number >= 0) & (number < count))
            def _(number=number, step=step):
                advance(number, step)

    tick(0)
    for fetch in fetches:
        fetch.wait()
    mask_bias[...] = jnp.where(segment_down[:, 0:1] == segment_across[0:1, :], 0.0, NEG_LARGE)

    def attend(now, carry):
        @pl.when(now < pairs)
        def _():
            back_pair(
                now, query, key, value, upper, logsum, mask_bias, (cosine, before, after),
                joined_low, width,
            )

        @pl.when(now + 1 < early)
        def _():
            tick(now + 1)
        return carry

    lax.fori_loop(0, max(pairs, early - 1), attend, 0)
    tokens_across[...] = tokens[...].T

    def weigh(at, carry):
        span = pl.ds(pl.multiple_of(at * (width // 2), LANES), width // 2)
        joined[:, span] = product(tokens_across[...], joined_low[:, span], 1, 0).astype(
            jnp.bfloat16
        )
        return carry

    lax.fori_loop(0, 6, weigh, 0)
    load(3)
    give(3)

    def back(at, carry):
        low = pl.ds(pl.multiple_of(at * 256, 256), 256)
        result_here[:, low] = (
            inner_grad[:, low] + product(joined_low[...], weight_here[low, :], 1, 1)
        ).astype(jnp.bfloat16)
        return carry

    lax.fori_loop(0, width // 256, back, 0)
    result_copy = pltpu.make_async_copy(result_here, input_grad, result_sem)
    result_copy.start()

    def late_tick(now, carry):
        tick(now)
        return carry

    lax.fori_loop(early, count + SLACK * (2 * levels + 1), late_tick, 0)

    everything = remote(small_in, small_in, small_sem.at[0], small_sem.at[1], rep, mate)
    everything.wait_recv()

    def gain(at, value):
        return value + small_in[at]

    small_out[...] = lax.fori_loop(0, total - 1, gain, small[shard])
    everything.wait_send()
    for turn in range(4):
        pltpu.make_async_copy(final.at[turn], outs[turn], out_sem.at[turn]).start()

    def drain(number, carry):
        turn, gap = item_of(number)
        whole_mate(turn, gap).wait_send()
        for order in range(plan.orders):
            for step in range(levels):
                for copy in cross(turn, gap, order, step)[0]:
                    copy.wait_send()

        @pl.when(gap > 0)
        def _():
            z_copy(turn, gap).wait_send()
        return carry

    lax.fori_loop(0, count, drain, 0)
    for turn in range(4):
        for order in range(plan.orders):
            for step in range(levels):
                for copy in spread(turn, order, step):
                    copy.wait_send()
        pltpu.make_async_copy(final.at[turn], outs[turn], out_sem.at[turn]).wait()
    result_copy.wait()


def sum_grads(plan, grads, small, carried, weight):
    hbm = pl.BlockSpec(memory_space=pl.ANY)
    vmem = pl.BlockSpec(memory_space=pltpu.VMEM)
    dma = pltpu.SemaphoreType.DMA
    chips, gaps, crossing = plan.chips, plan.chips - 1, plan.replicas - 1
    rows = grads[0].shape[0] // plan.shards
    low = jnp.bfloat16
    total = plan.replicas * plan.shards
    length, width = carried[0].shape
    return pl.pallas_call(
        functools.partial(sum_kernel, plan),
        out_shape=[jax.ShapeDtypeStruct((rows, plan.width), low)] * 4
        + [
            jax.ShapeDtypeStruct(small.shape[1:], small.dtype),
            jax.ShapeDtypeStruct((length, width), low),
        ],
        in_specs=[hbm] * 4 + [vmem] + [hbm] * (len(carried) + 1),
        out_specs=[hbm] * 4 + [vmem, hbm],
        scratch_shapes=[
            pltpu.VMEM((4, chips, rows, plan.width), low),
            pltpu.VMEM((4, chips, rows, plan.width), low),
            pltpu.VMEM((4, chips, plan.orders, crossing, rows, plan.piece), low),
            pltpu.VMEM((4, gaps, rows, plan.orders * plan.piece), low),
            pltpu.VMEM((4, rows, plan.width), low),
            pltpu.VMEM((total - 1,) + small.shape[1:], small.dtype),
            dma((4, chips)),
            dma((4,)),
            dma((2,)),
            dma((4, chips)),
            dma((4, chips)),
            dma((4, chips, plan.orders, crossing)),
            dma((4, chips, plan.orders, crossing)),
            dma((4, gaps)),
            dma((4, gaps)),
            dma((4, plan.orders, crossing)),
            dma((4, plan.orders, crossing)),
        ]
        + [pltpu.VMEM(array.shape, array.dtype) for array in carried]
        + [
            pltpu.VMEM((width, 3 * width), low),
            pltpu.VMEM((length, 3 * width), low),
            pltpu.VMEM((width, 3 * width), low),
            pltpu.VMEM((length, length), jnp.float32),
            pltpu.VMEM((width, length), low),
            dma((len(carried) + 1,)),
            dma,
            pltpu.VMEM((length, width), low),
        ],
        compiler_params=pltpu.CompilerParams(
            collective_id=1, has_side_effects=True, vmem_limit_bytes=VMEM_LIMIT
        ),
        name="sum_grads",
    )(*grads, small, *carried, weight)


def rotation(positions):
    halves = jnp.arange(HD // 2, dtype=jnp.float32)
    inverse = 1000.0 ** (-(2.0 * halves) / HD)
    angles = positions.astype(jnp.float32)[..., None] * inverse
    angles = jnp.concatenate([angles, angles], axis=-1)
    return (jnp.cos(angles), jnp.sin(angles))


def rotate(values, cosine, sine_table):
    half_size = values.shape[-1] // 2
    turned = jnp.concatenate([-values[..., half_size:], values[..., :half_size]], axis=-1)
    return values * cosine[..., None, :] + turned * sine_table[..., None, :]


def layer_norm(values, gain, shift):
    centred = values - jnp.mean(values, axis=-1, keepdims=True)
    variance = jnp.mean(centred * centred, axis=-1, keepdims=True)
    return centred * lax.rsqrt(variance + EPSILON) * gain + shift


def transposed_product(left, right):
    return lax.dot_general(
        left, right, (((1,), (1,)), ((), ())), preferred_element_type=jnp.float32
    )


def token_contract(left, right):
    return lax.dot_general(
        left, right, (((0,), (0,)), ((), ())), preferred_element_type=jnp.float32
    )


def to_heads(values, group_size):
    length = values.shape[0]
    per_head = values.reshape(length, H, HD).transpose(1, 0, 2)
    return per_head.reshape(H // group_size, group_size, length, HD)


def from_heads(values):
    length = values.shape[2]
    merged = values.reshape(H, length, HD).transpose(1, 0, 2)
    return merged.reshape(length, H * HD)


def on_device(
    tokens,
    joined_weight,
    mixing_weight,
    gate_weight,
    up_weight,
    down_weight,
    inner_gain,
    inner_shift,
    outer_gain,
    outer_shift,
    segments,
    positions,
    cotangent,
):
    replicas, shards = lax.axis_size("rep"), lax.axis_size("shard")
    plan = Plan(gate_weight.shape[1], replicas, shards)
    part_rows = joined_weight.shape[0]
    own_vectors = jnp.stack([inner_gain, inner_shift, outer_gain, outer_shift]).astype(jnp.float32)
    own_vectors = jnp.pad(own_vectors, ((0, 4), (0, LANES - part_rows)))
    attention_full, gate_full, upward_full, down_full, vectors = gather_weights(
        plan,
        (
            jnp.concatenate([joined_weight, mixing_weight], axis=1),
            gate_weight,
            up_weight,
            down_weight,
        ),
        own_vectors,
    )
    joined_full = attention_full[:, : joined_weight.shape[1]]
    mixing_full = attention_full[:, joined_weight.shape[1] :]
    vectors = vectors[:, :4, :part_rows].transpose(1, 0, 2).reshape(4, shards * part_rows)
    innergain_full, innershift_full, outergain_full, outershift_full = vectors
    length = tokens.shape[0]
    model_width = tokens.shape[1]
    group_size = 4
    score_scale = 1.0 / math.sqrt(HD)
    same_doc = segments[0][:, None] == segments[0][None, :]
    cosine, sine_table = rotation(positions[0])
    joined_rows = jnp.dot(tokens, joined_full, preferred_element_type=jnp.float32)
    pre_query = joined_rows[:, :model_width].reshape(length, H, HD)
    pre_key = joined_rows[:, model_width : 2 * model_width].reshape(length, H, HD)
    query_low = rotate(pre_query, cosine, sine_table).astype(jnp.bfloat16)
    query_low = query_low.reshape(length, model_width)
    key_low = rotate(pre_key, cosine, sine_table).astype(jnp.bfloat16)
    key_low = key_low.reshape(length, model_width)
    value_low = joined_rows[:, 2 * model_width :].astype(jnp.bfloat16)
    query_heads = to_heads(query_low, group_size)
    key_heads = to_heads(key_low, group_size)
    value_heads = to_heads(value_low, group_size)

    def head_scores(query_block, key_block):
        scores = (
            jnp.einsum("hqd,hkd->hqk", query_block, key_block, preferred_element_type=jnp.float32)
            * score_scale
        )
        return jnp.where(same_doc, scores, NEG_LARGE)

    def head_forward(block):
        query_block, key_block, value_block = block
        scores = head_scores(query_block, key_block)
        highest = jnp.max(scores, axis=-1, keepdims=True)
        shifted = jnp.exp(scores - highest)
        denominator = jnp.sum(shifted, axis=-1, keepdims=True)
        probs_low = (shifted / denominator).astype(jnp.bfloat16)
        attended = jnp.einsum(
            "hqk,hkd->hqd", probs_low, value_block, preferred_element_type=jnp.float32
        )
        return (attended.astype(jnp.bfloat16), highest + jnp.log(denominator))

    attended_heads, logsum = lax.map(head_forward, (query_heads, key_heads, value_heads))
    attended_low = from_heads(attended_heads)
    branch = jnp.dot(attended_low, mixing_full, preferred_element_type=jnp.float32)
    inner_resid = tokens.astype(jnp.float32) + branch
    normed, inner_pull = jax.vjp(
        layer_norm,
        inner_resid,
        innergain_full.astype(jnp.float32),
        innershift_full.astype(jnp.float32),
    )
    normed_low = normed.astype(jnp.bfloat16)
    gate_rows = jnp.dot(normed_low, gate_full, preferred_element_type=jnp.float32)
    upward = jnp.dot(normed_low, upward_full, preferred_element_type=jnp.float32)
    active, silu_pull = jax.vjp(
        lambda first, second: jax.nn.silu(first) * second, gate_rows, upward
    )
    active_low = active.astype(jnp.bfloat16)
    result = jnp.dot(active_low, down_full, preferred_element_type=jnp.float32)
    final, outer_pull = jax.vjp(
        layer_norm,
        normed + result,
        outergain_full.astype(jnp.float32),
        outershift_full.astype(jnp.float32),
    )
    layer_output = final.astype(jnp.bfloat16)
    gate_back, upward_back, down_back = gate_full, upward_full, down_full
    outer_grad, outergain_grad, outershift_grad = outer_pull(cotangent.astype(jnp.float32))
    result_grad = outer_grad.astype(jnp.bfloat16)
    down_grad = token_contract(active_low, result_grad)
    active_grad = transposed_product(result_grad, down_back)
    gate_part, upward_part = silu_pull(active_grad)
    gate_low = gate_part.astype(jnp.bfloat16)
    upward_low = upward_part.astype(jnp.bfloat16)
    gate_grad = token_contract(normed_low, gate_low)
    up_grad = token_contract(normed_low, upward_low)
    normed_grad = (
        outer_grad
        + transposed_product(gate_low, gate_back)
        + transposed_product(upward_low, upward_back)
    )
    inner_grad, innergain_grad, innershift_grad = inner_pull(normed_grad)
    mixing_back = mixing_full
    branch_grad = inner_grad.astype(jnp.bfloat16)
    mixing_grad = token_contract(attended_low, branch_grad)
    attended_grad = transposed_product(branch_grad, mixing_back).astype(jnp.bfloat16)

    small = jnp.stack([innergain_grad, innershift_grad, outergain_grad, outershift_grad])
    small = small.reshape(4, shards, part_rows).transpose(1, 0, 2)
    small = jnp.pad(small, ((0, 0), (0, 4), (0, LANES - part_rows)))
    low = jnp.bfloat16
    cosine_wide, before, after = turn_tables(cosine, sine_table)
    down_sum, gate_sum, up_sum, attention_sum, small_sum, input_grad = sum_grads(
        plan,
        (mixing_grad.astype(low), gate_grad.astype(low), up_grad.astype(low), down_grad.astype(low)),
        small,
        (
            query_low,
            key_low,
            value_low,
            attended_grad,
            logsum.reshape(H, length),
            jnp.broadcast_to(segments[0][:, None], (length, LANES)),
            segments,
            cosine_wide,
            before,
            after,
            tokens,
            inner_grad,
        ),
        attention_full,
    )
    down_sum = down_sum.reshape(part_rows, -1, model_width).transpose(1, 0, 2)
    full = jnp.float32
    return (
        layer_output,
        input_grad,
        attention_sum[:, : joined_weight.shape[1]].astype(full),
        attention_sum[:, joined_weight.shape[1] :].astype(full),
        gate_sum.astype(full),
        up_sum.astype(full),
        down_sum.reshape(down_weight.shape).astype(full),
        small_sum[0, :part_rows],
        small_sum[1, :part_rows],
        small_sum[2, :part_rows],
        small_sum[3, :part_rows],
    )


def solution(mesh):
    placed = (
        P(("rep", "shard"), None),
        P("shard", None),
        P("shard", None),
        P("shard", None),
        P("shard", None),
        P("shard", None),
        P("shard"),
        P("shard"),
        P("shard"),
        P("shard"),
        P(("rep", "shard"), None),
        P(("rep", "shard"), None),
        P(("rep", "shard"), None),
    )
    return jax.shard_map(
        on_device,
        mesh=mesh,
        in_specs=placed,
        out_specs=(
            P(("rep", "shard"), None),
            P(("rep", "shard"), None),
            P("shard", None),
            P("shard", None),
            P("shard", None),
            P("shard", None),
            P("shard", None),
            P("shard"),
            P("shard"),
            P("shard"),
            P("shard"),
        ),
        check_vma=False,
    )
```

```python
import functools
import math

import jax
import jax.numpy as jnp
import numpy as np
from jax import lax
from jax.experimental import pallas as pl
from jax.experimental.pallas import tpu as pltpu
from jax.sharding import PartitionSpec as P

H = 12
HD = 64

EPSILON = 1e-12
NEG_LARGE = -1e30
LANES = 128
MESH = pl.DeviceIdType.MESH
VMEM_LIMIT = 62 * 1024 * 1024
SLACK = 2
AHEAD = 3


class Plan:
    def __init__(self, width, replicas, shards):
        self.replicas, self.shards = replicas, shards
        self.chips = shards // 2
        self.levels = replicas.bit_length() - 1
        self.orders = 2 if self.levels > 1 and width % (2 * replicas * LANES) == 0 else 1
        self.ways = (tuple(range(self.levels)), tuple(reversed(range(self.levels))))[: self.orders]
        self.piece = width // (replicas * self.orders)
        self.width = width

    def flip(self, rep, bit):
        return rep + (1 << bit) * (1 - 2 * lax.rem(lax.div(rep, 1 << bit), 2))

    def with_bits(self, rep, bits, number):
        for at, bit in enumerate(bits):
            had = lax.rem(lax.div(rep, 1 << bit), 2)
            rep = rep + (1 << bit) * (((number >> at) & 1) - had)
        return rep

    def column(self, rep, order):
        return pl.multiple_of((rep * self.orders + order) * self.piece, LANES)

    def grow(self, rep, order, step):
        bits = self.ways[order][:step]
        return [self.with_bits(rep, bits, number) for number in range(1 << step)]

    def grow_at(self, step):
        return (1 << step) - 1

    def halve(self, rep, order, step):
        bits = self.ways[order][step + 1 :]
        return [self.with_bits(rep, bits, number) for number in range(1 << len(bits))]

    def halve_at(self, step):
        return sum(1 << (self.levels - 1 - at) for at in range(step))


def peer(rep, shard):
    return {"rep": rep, "shard": shard}


def remote(src, dst, send, recv, rep, shard):
    return pltpu.make_async_remote_copy(
        src_ref=src,
        dst_ref=dst,
        send_sem=send,
        recv_sem=recv,
        device_id=peer(rep, shard),
        device_id_type=MESH,
    )


def greet_all(plan, rep, shard):
    barrier = pltpu.get_barrier_semaphore()
    total = plan.replicas * plan.shards

    def hello(step, carry):
        other = lax.rem(rep * plan.shards + shard + step, total)
        pl.semaphore_signal(
            barrier,
            inc=1,
            device_id=peer(lax.div(other, plan.shards), lax.rem(other, plan.shards)),
            device_id_type=MESH,
        )
        return carry

    lax.fori_loop(1, total, hello, 0)
    pl.semaphore_wait(barrier, total - 1)


def greet_near(plan, rep, shard):
    barrier = pltpu.get_barrier_semaphore()
    for step in range(1, plan.shards):
        pl.semaphore_signal(
            barrier,
            inc=1,
            device_id=peer(rep, lax.rem(shard + step, plan.shards)),
            device_id_type=MESH,
        )
    for bit in range(plan.levels):
        pl.semaphore_signal(
            barrier, inc=1, device_id=peer(plan.flip(rep, bit), shard), device_id_type=MESH
        )
    pl.semaphore_wait(barrier, plan.shards - 1 + plan.levels)


def product(left, right, left_axis, right_axis):
    return lax.dot_general(
        left, right, (((left_axis,), (right_axis,)), ((), ())), preferred_element_type=jnp.float32
    )


def forward_pair(pair, query, key, value, mask_bias, attended, logsum):
    length = query.shape[0]
    block = min(length, 256)
    span = pl.ds(pl.multiple_of(pair * LANES, LANES), LANES)
    lane = lax.broadcasted_iota(jnp.int32, (1, LANES), 1)
    keys, values = key[:, span], value[:, span]
    parts = [0.0] * (length // block)
    for half in range(LANES // HD):
        pick = jnp.where(lane // HD == half, 1.0, 0.0).astype(jnp.bfloat16)
        scaled = pick * jnp.bfloat16(1.0 / math.sqrt(HD))
        picked = values * pick
        for at in range(length // block):
            rows = slice(at * block, (at + 1) * block)
            scores = product(keys, query[rows, span] * scaled, 1, 1) + mask_bias[:, rows]
            highest = jnp.max(scores, axis=0, keepdims=True)
            shifted = jnp.exp(scores - highest)
            denominator = jnp.sum(shifted, axis=0, keepdims=True)
            logsum[pl.ds(pair * (LANES // HD) + half, 1), rows] = highest + jnp.log(denominator)
            probs = (shifted * (1.0 / denominator)).astype(jnp.bfloat16)
            parts[at] += product(probs, picked, 0, 0)
    for at, part in enumerate(parts):
        attended[at * block : (at + 1) * block, span] = part.astype(jnp.bfloat16)


def gather_kernel(plan, *refs):
    own, small = refs[:4], refs[4]
    carried = refs[5:9]
    full, small_all = refs[9:13], refs[13]
    results = refs[14:23]
    stages = refs[23:27]
    (load_sem, store_sem, small_send, small_recv, z_send, z_recv, rep_send, rep_recv, core_send,
     core_recv) = refs[27:37]
    tokens, marks, segment_across, rates = refs[37:41]
    near = refs[41:50]
    query, key, value, attended, logsum, inner_resid, cosine, before, after = near
    weight, mask_bias, fetch_sem, weight_sem, result_sem = refs[50:55]
    rep, shard = lax.axis_index("rep"), lax.axis_index("shard")
    chips, piece = plan.chips, plan.piece
    place, core = lax.div(shard, 2), lax.rem(shard, 2)
    mate = place * 2 + (1 - core)
    rows = own[0].shape[0]
    length, width = tokens.shape
    pairs = width // LANES

    def part(ref, mat, top, section_rep, order):
        if mat < 3:
            return ref.at[
                pl.ds(pl.multiple_of(top, 8), rows),
                pl.ds(plan.column(section_rep, order), piece),
            ]
        per = own[3].shape[1] // piece
        section = section_rep * plan.orders + order
        return ref.at[
            pl.ds(pl.multiple_of(top + lax.div(section, per) * rows, 8), rows),
            pl.ds(pl.multiple_of(lax.rem(section, per) * piece, LANES), piece),
        ]

    def slab_part(mat, slab, section_rep, order):
        return part(full[mat], mat, slab * own[mat].shape[0], section_rep, order)

    def slab_of(mat, slab):
        deep = own[mat].shape[0]
        return full[mat].at[pl.ds(pl.multiple_of(slab * deep, 8), deep), :]

    sent = []

    def launch(copy):
        copy.start()
        sent.append(copy)

    loads = [pltpu.make_async_copy(own[mat], stages[mat], load_sem.at[mat]) for mat in range(4)]
    for load in loads:
        load.start()
    fetches = [
        pltpu.make_async_copy(far, here, fetch_sem.at[at])
        for at, (far, here) in enumerate(zip(carried, (tokens, marks, segment_across, rates)))
    ]
    for fetch in fetches:
        fetch.start()
    small_all[shard] = small[...]
    greet_near(plan, rep, shard)

    def small_copy(step):
        return remote(
            small, small_all.at[shard], small_send.at[step - 1], small_recv.at[step - 1],
            rep, lax.rem(shard + step, plan.shards),
        )

    fewest = jnp.minimum(place, chips - 1 - place)
    longer_above = jnp.where(2 * place < chips - 1, 1, 0)

    def nearest(number):
        inside = number <= 2 * fewest
        above = jnp.where(inside, number % 2, longer_above)
        distance = jnp.where(inside, (number + 1) // 2, number - fewest)
        return place + distance * (2 * above - 1), above

    def hop(mat, origin, down, order, source):
        return remote(
            source,
            slab_part(mat, origin * 2 + core, rep, order),
            z_send.at[mat, origin, down, order],
            z_recv.at[mat, origin, order],
            rep, (place + 1 - 2 * down) * 2 + core,
        )

    def own_hop(mat, down, order):
        return hop(mat, place, down, order, part(own[mat], mat, 0, rep, order))

    def next_hop(mat, number, order):
        origin, above = nearest(number)
        there = slab_part(mat, origin * 2 + core, rep, order)
        return hop(mat, origin, above, order, there)

    def leads(down):
        return (place > 0) if down else (place < chips - 1)

    def goes_on(number):
        _, above = nearest(number)
        onward = place + 1 - 2 * above
        return (onward >= 0) & (onward < chips)

    def along(mat, act):
        for down in range(2):
            @pl.when(leads(down))
            def _(down=down):
                for order in range(plan.orders):
                    act(own_hop(mat, down, order))

    def on(mat, number, act):
        @pl.when(goes_on(number))
        def _():
            for order in range(plan.orders):
                act(next_hop(mat, number, order))

    def give(mat):
        launch(remote(
            own[mat], slab_of(mat, shard), core_send.at[mat, 0], core_recv.at[mat, 0], rep, mate
        ))

    for mat in range(2):
        along(mat, lambda copy: copy.start())
    give(0)
    for step in range(1, plan.shards):
        launch(small_copy(step))
    for mat in range(1, 4):
        give(mat)
    stores = []
    for mat in range(4):
        loads[mat].wait()
        store = pltpu.make_async_copy(stages[mat], slab_of(mat, shard), store_sem.at[mat])
        store.start()
        stores.append(store)

    for fetch in fetches:
        fetch.wait()
    mask_bias[...] = jnp.where(marks[:, 0:1] == segment_across[0:1, :], 0.0, NEG_LARGE)
    angles = marks[:, 1:2].astype(jnp.float32) * rates[0:1, :]
    first = lax.broadcasted_iota(jnp.int32, (1, LANES), 1) % HD < HD // 2
    cosine[...] = jnp.cos(angles)
    sine = jnp.sin(angles)
    before[...] = jnp.where(first, -sine, 0.0)
    after[...] = jnp.where(first, 0.0, sine)

    def source(number):
        return nearest(number)[0] * 2 + core

    def exchange(mat, number, order, step):
        slab = source(number)
        far = plan.flip(rep, plan.ways[order][step])
        at = plan.grow_at(step)
        return [
            remote(
                slab_part(mat, slab, section, order),
                slab_part(mat, slab, section, order),
                rep_send.at[mat, number - 1, order, at + index],
                rep_recv.at[mat, number - 1, order, at + index],
                far, shard,
            )
            for index, section in enumerate(plan.grow(rep, order, step))
        ]

    def await_exchange(mat, number, order, step):
        slab = source(number)
        far = plan.flip(rep, plan.ways[order][step])
        at = plan.grow_at(step)
        for index, section in enumerate(plan.grow(far, order, step)):
            there = slab_part(mat, slab, section, order)
            remote(
                there, there,
                rep_send.at[mat, number - 1, order, at + index],
                rep_recv.at[mat, number - 1, order, at + index],
                far, shard,
            ).wait_recv()

    def relay(mat, number, step):
        for order in range(plan.orders):
            if step == 0:
                origin, _ = nearest(number)
                there = slab_part(mat, origin * 2 + core, rep, order)
                remote(
                    there, there, z_send.at[mat, origin, 0, order], z_recv.at[mat, origin, order],
                    rep, mate,
                ).wait_recv()
            else:
                await_exchange(mat, number, order, step - 1)
            if step < plan.levels:
                for copy in exchange(mat, number, order, step):
                    launch(copy)
        if step == 0:
            on(mat, number, lambda copy: copy.start())
            if number == 1 and mat + 2 < 4:
                along(mat + 2, lambda copy: copy.start())
        if step == plan.levels:
            there = slab_of(mat, source(number))
            launch(remote(
                there, there, core_send.at[mat, number], core_recv.at[mat, number], rep, mate
            ))

    def await_core(mat):
        stores[mat].wait()
        for number in range(chips):
            slab = (place if number == 0 else nearest(number)[0]) * 2 + (1 - core)
            there = slab_of(mat, slab)
            remote(
                there, there, core_send.at[mat, number], core_recv.at[mat, number], rep, mate
            ).wait_recv()

    weight_load = pltpu.make_async_copy(full[0], weight, weight_sem)

    def fetch_weight():
        await_core(0)
        weight_load.start()

    def project():
        weight_load.wait()
        tile = width // 2

        def columns(at):
            span = pl.ds(pl.multiple_of(at * tile, LANES), tile)
            return product(tokens[...], weight[:, span], 1, 0)

        def turned(at, carry):
            joined = columns(at)
            for down in range(tile // LANES):
                vector = joined[:, down * LANES : (down + 1) * LANES]
                spot = pl.ds(pl.multiple_of(lax.rem(at, 2) * tile + down * LANES, LANES), LANES)
                low = (
                    vector * cosine[...]
                    + pltpu.roll(vector, LANES - HD // 2, 1) * before[...]
                    + pltpu.roll(vector, HD // 2, 1) * after[...]
                ).astype(jnp.bfloat16)

                @pl.when(at < 2)
                def _():
                    query[:, spot] = low

                @pl.when(at >= 2)
                def _():
                    key[:, spot] = low
            return carry

        lax.fori_loop(0, 4, turned, 0)

        def plain(at, carry):
            value[:, pl.ds(pl.multiple_of(at * tile, LANES), tile)] = columns(at + 4).astype(
                jnp.bfloat16
            )
            return carry

        lax.fori_loop(0, 2, plain, 0)

    def attend(low, high):
        def one(pair, carry):
            forward_pair(pair, query, key, value, mask_bias, attended, logsum)
            return carry

        lax.fori_loop(low, high, one, 0)

    copies = [
        pltpu.make_async_copy(here, far, result_sem.at[at])
        for at, (here, far) in enumerate(zip(near, results))
    ]

    def mix():
        def one(at, carry):
            span = pl.ds(pl.multiple_of(at * 256, 256), 256)
            across = pl.ds(pl.multiple_of(3 * width + at * 256, 256), 256)
            inner_resid[:, span] = tokens[:, span].astype(jnp.float32) + product(
                attended[...], weight[:, across], 1, 0
            )
            return carry

        lax.fori_loop(0, width // 256, one, 0)
        for copy in copies:
            copy.start()

    items = [(mat, number) for mat in range(4) for number in range(1, chips)]
    events = [
        (at + SLACK * step, -step, functools.partial(relay, *item, step))
        for at, item in enumerate(items)
        for step in range(plan.levels + 1)
    ]
    ready = chips - 1 + SLACK * plan.levels
    for late, work in (
        (0, fetch_weight),
        (1, project),
        (2, functools.partial(attend, 0, pairs // 2)),
        (3, functools.partial(attend, pairs // 2, pairs)),
        (4, mix),
    ):
        events.append((ready + late, 1, work))
    for _, _, event in sorted(events, key=lambda event: event[:2]):
        event()

    for mat in range(1, 4):
        await_core(mat)
    for step in range(1, plan.shards):
        small_copy(step).wait_recv()
    for copy in sent:
        copy.wait_send()
    for mat in range(4):
        along(mat, lambda copy: copy.wait_send())
        for number in range(1, chips):
            on(mat, number, lambda copy: copy.wait_send())
    for copy in copies:
        copy.wait()


def gather_weights(plan, own, small, carried):
    hbm = pl.BlockSpec(memory_space=pl.ANY)
    vmem = pl.BlockSpec(memory_space=pltpu.VMEM)
    dma = pltpu.SemaphoreType.DMA
    shapes = [
        jax.ShapeDtypeStruct((array.shape[0] * plan.shards, array.shape[1]), array.dtype)
        for array in own
    ]
    gaps = plan.chips - 1
    crossing = plan.replicas - 1
    length, width = carried[0].shape
    wide, low = jnp.float32, jnp.bfloat16
    results = (
        [jax.ShapeDtypeStruct((length, width), low)] * 4
        + [
            jax.ShapeDtypeStruct((width // HD, length), wide),
            jax.ShapeDtypeStruct((length, width), wide),
        ]
        + [jax.ShapeDtypeStruct((length, LANES), wide)] * 3
    )
    return pl.pallas_call(
        functools.partial(gather_kernel, plan),
        out_shape=shapes + [jax.ShapeDtypeStruct((plan.shards,) + small.shape, small.dtype)]
        + results,
        in_specs=[hbm] * 4 + [vmem] + [hbm] * len(carried),
        out_specs=[hbm] * 4 + [vmem] + [hbm] * len(results),
        scratch_shapes=[pltpu.VMEM(array.shape, array.dtype) for array in own]
        + [
            dma((4,)),
            dma((4,)),
            dma((plan.shards - 1,)),
            dma((plan.shards - 1,)),
            dma((4, plan.chips, 2, plan.orders)),
            dma((4, plan.chips, plan.orders)),
            dma((4, gaps, plan.orders, crossing)),
            dma((4, gaps, plan.orders, crossing)),
            dma((4, plan.chips)),
            dma((4, plan.chips)),
        ]
        + [pltpu.VMEM(array.shape, array.dtype) for array in carried]
        + [pltpu.VMEM(result.shape, result.dtype) for result in results]
        + [
            pltpu.VMEM(shapes[0].shape, low),
            pltpu.VMEM((length, length), wide),
            dma((len(carried),)),
            dma,
            dma((len(results),)),
        ],
        compiler_params=pltpu.CompilerParams(
            collective_id=0, has_side_effects=True, vmem_limit_bytes=VMEM_LIMIT
        ),
        name="gather_weights",
    )(*own, small, *carried)


def back_pair(pair, query, key, value, upper, logsum, mask_bias, tables, joined_low, width):
    length = query.shape[0]
    block = min(length, 256)
    span = pl.ds(pl.multiple_of(pair * LANES, LANES), LANES)
    lane = lax.broadcasted_iota(jnp.int32, (1, LANES), 1)
    keys, values = key[:, span], value[:, span]
    query_parts = [0.0] * (length // block)
    key_total = value_total = 0.0
    for half in range(LANES // HD):
        pick = jnp.where(lane // HD == half, 1.0, 0.0).astype(jnp.bfloat16)
        scaled = pick * jnp.bfloat16(1.0 / math.sqrt(HD))
        keys_scaled = keys * scaled
        rowsum = logsum[pl.ds(pair * (LANES // HD) + half, 1), :]
        for at in range(length // block):
            rows = slice(at * block, (at + 1) * block)
            queries_scaled = query[rows, span] * scaled
            grads = upper[rows, span] * pick
            scores = product(keys, queries_scaled, 1, 1) + mask_bias[:, rows]
            probs = jnp.exp(scores - rowsum[:, rows])
            dprobs = product(values, grads, 1, 1)
            dots = jnp.sum(probs * dprobs, axis=0, keepdims=True)
            score_grad = (probs * (dprobs - dots)).astype(jnp.bfloat16)
            value_total += product(probs.astype(jnp.bfloat16), grads, 1, 0)
            key_total += product(score_grad, queries_scaled, 1, 0)
            query_parts[at] += product(score_grad, keys_scaled, 0, 0)
    cosine, before, after = tables

    def unrotate(grad, rows):
        return (
            grad * cosine[rows, :]
            - pltpu.roll(grad, LANES - HD // 2, 1) * before[rows, :]
            - pltpu.roll(grad, HD // 2, 1) * after[rows, :]
        ).astype(jnp.bfloat16)

    for at, part in enumerate(query_parts):
        rows = slice(at * block, (at + 1) * block)
        joined_low[rows, span] = unrotate(part, rows)
    everything = slice(0, length)
    joined_low[:, pl.ds(pl.multiple_of(width + pair * LANES, LANES), LANES)] = unrotate(
        key_total, everything
    )
    joined_low[:, pl.ds(pl.multiple_of(2 * width + pair * LANES, LANES), LANES)] = (
        value_total.astype(jnp.bfloat16)
    )


def sum_kernel(plan, *refs):
    mixing, gate, up, down, small = refs[:5]
    carried, weight = refs[5:17], refs[17]
    outs, small_out, input_grad = refs[18:22], refs[22], refs[23]
    (held, mate_in, rep_in, z_in, final, small_in, load_sem, out_sem, small_sem, mate_send,
     mate_recv, rep_send, rep_recv, z_send, z_recv, last_send, last_recv) = refs[24:41]
    here, weight_here = refs[41:53], refs[53]
    joined_low, joined, mask_bias, tokens_across, fetch_sem, result_sem = refs[54:60]
    result_here = refs[60]
    rep, shard = lax.axis_index("rep"), lax.axis_index("shard")
    chips, piece, levels = plan.chips, plan.piece, plan.levels
    place, core = lax.div(shard, 2), lax.rem(shard, 2)
    mate = place * 2 + (1 - core)
    rows = held.shape[2]
    total = plan.replicas * plan.shards
    early = 3 * chips
    count = 4 * chips
    (query, key, value, upper, logsum, segment_down, segment_across, cosine, before, after, tokens,
     inner_grad) = here
    width = query.shape[1]
    pairs = width // LANES

    def fragments(turn, slab):
        top = pl.multiple_of(slab * rows, 8)
        if turn == 3:
            wide = joined.shape[1]
            return [
                (joined.at[pl.ds(top, rows), :], 0, wide),
                (mixing.at[pl.ds(top, rows), :], wide, mixing.shape[1]),
            ]
        if turn > 0:
            return [((gate, up)[turn - 1].at[pl.ds(top, rows), :], 0, plan.width)]
        wide = down.shape[1]
        return [
            (
                down.at[
                    pl.ds(pl.multiple_of(slab * (rows * (plan.width // wide)) + at * rows, 8), rows),
                    :,
                ],
                at * wide,
                wide,
            )
            for at in range(plan.width // wide)
        ]

    gaps = list(range(1, chips)) + [0]

    def slab_at(gap, which):
        return lax.rem(place + gap, chips) * 2 + which

    def load(turn):
        for gap in gaps:
            for ref, left, wide in fragments(turn, slab_at(gap, core)):
                pltpu.make_async_copy(
                    ref, held.at[turn, gap, :, pl.ds(left, wide)], load_sem.at[turn, gap]
                ).start()

    def give(turn):
        for gap in gaps:
            for ref, left, wide in fragments(turn, slab_at(gap, 1 - core)):
                remote(
                    ref, mate_in.at[turn, gap, :, pl.ds(left, wide)],
                    mate_send.at[turn, gap], mate_recv.at[turn, gap], rep, mate,
                ).start()

    for turn in range(3):
        load(turn)
    fetches = [
        pltpu.make_async_copy(far, near, fetch_sem.at[at])
        for at, (far, near) in enumerate(zip(carried, here))
    ]
    fetches.append(
        pltpu.make_async_copy(
            weight.at[:, pl.ds(0, 3 * width)], weight_here, fetch_sem.at[len(carried)]
        )
    )
    for fetch in fetches:
        fetch.start()
    greet_all(plan, rep, shard)
    for turn in range(3):
        give(turn)

    def small_go(step, carry):
        other = lax.rem(rep * plan.shards + shard + step, total)
        other_rep, other_shard = lax.div(other, plan.shards), lax.rem(other, plan.shards)
        remote(
            small.at[other_shard], small_in.at[step - 1], small_sem.at[0], small_sem.at[1],
            other_rep, other_shard,
        ).start()
        return carry

    lax.fori_loop(1, total, small_go, 0)

    def whole_mate(turn, gap):
        return remote(
            mate_in.at[turn, gap], mate_in.at[turn, gap],
            mate_send.at[turn, gap], mate_recv.at[turn, gap], rep, mate,
        )

    def cross(turn, gap, order, step):
        far = plan.flip(rep, plan.ways[order][step])
        at = plan.halve_at(step)
        copies = [
            remote(
                held.at[turn, gap, :, pl.ds(plan.column(section, order), piece)],
                rep_in.at[turn, gap, order, at + number],
                rep_send.at[turn, gap, order, at + number],
                rep_recv.at[turn, gap, order, at + number],
                far, shard,
            )
            for number, section in enumerate(plan.halve(far, order, step))
        ]
        return copies, [plan.column(section, order) for section in plan.halve(rep, order, step)]

    wide_piece = plan.orders * piece
    own_columns = pl.ds(pl.multiple_of(rep * wide_piece, LANES), wide_piece)

    def z_copy(turn, gap):
        return remote(
            held.at[turn, gap, :, own_columns],
            z_in.at[turn, gap - 1],
            z_send.at[turn, gap - 1], z_recv.at[turn, gap - 1],
            rep, slab_at(gap, core),
        )

    def item_of(number):
        return lax.div(number, chips), lax.rem(lax.rem(number, chips) + 1, chips)

    def advance(number, step):
        turn, gap = item_of(number)
        if step == 0:
            pltpu.make_async_copy(
                held.at[turn, gap], held.at[turn, gap], load_sem.at[turn, gap]
            ).wait()
            whole_mate(turn, gap).wait_recv()

            def add(at, carry):
                span = pl.ds(pl.multiple_of(at * piece, LANES), piece)
                held[turn, gap, :, span] = (
                    held[turn, gap, :, span].astype(jnp.float32)
                    + mate_in[turn, gap, :, span].astype(jnp.float32)
                ).astype(jnp.bfloat16)
                return carry

            lax.fori_loop(0, plan.width // piece, add, 0)
        else:
            for order in range(plan.orders):
                copies, columns = cross(turn, gap, order, step - 1)
                at = plan.halve_at(step - 1)
                for index, (copy, column) in enumerate(zip(copies, columns)):
                    copy.wait_recv()
                    span = pl.ds(column, piece)
                    held[turn, gap, :, span] = (
                        held[turn, gap, :, span].astype(jnp.float32)
                        + rep_in[turn, gap, order, at + index].astype(jnp.float32)
                    ).astype(jnp.bfloat16)
        if step < levels:
            for order in range(plan.orders):
                for copy in cross(turn, gap, order, step)[0]:
                    copy.start()
        else:
            @pl.when(gap > 0)
            def _():
                z_copy(turn, gap).start()

    def spread(turn, order, step):
        far = plan.flip(rep, plan.ways[order][step])
        at = plan.grow_at(step)
        return [
            remote(
                final.at[turn, :, pl.ds(plan.column(section, order), piece)],
                final.at[turn, :, pl.ds(plan.column(section, order), piece)],
                last_send.at[turn, order, at + number],
                last_recv.at[turn, order, at + number],
                far, shard,
            )
            for number, section in enumerate(plan.grow(rep, order, step))
        ]

    def await_spread(turn, order, step):
        far = plan.flip(rep, plan.ways[order][step])
        at = plan.grow_at(step)
        for number, section in enumerate(plan.grow(far, order, step)):
            there = final.at[turn, :, pl.ds(plan.column(section, order), piece)]
            remote(
                there, there,
                last_send.at[turn, order, at + number],
                last_recv.at[turn, order, at + number],
                far, shard,
            ).wait_recv()

    def finish(turn, step):
        if step == 0:
            for gap in range(1, chips):
                z_copy(turn, gap).wait_recv()
            for order in range(plan.orders):
                span = pl.ds(plan.column(rep, order), piece)
                part = pl.ds(order * piece, piece)
                value = held[turn, 0, :, span].astype(jnp.float32)
                for gap in range(1, chips):
                    value = value + z_in[turn, gap - 1, :, part].astype(jnp.float32)
                final[turn, :, span] = value.astype(jnp.bfloat16)
        else:
            for order in range(plan.orders):
                await_spread(turn, order, step - 1)
        if step < levels:
            for order in range(plan.orders):
                for copy in spread(turn, order, step):
                    copy.start()

    def tick(now):
        for step in reversed(range(levels + 1)):
            late = now - (SLACK * (levels + step + 1) + chips - 1)

            @pl.when((late >= 0) & (lax.rem(late + chips, chips) == 0) & (late < count))
            def _(late=late, step=step):
                finish(lax.div(late, chips), step)

        for step in reversed(range(levels + 1)):
            number = now - SLACK * step

            @pl.when((number >= 0) & (number < count))
            def _(number=number, step=step):
                advance(number, step)

    tick(0)
    for fetch in fetches:
        fetch.wait()
    mask_bias[...] = jnp.where(segment_down[:, 0:1] == segment_across[0:1, :], 0.0, NEG_LARGE)

    def attend(now, carry):
        @pl.when(now < pairs)
        def _():
            back_pair(
                now, query, key, value, upper, logsum, mask_bias, (cosine, before, after),
                joined_low, width,
            )

        @pl.when(now + 1 < early)
        def _():
            tick(now + 1)
        return carry

    lax.fori_loop(0, max(pairs, early - 1), attend, 0)
    tokens_across[...] = tokens[...].T

    def weigh(at, carry):
        span = pl.ds(pl.multiple_of(at * (width // 2), LANES), width // 2)
        joined[:, span] = product(tokens_across[...], joined_low[:, span], 1, 0).astype(
            jnp.bfloat16
        )
        return carry

    lax.fori_loop(0, 6, weigh, 0)
    load(3)
    give(3)

    def back(at, carry):
        low = pl.ds(pl.multiple_of(at * 256, 256), 256)
        result_here[:, low] = (
            inner_grad[:, low] + product(joined_low[...], weight_here[low, :], 1, 1)
        ).astype(jnp.bfloat16)
        return carry

    lax.fori_loop(0, width // 256, back, 0)
    result_copy = pltpu.make_async_copy(result_here, input_grad, result_sem)
    result_copy.start()

    def late_tick(now, carry):
        tick(now)
        return carry

    lax.fori_loop(early, count + SLACK * (2 * levels + 1), late_tick, 0)

    everything = remote(small_in, small_in, small_sem.at[0], small_sem.at[1], rep, mate)
    everything.wait_recv()

    def gain(at, value):
        return value + small_in[at]

    small_out[...] = lax.fori_loop(0, total - 1, gain, small[shard])
    everything.wait_send()
    for turn in range(4):
        pltpu.make_async_copy(final.at[turn], outs[turn], out_sem.at[turn]).start()

    def drain(number, carry):
        turn, gap = item_of(number)
        whole_mate(turn, gap).wait_send()
        for order in range(plan.orders):
            for step in range(levels):
                for copy in cross(turn, gap, order, step)[0]:
                    copy.wait_send()

        @pl.when(gap > 0)
        def _():
            z_copy(turn, gap).wait_send()
        return carry

    lax.fori_loop(0, count, drain, 0)
    for turn in range(4):
        for order in range(plan.orders):
            for step in range(levels):
                for copy in spread(turn, order, step):
                    copy.wait_send()
        pltpu.make_async_copy(final.at[turn], outs[turn], out_sem.at[turn]).wait()
    result_copy.wait()


def sum_grads(plan, grads, small, carried, weight):
    hbm = pl.BlockSpec(memory_space=pl.ANY)
    vmem = pl.BlockSpec(memory_space=pltpu.VMEM)
    dma = pltpu.SemaphoreType.DMA
    chips, gaps, crossing = plan.chips, plan.chips - 1, plan.replicas - 1
    rows = grads[0].shape[0] // plan.shards
    low = jnp.bfloat16
    total = plan.replicas * plan.shards
    length, width = carried[0].shape
    return pl.pallas_call(
        functools.partial(sum_kernel, plan),
        out_shape=[jax.ShapeDtypeStruct((rows, plan.width), low)] * 4
        + [
            jax.ShapeDtypeStruct(small.shape[1:], small.dtype),
            jax.ShapeDtypeStruct((length, width), low),
        ],
        in_specs=[hbm] * 4 + [vmem] + [hbm] * (len(carried) + 1),
        out_specs=[hbm] * 4 + [vmem, hbm],
        scratch_shapes=[
            pltpu.VMEM((4, chips, rows, plan.width), low),
            pltpu.VMEM((4, chips, rows, plan.width), low),
            pltpu.VMEM((4, chips, plan.orders, crossing, rows, plan.piece), low),
            pltpu.VMEM((4, gaps, rows, plan.orders * plan.piece), low),
            pltpu.VMEM((4, rows, plan.width), low),
            pltpu.VMEM((total - 1,) + small.shape[1:], small.dtype),
            dma((4, chips)),
            dma((4,)),
            dma((2,)),
            dma((4, chips)),
            dma((4, chips)),
            dma((4, chips, plan.orders, crossing)),
            dma((4, chips, plan.orders, crossing)),
            dma((4, gaps)),
            dma((4, gaps)),
            dma((4, plan.orders, crossing)),
            dma((4, plan.orders, crossing)),
        ]
        + [pltpu.VMEM(array.shape, array.dtype) for array in carried]
        + [
            pltpu.VMEM((width, 3 * width), low),
            pltpu.VMEM((length, 3 * width), low),
            pltpu.VMEM((width, 3 * width), low),
            pltpu.VMEM((length, length), jnp.float32),
            pltpu.VMEM((width, length), low),
            dma((len(carried) + 1,)),
            dma,
            pltpu.VMEM((length, width), low),
        ],
        compiler_params=pltpu.CompilerParams(
            collective_id=1, has_side_effects=True, vmem_limit_bytes=VMEM_LIMIT
        ),
        name="sum_grads",
    )(*grads, small, *carried, weight)


def layer_norm(values, gain, shift):
    centred = values - jnp.mean(values, axis=-1, keepdims=True)
    variance = jnp.mean(centred * centred, axis=-1, keepdims=True)
    return centred * lax.rsqrt(variance + EPSILON) * gain + shift


def transposed_product(left, right):
    return lax.dot_general(
        left, right, (((1,), (1,)), ((), ())), preferred_element_type=jnp.float32
    )


def token_contract(left, right):
    return lax.dot_general(
        left, right, (((0,), (0,)), ((), ())), preferred_element_type=jnp.float32
    )


def on_device(
    tokens,
    joined_weight,
    mixing_weight,
    gate_weight,
    up_weight,
    down_weight,
    inner_gain,
    inner_shift,
    outer_gain,
    outer_shift,
    segments,
    positions,
    cotangent,
):
    replicas, shards = lax.axis_size("rep"), lax.axis_size("shard")
    plan = Plan(gate_weight.shape[1], replicas, shards)
    part_rows = joined_weight.shape[0]
    own_vectors = jnp.stack([inner_gain, inner_shift, outer_gain, outer_shift]).astype(jnp.float32)
    own_vectors = jnp.pad(own_vectors, ((0, 4), (0, LANES - part_rows)))
    length, model_width = tokens.shape
    halves = np.arange(LANES) % (HD // 2)
    rates = np.float32(1000.0) ** (-(2.0 * halves.astype(np.float32)) / np.float32(HD))
    marks = jnp.where(
        jnp.arange(LANES)[None, :] == 0, segments[0][:, None], positions[0][:, None]
    )
    (
        attention_full,
        gate_full,
        upward_full,
        down_full,
        vectors,
        query_low,
        key_low,
        value_low,
        attended_low,
        logsum,
        inner_resid,
        cosine_wide,
        before,
        after,
    ) = gather_weights(
        plan,
        (
            jnp.concatenate([joined_weight, mixing_weight], axis=1),
            gate_weight,
            up_weight,
            down_weight,
        ),
        own_vectors,
        (tokens, marks, segments, jnp.asarray(np.tile(rates[None, :], (8, 1)))),
    )
    mixing_full = attention_full[:, joined_weight.shape[1] :]
    vectors = vectors[:, :4, :part_rows].transpose(1, 0, 2).reshape(4, shards * part_rows)
    innergain_full, innershift_full, outergain_full, outershift_full = vectors
    normed, inner_pull = jax.vjp(
        layer_norm,
        inner_resid,
        innergain_full.astype(jnp.float32),
        innershift_full.astype(jnp.float32),
    )
    normed_low = normed.astype(jnp.bfloat16)
    gate_rows = jnp.dot(normed_low, gate_full, preferred_element_type=jnp.float32)
    upward = jnp.dot(normed_low, upward_full, preferred_element_type=jnp.float32)
    active, silu_pull = jax.vjp(
        lambda first, second: jax.nn.silu(first) * second, gate_rows, upward
    )
    active_low = active.astype(jnp.bfloat16)
    result = jnp.dot(active_low, down_full, preferred_element_type=jnp.float32)
    final, outer_pull = jax.vjp(
        layer_norm,
        normed + result,
        outergain_full.astype(jnp.float32),
        outershift_full.astype(jnp.float32),
    )
    layer_output = final.astype(jnp.bfloat16)
    gate_back, upward_back, down_back = gate_full, upward_full, down_full
    outer_grad, outergain_grad, outershift_grad = outer_pull(cotangent.astype(jnp.float32))
    result_grad = outer_grad.astype(jnp.bfloat16)
    down_grad = token_contract(active_low, result_grad)
    active_grad = transposed_product(result_grad, down_back)
    gate_part, upward_part = silu_pull(active_grad)
    gate_low = gate_part.astype(jnp.bfloat16)
    upward_low = upward_part.astype(jnp.bfloat16)
    gate_grad = token_contract(normed_low, gate_low)
    up_grad = token_contract(normed_low, upward_low)
    normed_grad = (
        outer_grad
        + transposed_product(gate_low, gate_back)
        + transposed_product(upward_low, upward_back)
    )
    inner_grad, innergain_grad, innershift_grad = inner_pull(normed_grad)
    mixing_back = mixing_full
    branch_grad = inner_grad.astype(jnp.bfloat16)
    mixing_grad = token_contract(attended_low, branch_grad)
    attended_grad = transposed_product(branch_grad, mixing_back).astype(jnp.bfloat16)

    small = jnp.stack([innergain_grad, innershift_grad, outergain_grad, outershift_grad])
    small = small.reshape(4, shards, part_rows).transpose(1, 0, 2)
    small = jnp.pad(small, ((0, 0), (0, 4), (0, LANES - part_rows)))
    low = jnp.bfloat16
    down_sum, gate_sum, up_sum, attention_sum, small_sum, input_grad = sum_grads(
        plan,
        (mixing_grad.astype(low), gate_grad.astype(low), up_grad.astype(low), down_grad.astype(low)),
        small,
        (
            query_low,
            key_low,
            value_low,
            attended_grad,
            logsum,
            marks,
            segments,
            cosine_wide,
            before,
            after,
            tokens,
            inner_grad,
        ),
        attention_full,
    )
    down_sum = down_sum.reshape(part_rows, -1, model_width).transpose(1, 0, 2)
    full = jnp.float32
    return (
        layer_output,
        input_grad,
        attention_sum[:, : joined_weight.shape[1]].astype(full),
        attention_sum[:, joined_weight.shape[1] :].astype(full),
        gate_sum.astype(full),
        up_sum.astype(full),
        down_sum.reshape(down_weight.shape).astype(full),
        small_sum[0, :part_rows],
        small_sum[1, :part_rows],
        small_sum[2, :part_rows],
        small_sum[3, :part_rows],
    )


def solution(mesh):
    placed = (
        P(("rep", "shard"), None),
        P("shard", None),
        P("shard", None),
        P("shard", None),
        P("shard", None),
        P("shard", None),
        P("shard"),
        P("shard"),
        P("shard"),
        P("shard"),
        P(("rep", "shard"), None),
        P(("rep", "shard"), None),
        P(("rep", "shard"), None),
    )
    return jax.shard_map(
        on_device,
        mesh=mesh,
        in_specs=placed,
        out_specs=(
            P(("rep", "shard"), None),
            P(("rep", "shard"), None),
            P("shard", None),
            P("shard", None),
            P("shard", None),
            P("shard", None),
            P("shard", None),
            P("shard"),
            P("shard"),
            P("shard"),
            P("shard"),
        ),
        check_vma=False,
    )
```

```python
import functools
import math

import jax
import jax.numpy as jnp
import numpy as np
from jax import lax
from jax.experimental import pallas as pl
from jax.experimental.pallas import tpu as pltpu
from jax.sharding import PartitionSpec as P

H = 12
HD = 64

EPSILON = 1e-12
NEG_LARGE = -1e30
LANES = 128
MESH = pl.DeviceIdType.MESH
VMEM_LIMIT = 62 * 1024 * 1024
SLACK = 2
VMEM_MOST = 67043328
AHEAD = 3


class Plan:
    def __init__(self, width, replicas, shards):
        self.replicas, self.shards = replicas, shards
        self.chips = shards // 2
        self.levels = replicas.bit_length() - 1
        self.orders = 2 if self.levels > 1 and width % (2 * replicas * LANES) == 0 else 1
        self.ways = (tuple(range(self.levels)), tuple(reversed(range(self.levels))))[: self.orders]
        self.piece = width // (replicas * self.orders)
        self.width = width

    def flip(self, rep, bit):
        return rep + (1 << bit) * (1 - 2 * lax.rem(lax.div(rep, 1 << bit), 2))

    def with_bits(self, rep, bits, number):
        for at, bit in enumerate(bits):
            had = lax.rem(lax.div(rep, 1 << bit), 2)
            rep = rep + (1 << bit) * (((number >> at) & 1) - had)
        return rep

    def column(self, rep, order):
        return pl.multiple_of((rep * self.orders + order) * self.piece, LANES)

    def grow(self, rep, order, step):
        bits = self.ways[order][:step]
        return [self.with_bits(rep, bits, number) for number in range(1 << step)]

    def grow_at(self, step):
        return (1 << step) - 1

    def halve(self, rep, order, step):
        bits = self.ways[order][step + 1 :]
        return [self.with_bits(rep, bits, number) for number in range(1 << len(bits))]

    def halve_at(self, step):
        return sum(1 << (self.levels - 1 - at) for at in range(step))


def peer(rep, shard):
    return {"rep": rep, "shard": shard}


def remote(src, dst, send, recv, rep, shard):
    return pltpu.make_async_remote_copy(
        src_ref=src,
        dst_ref=dst,
        send_sem=send,
        recv_sem=recv,
        device_id=peer(rep, shard),
        device_id_type=MESH,
    )


def greet_all(plan, rep, shard):
    barrier = pltpu.get_barrier_semaphore()
    total = plan.replicas * plan.shards

    def hello(step, carry):
        other = lax.rem(rep * plan.shards + shard + step, total)
        pl.semaphore_signal(
            barrier,
            inc=1,
            device_id=peer(lax.div(other, plan.shards), lax.rem(other, plan.shards)),
            device_id_type=MESH,
        )
        return carry

    lax.fori_loop(1, total, hello, 0)
    pl.semaphore_wait(barrier, total - 1)


def greet_near(plan, rep, shard):
    barrier = pltpu.get_barrier_semaphore()
    for step in range(1, plan.shards):
        pl.semaphore_signal(
            barrier,
            inc=1,
            device_id=peer(rep, lax.rem(shard + step, plan.shards)),
            device_id_type=MESH,
        )
    for bit in range(plan.levels):
        pl.semaphore_signal(
            barrier, inc=1, device_id=peer(plan.flip(rep, bit), shard), device_id_type=MESH
        )
    pl.semaphore_wait(barrier, plan.shards - 1 + plan.levels)


def product(left, right, left_axis, right_axis):
    return lax.dot_general(
        left, right, (((left_axis,), (right_axis,)), ((), ())), preferred_element_type=jnp.float32
    )


def forward_pair(pair, query, key, value, mask_bias, attended, logsum):
    length = query.shape[0]
    block = min(length, 256)
    span = pl.ds(pl.multiple_of(pair * LANES, LANES), LANES)
    lane = lax.broadcasted_iota(jnp.int32, (1, LANES), 1)
    keys, values = key[:, span], value[:, span]
    parts = [0.0] * (length // block)
    for half in range(LANES // HD):
        pick = jnp.where(lane // HD == half, 1.0, 0.0).astype(jnp.bfloat16)
        scaled = pick * jnp.bfloat16(1.0 / math.sqrt(HD))
        picked = values * pick
        for at in range(length // block):
            rows = slice(at * block, (at + 1) * block)
            scores = product(keys, query[rows, span] * scaled, 1, 1) + mask_bias[:, rows]
            highest = jnp.max(scores, axis=0, keepdims=True)
            shifted = jnp.exp(scores - highest)
            denominator = jnp.sum(shifted, axis=0, keepdims=True)
            logsum[pl.ds(pair * (LANES // HD) + half, 1), rows] = highest + jnp.log(denominator)
            probs = (shifted * (1.0 / denominator)).astype(jnp.bfloat16)
            parts[at] += product(probs, picked, 0, 0)
    for at, part in enumerate(parts):
        attended[at * block : (at + 1) * block, span] = part.astype(jnp.bfloat16)


def gather_kernel(plan, *refs):
    own, small = refs[:4], refs[4]
    carried = refs[5:9]
    full, small_all = refs[9:13], refs[13]
    results = refs[14:23]
    stages = refs[23:27]
    (load_sem, store_sem, small_send, small_recv, z_send, z_recv, rep_send, rep_recv, core_send,
     core_recv) = refs[27:37]
    tokens, marks, segment_across, rates = refs[37:41]
    near = refs[41:50]
    query, key, value, attended, logsum, inner_resid, cosine, before, after = near
    weight, mask_bias, fetch_sem, weight_sem, result_sem = refs[50:55]
    rep, shard = lax.axis_index("rep"), lax.axis_index("shard")
    chips, piece = plan.chips, plan.piece
    place, core = lax.div(shard, 2), lax.rem(shard, 2)
    mate = place * 2 + (1 - core)
    rows = own[0].shape[0]
    length, width = tokens.shape
    pairs = width // LANES

    def part(ref, mat, top, section_rep, order):
        if mat < 3:
            return ref.at[
                pl.ds(pl.multiple_of(top, 8), rows),
                pl.ds(plan.column(section_rep, order), piece),
            ]
        per = own[3].shape[1] // piece
        section = section_rep * plan.orders + order
        return ref.at[
            pl.ds(pl.multiple_of(top + lax.div(section, per) * rows, 8), rows),
            pl.ds(pl.multiple_of(lax.rem(section, per) * piece, LANES), piece),
        ]

    def slab_part(mat, slab, section_rep, order):
        return part(full[mat], mat, slab * own[mat].shape[0], section_rep, order)

    def slab_of(mat, slab):
        deep = own[mat].shape[0]
        return full[mat].at[pl.ds(pl.multiple_of(slab * deep, 8), deep), :]

    sent = []

    def launch(copy):
        copy.start()
        sent.append(copy)

    loads = [pltpu.make_async_copy(own[mat], stages[mat], load_sem.at[mat]) for mat in range(4)]
    for load in loads:
        load.start()
    fetches = [
        pltpu.make_async_copy(far, here, fetch_sem.at[at])
        for at, (far, here) in enumerate(zip(carried, (tokens, marks, segment_across, rates)))
    ]
    for fetch in fetches:
        fetch.start()
    small_all[shard] = small[...]
    greet_near(plan, rep, shard)

    def small_copy(step):
        return remote(
            small, small_all.at[shard], small_send.at[step - 1], small_recv.at[step - 1],
            rep, lax.rem(shard + step, plan.shards),
        )

    fewest = jnp.minimum(place, chips - 1 - place)
    longer_above = jnp.where(2 * place < chips - 1, 1, 0)

    def nearest(number):
        inside = number <= 2 * fewest
        above = jnp.where(inside, number % 2, longer_above)
        distance = jnp.where(inside, (number + 1) // 2, number - fewest)
        return place + distance * (2 * above - 1), above

    def hop(mat, origin, down, order, source):
        return remote(
            source,
            slab_part(mat, origin * 2 + core, rep, order),
            z_send.at[mat, origin, down, order],
            z_recv.at[mat, origin, order],
            rep, (place + 1 - 2 * down) * 2 + core,
        )

    def own_hop(mat, down, order):
        return hop(mat, place, down, order, part(own[mat], mat, 0, rep, order))

    def next_hop(mat, number, order):
        origin, above = nearest(number)
        there = slab_part(mat, origin * 2 + core, rep, order)
        return hop(mat, origin, above, order, there)

    def leads(down):
        return (place > 0) if down else (place < chips - 1)

    def goes_on(number):
        _, above = nearest(number)
        onward = place + 1 - 2 * above
        return (onward >= 0) & (onward < chips)

    def along(mat, act):
        for down in range(2):
            @pl.when(leads(down))
            def _(down=down):
                for order in range(plan.orders):
                    act(own_hop(mat, down, order))

    def on(mat, number, act):
        @pl.when(goes_on(number))
        def _():
            for order in range(plan.orders):
                act(next_hop(mat, number, order))

    def give(mat):
        launch(remote(
            own[mat], slab_of(mat, shard), core_send.at[mat, 0], core_recv.at[mat, 0], rep, mate
        ))

    for mat in range(2):
        along(mat, lambda copy: copy.start())
    give(0)
    for step in range(1, plan.shards):
        launch(small_copy(step))
    for mat in range(1, 4):
        give(mat)
    stores = []
    for mat in range(4):
        loads[mat].wait()
        store = pltpu.make_async_copy(stages[mat], slab_of(mat, shard), store_sem.at[mat])
        store.start()
        stores.append(store)

    for fetch in fetches:
        fetch.wait()
    mask_bias[...] = jnp.where(marks[:, 0:1] == segment_across[0:1, :], 0.0, NEG_LARGE)
    angles = marks[:, 1:2].astype(jnp.float32) * rates[0:1, :]
    first = lax.broadcasted_iota(jnp.int32, (1, LANES), 1) % HD < HD // 2
    cosine[...] = jnp.cos(angles)
    sine = jnp.sin(angles)
    before[...] = jnp.where(first, -sine, 0.0)
    after[...] = jnp.where(first, 0.0, sine)

    def source(number):
        return nearest(number)[0] * 2 + core

    def exchange(mat, number, order, step):
        slab = source(number)
        far = plan.flip(rep, plan.ways[order][step])
        at = plan.grow_at(step)
        return [
            remote(
                slab_part(mat, slab, section, order),
                slab_part(mat, slab, section, order),
                rep_send.at[mat, number - 1, order, at + index],
                rep_recv.at[mat, number - 1, order, at + index],
                far, shard,
            )
            for index, section in enumerate(plan.grow(rep, order, step))
        ]

    def await_exchange(mat, number, order, step):
        slab = source(number)
        far = plan.flip(rep, plan.ways[order][step])
        at = plan.grow_at(step)
        for index, section in enumerate(plan.grow(far, order, step)):
            there = slab_part(mat, slab, section, order)
            remote(
                there, there,
                rep_send.at[mat, number - 1, order, at + index],
                rep_recv.at[mat, number - 1, order, at + index],
                far, shard,
            ).wait_recv()

    def relay(mat, number, step):
        for order in range(plan.orders):
            if step == 0:
                origin, _ = nearest(number)
                there = slab_part(mat, origin * 2 + core, rep, order)
                remote(
                    there, there, z_send.at[mat, origin, 0, order], z_recv.at[mat, origin, order],
                    rep, mate,
                ).wait_recv()
            else:
                await_exchange(mat, number, order, step - 1)
            if step < plan.levels:
                for copy in exchange(mat, number, order, step):
                    launch(copy)
        if step == 0:
            on(mat, number, lambda copy: copy.start())
            if number == 1 and mat + 2 < 4:
                along(mat + 2, lambda copy: copy.start())
        if step == plan.levels:
            there = slab_of(mat, source(number))
            launch(remote(
                there, there, core_send.at[mat, number], core_recv.at[mat, number], rep, mate
            ))

    def await_core(mat):
        stores[mat].wait()
        for number in range(chips):
            slab = (place if number == 0 else nearest(number)[0]) * 2 + (1 - core)
            there = slab_of(mat, slab)
            remote(
                there, there, core_send.at[mat, number], core_recv.at[mat, number], rep, mate
            ).wait_recv()

    weight_load = pltpu.make_async_copy(full[0], weight, weight_sem)

    def fetch_weight():
        await_core(0)
        weight_load.start()

    def project():
        weight_load.wait()
        tile = width // 2

        def columns(at):
            span = pl.ds(pl.multiple_of(at * tile, LANES), tile)
            return product(tokens[...], weight[:, span], 1, 0)

        def turned(at, carry):
            joined = columns(at)
            for down in range(tile // LANES):
                vector = joined[:, down * LANES : (down + 1) * LANES]
                spot = pl.ds(pl.multiple_of(lax.rem(at, 2) * tile + down * LANES, LANES), LANES)
                low = (
                    vector * cosine[...]
                    + pltpu.roll(vector, LANES - HD // 2, 1) * before[...]
                    + pltpu.roll(vector, HD // 2, 1) * after[...]
                ).astype(jnp.bfloat16)

                @pl.when(at < 2)
                def _():
                    query[:, spot] = low

                @pl.when(at >= 2)
                def _():
                    key[:, spot] = low
            return carry

        lax.fori_loop(0, 4, turned, 0)

        def plain(at, carry):
            value[:, pl.ds(pl.multiple_of(at * tile, LANES), tile)] = columns(at + 4).astype(
                jnp.bfloat16
            )
            return carry

        lax.fori_loop(0, 2, plain, 0)

    def attend(low, high):
        def one(pair, carry):
            forward_pair(pair, query, key, value, mask_bias, attended, logsum)
            return carry

        lax.fori_loop(low, high, one, 0)

    copies = [
        pltpu.make_async_copy(here, far, result_sem.at[at])
        for at, (here, far) in enumerate(zip(near, results))
    ]

    def mix():
        def one(at, carry):
            span = pl.ds(pl.multiple_of(at * 256, 256), 256)
            across = pl.ds(pl.multiple_of(3 * width + at * 256, 256), 256)
            inner_resid[:, span] = tokens[:, span].astype(jnp.float32) + product(
                attended[...], weight[:, across], 1, 0
            )
            return carry

        lax.fori_loop(0, width // 256, one, 0)
        for copy in copies:
            copy.start()

    items = [(mat, number) for mat in range(4) for number in range(1, chips)]
    events = [
        (at + SLACK * step, -step, functools.partial(relay, *item, step))
        for at, item in enumerate(items)
        for step in range(plan.levels + 1)
    ]
    ready = chips - 1 + SLACK * plan.levels
    for late, work in (
        (0, fetch_weight),
        (1, project),
        (2, functools.partial(attend, 0, pairs // 2)),
        (3, functools.partial(attend, pairs // 2, pairs)),
        (4, mix),
    ):
        events.append((ready + late, 1, work))
    for _, _, event in sorted(events, key=lambda event: event[:2]):
        event()

    for mat in range(1, 4):
        await_core(mat)
    for step in range(1, plan.shards):
        small_copy(step).wait_recv()
    for copy in sent:
        copy.wait_send()
    for mat in range(4):
        along(mat, lambda copy: copy.wait_send())
        for number in range(1, chips):
            on(mat, number, lambda copy: copy.wait_send())
    for copy in copies:
        copy.wait()


def gather_weights(plan, own, small, carried):
    hbm = pl.BlockSpec(memory_space=pl.ANY)
    vmem = pl.BlockSpec(memory_space=pltpu.VMEM)
    dma = pltpu.SemaphoreType.DMA
    shapes = [
        jax.ShapeDtypeStruct((array.shape[0] * plan.shards, array.shape[1]), array.dtype)
        for array in own
    ]
    gaps = plan.chips - 1
    crossing = plan.replicas - 1
    length, width = carried[0].shape
    wide, low = jnp.float32, jnp.bfloat16
    results = (
        [jax.ShapeDtypeStruct((length, width), low)] * 4
        + [
            jax.ShapeDtypeStruct((width // HD, length), wide),
            jax.ShapeDtypeStruct((length, width), wide),
        ]
        + [jax.ShapeDtypeStruct((length, LANES), wide)] * 3
    )
    return pl.pallas_call(
        functools.partial(gather_kernel, plan),
        out_shape=shapes + [jax.ShapeDtypeStruct((plan.shards,) + small.shape, small.dtype)]
        + results,
        in_specs=[hbm] * 4 + [vmem] + [hbm] * len(carried),
        out_specs=[hbm] * 4 + [vmem] + [hbm] * len(results),
        scratch_shapes=[pltpu.VMEM(array.shape, array.dtype) for array in own]
        + [
            dma((4,)),
            dma((4,)),
            dma((plan.shards - 1,)),
            dma((plan.shards - 1,)),
            dma((4, plan.chips, 2, plan.orders)),
            dma((4, plan.chips, plan.orders)),
            dma((4, gaps, plan.orders, crossing)),
            dma((4, gaps, plan.orders, crossing)),
            dma((4, plan.chips)),
            dma((4, plan.chips)),
        ]
        + [pltpu.VMEM(array.shape, array.dtype) for array in carried]
        + [pltpu.VMEM(result.shape, result.dtype) for result in results]
        + [
            pltpu.VMEM(shapes[0].shape, low),
            pltpu.VMEM((length, length), wide),
            dma((len(carried),)),
            dma,
            dma((len(results),)),
        ],
        compiler_params=pltpu.CompilerParams(
            collective_id=0, has_side_effects=True, vmem_limit_bytes=VMEM_LIMIT
        ),
        name="gather_weights",
    )(*own, small, *carried)


def back_pair(pair, query, key, value, upper, logsum, mask_bias, tables, joined_low, width):
    length = query.shape[0]
    block = min(length, 256)
    span = pl.ds(pl.multiple_of(pair * LANES, LANES), LANES)
    lane = lax.broadcasted_iota(jnp.int32, (1, LANES), 1)
    keys, values = key[:, span], value[:, span]
    query_parts = [0.0] * (length // block)
    key_total = value_total = 0.0
    for half in range(LANES // HD):
        pick = jnp.where(lane // HD == half, 1.0, 0.0).astype(jnp.bfloat16)
        scaled = pick * jnp.bfloat16(1.0 / math.sqrt(HD))
        keys_scaled = keys * scaled
        rowsum = logsum[pl.ds(pair * (LANES // HD) + half, 1), :]
        for at in range(length // block):
            rows = slice(at * block, (at + 1) * block)
            queries_scaled = query[rows, span] * scaled
            grads = upper[rows, span] * pick
            scores = product(keys, queries_scaled, 1, 1) + mask_bias[:, rows]
            probs = jnp.exp(scores - rowsum[:, rows])
            dprobs = product(values, grads, 1, 1)
            dots = jnp.sum(probs * dprobs, axis=0, keepdims=True)
            score_grad = (probs * (dprobs - dots)).astype(jnp.bfloat16)
            value_total += product(probs.astype(jnp.bfloat16), grads, 1, 0)
            key_total += product(score_grad, queries_scaled, 1, 0)
            query_parts[at] += product(score_grad, keys_scaled, 0, 0)
    cosine, before, after = tables

    def unrotate(grad, rows):
        return (
            grad * cosine[rows, :]
            - pltpu.roll(grad, LANES - HD // 2, 1) * before[rows, :]
            - pltpu.roll(grad, HD // 2, 1) * after[rows, :]
        ).astype(jnp.bfloat16)

    for at, part in enumerate(query_parts):
        rows = slice(at * block, (at + 1) * block)
        joined_low[rows, span] = unrotate(part, rows)
    everything = slice(0, length)
    joined_low[:, pl.ds(pl.multiple_of(width + pair * LANES, LANES), LANES)] = unrotate(
        key_total, everything
    )
    joined_low[:, pl.ds(pl.multiple_of(2 * width + pair * LANES, LANES), LANES)] = (
        value_total.astype(jnp.bfloat16)
    )


def sum_kernel(plan, *refs):
    (gate_far, up_far, active_far, gate_weight, up_weight, down_weight, attention) = refs[:7]
    carried = refs[7:23]
    outs, small_out, input_grad = refs[23:27], refs[27], refs[28]
    (pool, mate_in, rep_in, z_in, final, small_in, out_sem, small_sem, mate_send, mate_recv,
     rep_send, rep_recv, z_send, z_recv, last_send, last_recv) = refs[29:45]
    here = refs[45:61]
    (weight, joined_low, mask_bias, across, branch, upper, small, gate_low, upward_low, active,
     fetch_sem, tile_sem, weight_sem, result_sem) = refs[61:]
    (query, key, value, attended, logsum, marks, segment_across, cosine, before, after, tokens,
     inner_resid, grad, result_grad, normed_low, sums) = here
    rep, shard = lax.axis_index("rep"), lax.axis_index("shard")
    chips, piece, levels = plan.chips, plan.piece, plan.levels
    place, core = lax.div(shard, 2), lax.rem(shard, 2)
    mate = place * 2 + (1 - core)
    rows = pool.shape[2]
    total = plan.replicas * plan.shards
    early = 3 * chips
    count = 4 * chips
    length, width = query.shape
    pairs = width // LANES
    groups = plan.width // width
    tile = width // 2
    low_type, wide_type = jnp.bfloat16, jnp.float32
    gaps = list(range(1, chips)) + [0]
    held = pool

    def slab_at(gap, which):
        return lax.rem(place + gap, chips) * 2 + which

    def stage(turn):
        return 4 + turn % 3

    def scatter(turn, slab, span, block):
        gap = lax.rem(lax.div(slab, 2) - place + chips, chips)
        other = lax.rem(slab + core, 2)
        pool[turn + other * (stage(turn) - turn), gap, :, span] = block.astype(low_type)

    def give(turn, gap):
        remote(
            pool.at[stage(turn), gap], mate_in.at[turn, gap],
            mate_send.at[turn, gap], mate_recv.at[turn, gap], rep, mate,
        ).start()

    fetches = [
        pltpu.make_async_copy(far, near, fetch_sem.at[at])
        for at, (far, near) in enumerate(zip(carried, here))
    ]
    late = fetches[:11]
    soon = fetches[11:]
    for fetch in soon + late:
        fetch.start()

    quarter = max(chips // groups, 1)
    home = lax.rem(lax.div(place, quarter), groups)

    def tile_start(at):
        group = lax.rem(home + 1 + lax.div(at, 2), groups)
        return group * width + lax.rem(at, 2) * tile

    def slot_columns(left, slot):
        return pl.ds(pl.multiple_of(left + slot * tile, LANES), tile)

    def slot_rows(slot):
        return pl.ds(pl.multiple_of(slot * tile, LANES), tile)

    tail = pl.ds(4 * tile, width)

    def tile_copies(at):
        slot = lax.rem(at, 2)
        span = pl.ds(pl.multiple_of(tile_start(at), LANES), tile)
        pairs_of = (
            (gate_far.at[:, span], gate_low.at[slot]),
            (up_far.at[:, span], upward_low.at[slot]),
            (active_far.at[:, span], active.at[slot]),
            (gate_weight.at[:, span], weight.at[:, slot_columns(0, slot)]),
            (up_weight.at[:, span], weight.at[:, slot_columns(2 * tile, slot)]),
            (down_weight.at[span, :], weight.at[slot_rows(slot), tail]),
        )
        return [
            pltpu.make_async_copy(far, near, tile_sem.at[number, slot])
            for number, (far, near) in enumerate(pairs_of)
        ]

    for copy in tile_copies(0):
        copy.start()
    greet_all(plan, rep, shard)
    for fetch in soon:
        fetch.wait()
    across[...] = normed_low[...].T

    def small_go(step, carry):
        other = lax.rem(rep * plan.shards + shard + step, total)
        other_rep, other_shard = lax.div(other, plan.shards), lax.rem(other, plan.shards)
        remote(
            small.at[other_shard], small_in.at[step - 1], small_sem.at[0], small_sem.at[1],
            other_rep, other_shard,
        ).start()
        return carry

    def whole_mate(turn, gap):
        return remote(
            mate_in.at[turn, gap], mate_in.at[turn, gap],
            mate_send.at[turn, gap], mate_recv.at[turn, gap], rep, mate,
        )

    def cross(turn, gap, order, step):
        far = plan.flip(rep, plan.ways[order][step])
        at = plan.halve_at(step)
        copies = [
            remote(
                held.at[turn, gap, :, pl.ds(plan.column(section, order), piece)],
                rep_in.at[turn, gap, order, at + number],
                rep_send.at[turn, gap, order, at + number],
                rep_recv.at[turn, gap, order, at + number],
                far, shard,
            )
            for number, section in enumerate(plan.halve(far, order, step))
        ]
        return copies, [plan.column(section, order) for section in plan.halve(rep, order, step)]

    wide_piece = plan.orders * piece
    own_columns = pl.ds(pl.multiple_of(rep * wide_piece, LANES), wide_piece)

    def z_copy(turn, gap):
        return remote(
            held.at[turn, gap, :, own_columns],
            z_in.at[turn, gap - 1],
            z_send.at[turn, gap - 1], z_recv.at[turn, gap - 1],
            rep, slab_at(gap, core),
        )

    def item_of(number):
        return lax.div(number, chips), lax.rem(lax.rem(number, chips) + 1, chips)

    def advance(number, step):
        turn, gap = item_of(number)
        if step == 0:
            whole_mate(turn, gap).wait_recv()

            def add(at, carry):
                span = pl.ds(pl.multiple_of(at * piece, LANES), piece)
                held[turn, gap, :, span] = (
                    held[turn, gap, :, span].astype(jnp.float32)
                    + mate_in[turn, gap, :, span].astype(jnp.float32)
                ).astype(jnp.bfloat16)
                return carry

            lax.fori_loop(0, plan.width // piece, add, 0)
        else:
            for order in range(plan.orders):
                copies, columns = cross(turn, gap, order, step - 1)
                at = plan.halve_at(step - 1)
                for index, (copy, column) in enumerate(zip(copies, columns)):
                    copy.wait_recv()
                    span = pl.ds(column, piece)
                    held[turn, gap, :, span] = (
                        held[turn, gap, :, span].astype(jnp.float32)
                        + rep_in[turn, gap, order, at + index].astype(jnp.float32)
                    ).astype(jnp.bfloat16)
        if step < levels:
            for order in range(plan.orders):
                for copy in cross(turn, gap, order, step)[0]:
                    copy.start()
        else:
            @pl.when(gap > 0)
            def _():
                z_copy(turn, gap).start()

    def spread(turn, order, step):
        far = plan.flip(rep, plan.ways[order][step])
        at = plan.grow_at(step)
        return [
            remote(
                final.at[turn, :, pl.ds(plan.column(section, order), piece)],
                final.at[turn, :, pl.ds(plan.column(section, order), piece)],
                last_send.at[turn, order, at + number],
                last_recv.at[turn, order, at + number],
                far, shard,
            )
            for number, section in enumerate(plan.grow(rep, order, step))
        ]

    def await_spread(turn, order, step):
        far = plan.flip(rep, plan.ways[order][step])
        at = plan.grow_at(step)
        for number, section in enumerate(plan.grow(far, order, step)):
            there = final.at[turn, :, pl.ds(plan.column(section, order), piece)]
            remote(
                there, there,
                last_send.at[turn, order, at + number],
                last_recv.at[turn, order, at + number],
                far, shard,
            ).wait_recv()

    def finish(turn, step):
        if step == 0:
            for gap in range(1, chips):
                z_copy(turn, gap).wait_recv()
            for order in range(plan.orders):
                span = pl.ds(plan.column(rep, order), piece)
                part = pl.ds(order * piece, piece)
                amount = held[turn, 0, :, span].astype(jnp.float32)
                for gap in range(1, chips):
                    amount = amount + z_in[turn, gap - 1, :, part].astype(jnp.float32)
                final[turn, :, span] = amount.astype(jnp.bfloat16)
        else:
            for order in range(plan.orders):
                await_spread(turn, order, step - 1)
        if step < levels:
            for order in range(plan.orders):
                for copy in spread(turn, order, step):
                    copy.start()

    def tick(now):
        for step in reversed(range(levels + 1)):
            behind = now - (SLACK * (levels + step + 1) + chips - 1)

            @pl.when((behind >= 0) & (lax.rem(behind + chips, chips) == 0) & (behind < count))
            def _(behind=behind, step=step):
                finish(lax.div(behind, chips), step)

        for step in reversed(range(levels + 1)):
            number = now - SLACK * step

            @pl.when((number >= 0) & (number < count))
            def _(number=number, step=step):
                advance(number, step)

    block = min(length, 256)

    def hidden(at, carry):
        slot = lax.rem(at, 2)
        for copy in tile_copies(at):
            copy.wait()

        @pl.when(at + 1 < 2 * groups)
        def _():
            for copy in tile_copies(at + 1):
                copy.start()

        start = tile_start(at)
        span = pl.ds(pl.multiple_of(start, LANES), tile)
        gate_tile = weight[:, slot_columns(0, slot)]
        up_tile = weight[:, slot_columns(2 * tile, slot)]
        down_tile = weight[slot_rows(slot), tail]

        def some(number, carry):
            some_rows = pl.ds(pl.multiple_of(number * block, block), block)
            active_grad = product(result_grad[some_rows, :], down_tile, 1, 1)
            gate = gate_low[slot, some_rows, :].astype(wide_type)
            upward = upward_low[slot, some_rows, :].astype(wide_type)
            sigmoid = 1.0 / (1.0 + jnp.exp(-gate))
            gate_part = (
                active_grad * upward * sigmoid * (1.0 + gate * (1.0 - sigmoid))
            ).astype(low_type)
            upward_part = (active_grad * (gate * sigmoid)).astype(low_type)
            gate_low[slot, some_rows, :] = gate_part
            upward_low[slot, some_rows, :] = upward_part
            grad[some_rows, :] += product(gate_part, gate_tile, 1, 1) + product(
                upward_part, up_tile, 1, 1
            )
            return carry

        lax.fori_loop(0, length // block, some, 0)
        down_part = product(active[slot], result_grad[...], 0, 0)
        per = plan.width // width
        for number in range(tile // rows):
            chunk = lax.div(start, rows) + number
            left = pl.multiple_of(lax.rem(chunk, per) * width, LANES)
            scatter(
                0, lax.div(chunk, per), pl.ds(left, width),
                down_part[number * rows : (number + 1) * rows, :],
            )
        for turn, low in ((1, gate_low), (2, upward_low)):
            for some_half in range(2):
                top = some_half * (width // 2)
                part = product(across[top : top + width // 2, :], low[slot], 1, 0)
                for number in range(width // 2 // rows):
                    scatter(
                        turn, top // rows + number, span,
                        part[number * rows : (number + 1) * rows, :],
                    )
        if chips == groups:
            @pl.when(lax.rem(at, 2) == 1)
            def _():
                number = lax.div(at, 2)
                give(0, lax.rem(number + 1, chips))

                @pl.when(number > 0)
                def _():
                    tick(number - 1)
        return carry

    lax.fori_loop(0, 2 * groups, hidden, 0)
    done = chips - 1 if chips == groups else 0
    for gap in gaps:
        if chips != groups:
            give(0, gap)
    for turn in (1, 2):
        for gap in gaps:
            give(turn, gap)
    weight_load = pltpu.make_async_copy(attention, weight, weight_sem)
    weight_load.start()
    for fetch in late:
        fetch.wait()
    mask_bias[...] = jnp.where(marks[:, 0:1] == segment_across[0:1, :], 0.0, NEG_LARGE)

    def norm_back():
        gain = sums[4:5, :]
        step_rows = min(length, 128)

        def some(number, carry):
            gain_sum, shift_sum = carry
            some_rows = pl.ds(pl.multiple_of(number * step_rows, step_rows), step_rows)
            centred = inner_resid[some_rows, :]
            centred = centred - jnp.mean(centred, axis=1, keepdims=True)
            inverse = lax.rsqrt(jnp.mean(centred * centred, axis=1, keepdims=True) + EPSILON)
            normalized = centred * inverse
            upstream = grad[some_rows, :]
            gain_sum += jnp.sum(upstream * normalized, axis=0, keepdims=True)
            shift_sum += jnp.sum(upstream, axis=0, keepdims=True)
            scaled = upstream * gain
            back = inverse * (
                scaled
                - jnp.mean(scaled, axis=1, keepdims=True)
                - normalized * jnp.mean(scaled * normalized, axis=1, keepdims=True)
            )
            grad[some_rows, :] = back
            branch[some_rows, :] = back.astype(low_type)
            return gain_sum, shift_sum

        nothing = jnp.zeros((1, width), wide_type)
        gain_sum, shift_sum = lax.fori_loop(0, length // step_rows, some, (nothing, nothing))
        sums[0:1, :] = gain_sum
        sums[1:2, :] = shift_sum
        vectors = sums[...]
        for number in range(plan.shards):
            small[number] = pltpu.roll(vectors, (width - rows * number) % width, 1)[:, :LANES]

    def columns_loop(number, work):
        def one(at, carry):
            work(at)
            return carry

        lax.fori_loop(0, number, one, 0)

    def raise_up():
        weight_load.wait()

        def one(at):
            span = pl.ds(pl.multiple_of(at * 256, 256), 256)
            upper[:, span] = product(
                branch[...], weight[span, 3 * width : 4 * width], 1, 1
            ).astype(low_type)

        columns_loop(width // 256, one)

    def weigh(left, right, lefts):
        def one(at):
            span = pl.ds(pl.multiple_of(left + at * tile, LANES), tile)
            source = pl.ds(pl.multiple_of(at * tile, LANES), tile)
            for some_half in range(2):
                top = some_half * (width // 2)
                part = product(across[top : top + width // 2, :], right[:, source], 1, 0)
                for number in range(width // 2 // rows):
                    scatter(
                        3, top // rows + number, span, part[number * rows : (number + 1) * rows, :]
                    )

        columns_loop(lefts, one)

    def middle(at, carry):
        @pl.when(at == 0)
        def _():
            norm_back()
            lax.fori_loop(1, total, small_go, 0)
            raise_up()

        @pl.when((at >= 1) & (at < pairs + 1))
        def _():
            back_pair(
                at - 1, query, key, value, upper, logsum, mask_bias, (cosine, before, after),
                joined_low, width,
            )

        @pl.when(at + done < early)
        def _():
            tick(at + done)
        return carry

    lax.fori_loop(0, max(pairs + 1, early - done), middle, 0)
    for gap in gaps:
        whole_mate(0, gap).wait_send()
    across[...] = attended[...].T
    weigh(3 * width, branch, width // tile)
    across[...] = tokens[...].T
    weigh(0, joined_low, 3 * width // tile)
    for gap in gaps:
        give(3, gap)

    def back(at):
        low = pl.ds(pl.multiple_of(at * 256, 256), 256)
        result_grad[:, low] = (
            grad[:, low] + product(joined_low[...], weight[low, 0 : 3 * width], 1, 1)
        ).astype(jnp.bfloat16)

    columns_loop(width // 256, back)
    result_copy = pltpu.make_async_copy(result_grad, input_grad, result_sem)
    result_copy.start()

    def late_tick(now, carry):
        tick(now)
        return carry

    lax.fori_loop(early, count + SLACK * (2 * levels + 1), late_tick, 0)

    everything = remote(small_in, small_in, small_sem.at[0], small_sem.at[1], rep, mate)
    everything.wait_recv()

    def gain_of(at, amount):
        return amount + small_in[at]

    small_out[...] = lax.fori_loop(0, total - 1, gain_of, small[shard])
    everything.wait_send()
    for turn in range(4):
        pltpu.make_async_copy(final.at[turn], outs[turn], out_sem.at[turn]).start()

    def drain(number, carry):
        turn, gap = item_of(number)

        @pl.when(turn > 0)
        def _():
            whole_mate(turn, gap).wait_send()
        for order in range(plan.orders):
            for step in range(levels):
                for copy in cross(turn, gap, order, step)[0]:
                    copy.wait_send()

        @pl.when(gap > 0)
        def _():
            z_copy(turn, gap).wait_send()
        return carry

    lax.fori_loop(0, count, drain, 0)
    for turn in range(4):
        for order in range(plan.orders):
            for step in range(levels):
                for copy in spread(turn, order, step):
                    copy.wait_send()
        pltpu.make_async_copy(final.at[turn], outs[turn], out_sem.at[turn]).wait()
    result_copy.wait()


def sum_grads(plan, streamed, carried):
    hbm = pl.BlockSpec(memory_space=pl.ANY)
    vmem = pl.BlockSpec(memory_space=pltpu.VMEM)
    dma = pltpu.SemaphoreType.DMA
    chips, gaps, crossing = plan.chips, plan.chips - 1, plan.replicas - 1
    length, width = carried[0].shape
    rows = width // plan.shards
    low, wide = jnp.bfloat16, jnp.float32
    total = plan.replicas * plan.shards
    return pl.pallas_call(
        functools.partial(sum_kernel, plan),
        out_shape=[jax.ShapeDtypeStruct((rows, plan.width), low)] * 4
        + [
            jax.ShapeDtypeStruct((8, LANES), wide),
            jax.ShapeDtypeStruct((length, width), low),
        ],
        in_specs=[hbm] * (len(streamed) + len(carried)),
        out_specs=[hbm] * 4 + [vmem, hbm],
        scratch_shapes=[
            pltpu.VMEM((7, chips, rows, plan.width), low),
            pltpu.VMEM((4, chips, rows, plan.width), low),
            pltpu.VMEM((4, chips, plan.orders, crossing, rows, plan.piece), low),
            pltpu.VMEM((4, gaps, rows, plan.orders * plan.piece), low),
            pltpu.VMEM((4, rows, plan.width), low),
            pltpu.VMEM((total - 1, 8, LANES), wide),
            dma((4,)),
            dma((2,)),
            dma((4, chips)),
            dma((4, chips)),
            dma((4, chips, plan.orders, crossing)),
            dma((4, chips, plan.orders, crossing)),
            dma((4, gaps)),
            dma((4, gaps)),
            dma((4, plan.orders, crossing)),
            dma((4, plan.orders, crossing)),
        ]
        + [pltpu.VMEM(array.shape, array.dtype) for array in carried]
        + [
            pltpu.VMEM((width, 4 * width), low),
            pltpu.VMEM((length, 3 * width), low),
            pltpu.VMEM((length, length), wide),
            pltpu.VMEM((width, length), low),
            pltpu.VMEM((length, width), low),
            pltpu.VMEM((length, width), low),
            pltpu.VMEM((plan.shards, 8, LANES), wide),
            pltpu.VMEM((2, length, width // 2), low),
            pltpu.VMEM((2, length, width // 2), low),
            pltpu.VMEM((2, length, width // 2), low),
            dma((len(carried),)),
            dma((6, 2)),
            dma,
            dma,
        ],
        compiler_params=pltpu.CompilerParams(
            collective_id=1, has_side_effects=True, vmem_limit_bytes=VMEM_MOST
        ),
        name="sum_grads",
    )(*streamed, *carried)


def layer_norm(values, gain, shift):
    centred = values - jnp.mean(values, axis=-1, keepdims=True)
    variance = jnp.mean(centred * centred, axis=-1, keepdims=True)
    return centred * lax.rsqrt(variance + EPSILON) * gain + shift


def on_device(
    tokens,
    joined_weight,
    mixing_weight,
    gate_weight,
    up_weight,
    down_weight,
    inner_gain,
    inner_shift,
    outer_gain,
    outer_shift,
    segments,
    positions,
    cotangent,
):
    replicas, shards = lax.axis_size("rep"), lax.axis_size("shard")
    plan = Plan(gate_weight.shape[1], replicas, shards)
    part_rows = joined_weight.shape[0]
    own_vectors = jnp.stack([inner_gain, inner_shift, outer_gain, outer_shift]).astype(jnp.float32)
    own_vectors = jnp.pad(own_vectors, ((0, 4), (0, LANES - part_rows)))
    length, model_width = tokens.shape
    halves = np.arange(LANES) % (HD // 2)
    rates = np.float32(1000.0) ** (-(2.0 * halves.astype(np.float32)) / np.float32(HD))
    marks = jnp.where(
        jnp.arange(LANES)[None, :] == 0, segments[0][:, None], positions[0][:, None]
    )
    (
        attention_full,
        gate_full,
        upward_full,
        down_full,
        vectors,
        query_low,
        key_low,
        value_low,
        attended_low,
        logsum,
        inner_resid,
        cosine_wide,
        before,
        after,
    ) = gather_weights(
        plan,
        (
            jnp.concatenate([joined_weight, mixing_weight], axis=1),
            gate_weight,
            up_weight,
            down_weight,
        ),
        own_vectors,
        (tokens, marks, segments, jnp.asarray(np.tile(rates[None, :], (8, 1)))),
    )
    vectors = vectors[:, :4, :part_rows].transpose(1, 0, 2).reshape(4, shards * part_rows)
    innergain_full, innershift_full, outergain_full, outershift_full = vectors
    normed = layer_norm(inner_resid, innergain_full, innershift_full)
    normed_low = normed.astype(jnp.bfloat16)
    gate_rows = jnp.dot(normed_low, gate_full, preferred_element_type=jnp.float32)
    upward = jnp.dot(normed_low, upward_full, preferred_element_type=jnp.float32)
    active_low = (jax.nn.silu(gate_rows) * upward).astype(jnp.bfloat16)
    result = jnp.dot(active_low, down_full, preferred_element_type=jnp.float32)
    final, outer_pull = jax.vjp(
        layer_norm,
        normed + result,
        outergain_full.astype(jnp.float32),
        outershift_full.astype(jnp.float32),
    )
    layer_output = final.astype(jnp.bfloat16)
    outer_grad, outergain_grad, outershift_grad = outer_pull(cotangent.astype(jnp.float32))
    result_grad = outer_grad.astype(jnp.bfloat16)
    low = jnp.bfloat16
    nothing = jnp.zeros_like(outergain_grad)
    sums = jnp.stack(
        [nothing, nothing, outergain_grad, outershift_grad, innergain_full] + [nothing] * 3
    )
    down_sum, gate_sum, up_sum, attention_sum, small_sum, input_grad = sum_grads(
        plan,
        (
            gate_rows.astype(low),
            upward.astype(low),
            active_low,
            gate_full,
            upward_full,
            down_full,
            attention_full,
        ),
        (
            query_low,
            key_low,
            value_low,
            attended_low,
            logsum,
            marks,
            segments,
            cosine_wide,
            before,
            after,
            tokens,
            inner_resid,
            outer_grad,
            result_grad,
            normed_low,
            sums,
        ),
    )
    down_sum = down_sum.reshape(part_rows, -1, model_width).transpose(1, 0, 2)
    full = jnp.float32
    return (
        layer_output,
        input_grad,
        attention_sum[:, : joined_weight.shape[1]].astype(full),
        attention_sum[:, joined_weight.shape[1] :].astype(full),
        gate_sum.astype(full),
        up_sum.astype(full),
        down_sum.reshape(down_weight.shape).astype(full),
        small_sum[0, :part_rows],
        small_sum[1, :part_rows],
        small_sum[2, :part_rows],
        small_sum[3, :part_rows],
    )


def solution(mesh):
    placed = (
        P(("rep", "shard"), None),
        P("shard", None),
        P("shard", None),
        P("shard", None),
        P("shard", None),
        P("shard", None),
        P("shard"),
        P("shard"),
        P("shard"),
        P("shard"),
        P(("rep", "shard"), None),
        P(("rep", "shard"), None),
        P(("rep", "shard"), None),
    )
    return jax.shard_map(
        on_device,
        mesh=mesh,
        in_specs=placed,
        out_specs=(
            P(("rep", "shard"), None),
            P(("rep", "shard"), None),
            P("shard", None),
            P("shard", None),
            P("shard", None),
            P("shard", None),
            P("shard", None),
            P("shard"),
            P("shard"),
            P("shard"),
            P("shard"),
        ),
        check_vma=False,
    )
```

```python
import functools
import math

import jax
import jax.numpy as jnp
import numpy as np
from jax import lax
from jax.experimental import pallas as pl
from jax.experimental.pallas import tpu as pltpu
from jax.sharding import PartitionSpec as P

H = 12
HD = 64

EPSILON = 1e-12
NEG_LARGE = -1e30
LANES = 128
MESH = pl.DeviceIdType.MESH
VMEM_LIMIT = 62 * 1024 * 1024
SLACK = 2
VMEM_MOST = 67043328
AHEAD = 3


class Plan:
    def __init__(self, width, replicas, shards):
        self.replicas, self.shards = replicas, shards
        self.chips = shards // 2
        self.levels = replicas.bit_length() - 1
        self.orders = 2 if self.levels > 1 and width % (2 * replicas * LANES) == 0 else 1
        self.ways = (tuple(range(self.levels)), tuple(reversed(range(self.levels))))[: self.orders]
        self.piece = width // (replicas * self.orders)
        self.width = width

    def flip(self, rep, bit):
        return rep + (1 << bit) * (1 - 2 * lax.rem(lax.div(rep, 1 << bit), 2))

    def with_bits(self, rep, bits, number):
        for at, bit in enumerate(bits):
            had = lax.rem(lax.div(rep, 1 << bit), 2)
            rep = rep + (1 << bit) * (((number >> at) & 1) - had)
        return rep

    def column(self, rep, order):
        return pl.multiple_of((rep * self.orders + order) * self.piece, LANES)

    def grow(self, rep, order, step):
        bits = self.ways[order][:step]
        return [self.with_bits(rep, bits, number) for number in range(1 << step)]

    def grow_at(self, step):
        return (1 << step) - 1

    def halve(self, rep, order, step):
        bits = self.ways[order][step + 1 :]
        return [self.with_bits(rep, bits, number) for number in range(1 << len(bits))]

    def halve_at(self, step):
        return sum(1 << (self.levels - 1 - at) for at in range(step))


def peer(rep, shard):
    return {"rep": rep, "shard": shard}


def remote(src, dst, send, recv, rep, shard):
    return pltpu.make_async_remote_copy(
        src_ref=src,
        dst_ref=dst,
        send_sem=send,
        recv_sem=recv,
        device_id=peer(rep, shard),
        device_id_type=MESH,
    )


def greet_all(plan, rep, shard):
    barrier = pltpu.get_barrier_semaphore()
    total = plan.replicas * plan.shards

    def hello(step, carry):
        other = lax.rem(rep * plan.shards + shard + step, total)
        pl.semaphore_signal(
            barrier,
            inc=1,
            device_id=peer(lax.div(other, plan.shards), lax.rem(other, plan.shards)),
            device_id_type=MESH,
        )
        return carry

    lax.fori_loop(1, total, hello, 0)
    pl.semaphore_wait(barrier, total - 1)


def greet_near(plan, rep, shard):
    barrier = pltpu.get_barrier_semaphore()
    for step in range(1, plan.shards):
        pl.semaphore_signal(
            barrier,
            inc=1,
            device_id=peer(rep, lax.rem(shard + step, plan.shards)),
            device_id_type=MESH,
        )
    for bit in range(plan.levels):
        pl.semaphore_signal(
            barrier, inc=1, device_id=peer(plan.flip(rep, bit), shard), device_id_type=MESH
        )
    pl.semaphore_wait(barrier, plan.shards - 1 + plan.levels)


def product(left, right, left_axis, right_axis):
    return lax.dot_general(
        left, right, (((left_axis,), (right_axis,)), ((), ())), preferred_element_type=jnp.float32
    )


def forward_pair(pair, query, key, value, mask_bias, attended, logsum):
    length = query.shape[0]
    block = min(length, 256)
    span = pl.ds(pl.multiple_of(pair * LANES, LANES), LANES)
    lane = lax.broadcasted_iota(jnp.int32, (1, LANES), 1)
    keys, values = key[:, span], value[:, span]
    parts = [0.0] * (length // block)
    for half in range(LANES // HD):
        pick = jnp.where(lane // HD == half, 1.0, 0.0).astype(jnp.bfloat16)
        scaled = pick * jnp.bfloat16(1.0 / math.sqrt(HD))
        picked = values * pick
        for at in range(length // block):
            rows = slice(at * block, (at + 1) * block)
            scores = product(keys, query[rows, span] * scaled, 1, 1) + mask_bias[:, rows]
            highest = jnp.max(scores, axis=0, keepdims=True)
            shifted = jnp.exp(scores - highest)
            denominator = jnp.sum(shifted, axis=0, keepdims=True)
            logsum[pl.ds(pair * (LANES // HD) + half, 1), rows] = highest + jnp.log(denominator)
            probs = (shifted * (1.0 / denominator)).astype(jnp.bfloat16)
            parts[at] += product(probs, picked, 0, 0)
    for at, part in enumerate(parts):
        attended[at * block : (at + 1) * block, span] = part.astype(jnp.bfloat16)


def gather_kernel(plan, *refs):
    own, small = refs[:4], refs[4]
    carried = refs[5:10]
    full, small_all = refs[10:14], refs[14]
    results = refs[15:34]
    stages = refs[34:38]
    (load_sem, store_sem, small_send, small_recv, z_send, z_recv, rep_send, rep_recv, core_send,
     core_recv) = refs[38:48]
    tokens, marks, segment_across, rates, cotangent = refs[48:53]
    near = refs[53:72]
    (query, key, value, attended, logsum, inner_resid, cosine, before, after, normed, normed_low,
     vectors) = near[:12]
    hidden_near, hidden_far = near[12:15], results[12:15]
    gate_low, upward_low, active = hidden_near
    outer_grad, result_grad, layer_output, sums = near[15:]
    weight, mask_bias, fetch_sem, weight_sem, result_sem = refs[72:77]
    hidden_weight, gate_rows, hidden_sem, down_near, down_sem, outer_sem = refs[77:]
    rep, shard = lax.axis_index("rep"), lax.axis_index("shard")
    chips, piece = plan.chips, plan.piece
    place, core = lax.div(shard, 2), lax.rem(shard, 2)
    mate = place * 2 + (1 - core)
    rows = own[0].shape[0]
    length, width = tokens.shape
    pairs = width // LANES

    def part(ref, mat, top, section_rep, order):
        if mat < 3:
            return ref.at[
                pl.ds(pl.multiple_of(top, 8), rows),
                pl.ds(plan.column(section_rep, order), piece),
            ]
        per = own[3].shape[1] // piece
        section = section_rep * plan.orders + order
        return ref.at[
            pl.ds(pl.multiple_of(top + lax.div(section, per) * rows, 8), rows),
            pl.ds(pl.multiple_of(lax.rem(section, per) * piece, LANES), piece),
        ]

    def slab_part(mat, slab, section_rep, order):
        return part(full[mat], mat, slab * own[mat].shape[0], section_rep, order)

    def slab_of(mat, slab):
        deep = own[mat].shape[0]
        return full[mat].at[pl.ds(pl.multiple_of(slab * deep, 8), deep), :]

    sent = []

    def launch(copy):
        copy.start()
        sent.append(copy)

    loads = [pltpu.make_async_copy(own[mat], stages[mat], load_sem.at[mat]) for mat in range(4)]
    for load in loads:
        load.start()
    fetches = [
        pltpu.make_async_copy(far, here, fetch_sem.at[at])
        for at, (far, here) in enumerate(zip(carried, refs[48:53]))
    ]
    for fetch in fetches:
        fetch.start()
    small_all[shard] = small[...]
    greet_near(plan, rep, shard)

    def small_copy(step):
        return remote(
            small, small_all.at[shard], small_send.at[step - 1], small_recv.at[step - 1],
            rep, lax.rem(shard + step, plan.shards),
        )

    fewest = jnp.minimum(place, chips - 1 - place)
    longer_above = jnp.where(2 * place < chips - 1, 1, 0)

    def nearest(number):
        inside = number <= 2 * fewest
        above = jnp.where(inside, number % 2, longer_above)
        distance = jnp.where(inside, (number + 1) // 2, number - fewest)
        return place + distance * (2 * above - 1), above

    def hop(mat, origin, down, order, source):
        return remote(
            source,
            slab_part(mat, origin * 2 + core, rep, order),
            z_send.at[mat, origin, down, order],
            z_recv.at[mat, origin, order],
            rep, (place + 1 - 2 * down) * 2 + core,
        )

    def own_hop(mat, down, order):
        return hop(mat, place, down, order, part(own[mat], mat, 0, rep, order))

    def next_hop(mat, number, order):
        origin, above = nearest(number)
        there = slab_part(mat, origin * 2 + core, rep, order)
        return hop(mat, origin, above, order, there)

    def leads(down):
        return (place > 0) if down else (place < chips - 1)

    def goes_on(number):
        _, above = nearest(number)
        onward = place + 1 - 2 * above
        return (onward >= 0) & (onward < chips)

    def along(mat, act):
        for down in range(2):
            @pl.when(leads(down))
            def _(down=down):
                for order in range(plan.orders):
                    act(own_hop(mat, down, order))

    def on(mat, number, act):
        @pl.when(goes_on(number))
        def _():
            for order in range(plan.orders):
                act(next_hop(mat, number, order))

    def give(mat):
        launch(remote(
            own[mat], slab_of(mat, shard), core_send.at[mat, 0], core_recv.at[mat, 0], rep, mate
        ))

    for mat in range(2):
        along(mat, lambda copy: copy.start())
    give(0)
    for step in range(1, plan.shards):
        launch(small_copy(step))
    for mat in range(1, 4):
        give(mat)
    stores = []
    for mat in range(4):
        loads[mat].wait()
        store = pltpu.make_async_copy(stages[mat], slab_of(mat, shard), store_sem.at[mat])
        store.start()
        stores.append(store)

    for fetch in fetches:
        fetch.wait()
    mask_bias[...] = jnp.where(marks[:, 0:1] == segment_across[0:1, :], 0.0, NEG_LARGE)
    angles = marks[:, 1:2].astype(jnp.float32) * rates[0:1, :]
    first = lax.broadcasted_iota(jnp.int32, (1, LANES), 1) % HD < HD // 2
    cosine[...] = jnp.cos(angles)
    sine = jnp.sin(angles)
    before[...] = jnp.where(first, -sine, 0.0)
    after[...] = jnp.where(first, 0.0, sine)

    def source(number):
        return nearest(number)[0] * 2 + core

    def exchange(mat, number, order, step):
        slab = source(number)
        far = plan.flip(rep, plan.ways[order][step])
        at = plan.grow_at(step)
        return [
            remote(
                slab_part(mat, slab, section, order),
                slab_part(mat, slab, section, order),
                rep_send.at[mat, number - 1, order, at + index],
                rep_recv.at[mat, number - 1, order, at + index],
                far, shard,
            )
            for index, section in enumerate(plan.grow(rep, order, step))
        ]

    def await_exchange(mat, number, order, step):
        slab = source(number)
        far = plan.flip(rep, plan.ways[order][step])
        at = plan.grow_at(step)
        for index, section in enumerate(plan.grow(far, order, step)):
            there = slab_part(mat, slab, section, order)
            remote(
                there, there,
                rep_send.at[mat, number - 1, order, at + index],
                rep_recv.at[mat, number - 1, order, at + index],
                far, shard,
            ).wait_recv()

    def relay(mat, number, step):
        for order in range(plan.orders):
            if step == 0:
                origin, _ = nearest(number)
                there = slab_part(mat, origin * 2 + core, rep, order)
                remote(
                    there, there, z_send.at[mat, origin, 0, order], z_recv.at[mat, origin, order],
                    rep, mate,
                ).wait_recv()
            else:
                await_exchange(mat, number, order, step - 1)
            if step < plan.levels:
                for copy in exchange(mat, number, order, step):
                    launch(copy)
        if step == 0:
            on(mat, number, lambda copy: copy.start())
            if number == 1 and mat + 2 < 4:
                along(mat + 2, lambda copy: copy.start())
        if step == plan.levels:
            there = slab_of(mat, source(number))
            launch(remote(
                there, there, core_send.at[mat, number], core_recv.at[mat, number], rep, mate
            ))

    def await_core(mat):
        stores[mat].wait()
        for number in range(chips):
            slab = (place if number == 0 else nearest(number)[0]) * 2 + (1 - core)
            there = slab_of(mat, slab)
            remote(
                there, there, core_send.at[mat, number], core_recv.at[mat, number], rep, mate
            ).wait_recv()

    weight_load = pltpu.make_async_copy(full[0], weight, weight_sem)

    def fetch_weight():
        await_core(0)
        weight_load.start()

    def project():
        weight_load.wait()
        tile = width // 2

        def columns(at):
            span = pl.ds(pl.multiple_of(at * tile, LANES), tile)
            return product(tokens[...], weight[:, span], 1, 0)

        def turned(at, carry):
            joined = columns(at)
            for down in range(tile // LANES):
                vector = joined[:, down * LANES : (down + 1) * LANES]
                spot = pl.ds(pl.multiple_of(lax.rem(at, 2) * tile + down * LANES, LANES), LANES)
                low = (
                    vector * cosine[...]
                    + pltpu.roll(vector, LANES - HD // 2, 1) * before[...]
                    + pltpu.roll(vector, HD // 2, 1) * after[...]
                ).astype(jnp.bfloat16)

                @pl.when(at < 2)
                def _():
                    query[:, spot] = low

                @pl.when(at >= 2)
                def _():
                    key[:, spot] = low
            return carry

        lax.fori_loop(0, 4, turned, 0)

        def plain(at, carry):
            value[:, pl.ds(pl.multiple_of(at * tile, LANES), tile)] = columns(at + 4).astype(
                jnp.bfloat16
            )
            return carry

        lax.fori_loop(0, 2, plain, 0)

    def attend(low, high):
        def one(pair, carry):
            forward_pair(pair, query, key, value, mask_bias, attended, logsum)
            return carry

        lax.fori_loop(low, high, one, 0)

    copies = [
        pltpu.make_async_copy(here, far, result_sem.at[at])
        for at, (here, far) in enumerate(zip(near[:12], results[:12]))
    ]

    def mix():
        def one(at, carry):
            span = pl.ds(pl.multiple_of(at * 256, 256), 256)
            across = pl.ds(pl.multiple_of(3 * width + at * 256, 256), 256)
            inner_resid[:, span] = tokens[:, span].astype(jnp.float32) + product(
                attended[...], weight[:, across], 1, 0
            )
            return carry

        lax.fori_loop(0, width // 256, one, 0)

    def normalize():
        for step in range(1, plan.shards):
            small_copy(step).wait_recv()
        rest = jnp.zeros((8, width - LANES), jnp.float32)
        whole = jnp.zeros((8, width), jnp.float32)
        for number in range(plan.shards):
            wide = jnp.concatenate([small_all[number], rest], axis=1)
            whole = whole + pltpu.roll(wide, number * rows, 1)
        vectors[...] = whole
        step_rows = min(length, 128)

        def some(at, carry):
            some_rows = pl.ds(pl.multiple_of(at * step_rows, step_rows), step_rows)
            centred = inner_resid[some_rows, :]
            centred = centred - jnp.mean(centred, axis=1, keepdims=True)
            inverse = lax.rsqrt(jnp.mean(centred * centred, axis=1, keepdims=True) + EPSILON)
            amount = centred * inverse * vectors[0:1, :] + vectors[1:2, :]
            normed[some_rows, :] = amount
            normed_low[some_rows, :] = amount.astype(jnp.bfloat16)
            return carry

        lax.fori_loop(0, length // step_rows, some, 0)
        for copy in copies:
            copy.start()

    tiles = 2 * plan.width // width

    def hidden_load(mat):
        return pltpu.make_async_copy(full[mat], hidden_weight, weight_sem)

    def hidden_copy(which, at):
        span = pl.ds(pl.multiple_of(at * (width // 2), LANES), width // 2)
        return pltpu.make_async_copy(
            hidden_near[which].at[:, span], hidden_far[which].at[:, span], hidden_sem.at[which, at]
        )

    def fetch_hidden(mat):
        await_core(mat)
        hidden_load(mat).start()

    def open_gate():
        hidden_load(1).wait()

        def one(at, carry):
            span = pl.ds(pl.multiple_of(at * (width // 2), LANES), width // 2)
            rows_of = product(normed_low[...], hidden_weight[:, span], 1, 0)
            gate_rows[:, span] = rows_of
            gate_low[:, span] = rows_of.astype(jnp.bfloat16)
            hidden_copy(0, at).start()
            return carry

        lax.fori_loop(0, tiles, one, 0)

    def activate():
        hidden_load(2).wait()

        def one(at, carry):
            span = pl.ds(pl.multiple_of(at * (width // 2), LANES), width // 2)
            upward = product(normed_low[...], hidden_weight[:, span], 1, 0)
            gate = gate_rows[:, span]
            upward_low[:, span] = upward.astype(jnp.bfloat16)
            active[:, span] = (gate / (1.0 + jnp.exp(-gate)) * upward).astype(jnp.bfloat16)
            hidden_copy(1, at).start()
            hidden_copy(2, at).start()
            return carry

        lax.fori_loop(0, tiles, one, 0)

    outer_copies = [
        pltpu.make_async_copy(here, far, outer_sem.at[at])
        for at, (here, far) in enumerate(zip(near[15:], results[15:]))
    ]

    def close():
        depth = plan.width // width
        loads = [
            pltpu.make_async_copy(
                full[3].at[pl.ds(at * width, width), :],
                down_near.at[pl.ds(at * width, width), :],
                down_sem.at[at],
            )
            for at in range(depth)
        ]
        for load in loads:
            load.start()
        block = min(length, 256)
        for at in range(depth):
            loads[at].wait()

            def some(number, carry, at=at):
                some_rows = pl.ds(pl.multiple_of(number * block, block), block)
                base = normed if at == 0 else outer_grad
                outer_grad[some_rows, :] = base[some_rows, :] + product(
                    active[some_rows, at * width : (at + 1) * width],
                    down_near[at * width : (at + 1) * width, :], 1, 0,
                )
                return carry

            lax.fori_loop(0, length // block, some, 0)
        gain, shift = vectors[2:3, :], vectors[3:4, :]
        step_rows = min(length, 128)

        def both(at, carry):
            gain_sum, shift_sum = carry
            some_rows = pl.ds(pl.multiple_of(at * step_rows, step_rows), step_rows)
            centred = outer_grad[some_rows, :]
            centred = centred - jnp.mean(centred, axis=1, keepdims=True)
            inverse = lax.rsqrt(jnp.mean(centred * centred, axis=1, keepdims=True) + EPSILON)
            normalized = centred * inverse
            layer_output[some_rows, :] = (normalized * gain + shift).astype(jnp.bfloat16)
            upstream = cotangent[some_rows, :].astype(jnp.float32)
            gain_sum += jnp.sum(upstream * normalized, axis=0, keepdims=True)
            shift_sum += jnp.sum(upstream, axis=0, keepdims=True)
            scaled = upstream * gain
            back = inverse * (
                scaled
                - jnp.mean(scaled, axis=1, keepdims=True)
                - normalized * jnp.mean(scaled * normalized, axis=1, keepdims=True)
            )
            outer_grad[some_rows, :] = back
            result_grad[some_rows, :] = back.astype(jnp.bfloat16)
            return gain_sum, shift_sum

        nothing = jnp.zeros((1, width), jnp.float32)
        gain_sum, shift_sum = lax.fori_loop(0, length // step_rows, both, (nothing, nothing))
        sums[...] = jnp.zeros_like(sums)
        sums[2:3, :] = gain_sum
        sums[3:4, :] = shift_sum
        sums[4:5, :] = vectors[0:1, :]
        for copy in outer_copies:
            copy.start()

    items = [(mat, number) for mat in range(4) for number in range(1, chips)]
    events = [
        (at + SLACK * step, -step, functools.partial(relay, *item, step))
        for at, item in enumerate(items)
        for step in range(plan.levels + 1)
    ]
    ready = chips - 1 + SLACK * plan.levels
    for late, work in (
        (0, fetch_weight),
        (1, project),
        (2, functools.partial(attend, 0, pairs // 2)),
        (3, functools.partial(attend, pairs // 2, pairs)),
        (4, mix),
        (4, normalize),
    ):
        events.append((ready + late, 1, work))
    ahead = chips - 1
    for due, work in (
        (ready + ahead, functools.partial(fetch_hidden, 1)),
        (max(ready + ahead, ready + 5), open_gate),
        (max(ready + 2 * ahead, ready + 5), functools.partial(fetch_hidden, 2)),
        (max(ready + 2 * ahead, ready + 5), activate),
    ):
        events.append((due, 2, work))
    for _, _, event in sorted(events, key=lambda event: event[:2]):
        event()

    await_core(3)
    close()
    for copy in sent:
        copy.wait_send()
    for mat in range(4):
        along(mat, lambda copy: copy.wait_send())
        for number in range(1, chips):
            on(mat, number, lambda copy: copy.wait_send())
    for copy in copies:
        copy.wait()
    for which in range(3):
        for at in range(tiles):
            hidden_copy(which, at).wait()
    for copy in outer_copies:
        copy.wait()


def gather_weights(plan, own, small, carried):
    hbm = pl.BlockSpec(memory_space=pl.ANY)
    vmem = pl.BlockSpec(memory_space=pltpu.VMEM)
    dma = pltpu.SemaphoreType.DMA
    shapes = [
        jax.ShapeDtypeStruct((array.shape[0] * plan.shards, array.shape[1]), array.dtype)
        for array in own
    ]
    gaps = plan.chips - 1
    crossing = plan.replicas - 1
    length, width = carried[0].shape
    wide, low = jnp.float32, jnp.bfloat16
    results = (
        [jax.ShapeDtypeStruct((length, width), low)] * 4
        + [
            jax.ShapeDtypeStruct((width // HD, length), wide),
            jax.ShapeDtypeStruct((length, width), wide),
        ]
        + [jax.ShapeDtypeStruct((length, LANES), wide)] * 3
        + [
            jax.ShapeDtypeStruct((length, width), wide),
            jax.ShapeDtypeStruct((length, width), low),
            jax.ShapeDtypeStruct((8, width), wide),
        ]
        + [jax.ShapeDtypeStruct((length, plan.width), low)] * 3
        + [
            jax.ShapeDtypeStruct((length, width), wide),
            jax.ShapeDtypeStruct((length, width), low),
            jax.ShapeDtypeStruct((length, width), low),
            jax.ShapeDtypeStruct((8, width), wide),
        ]
    )
    return pl.pallas_call(
        functools.partial(gather_kernel, plan),
        out_shape=shapes + [jax.ShapeDtypeStruct((plan.shards,) + small.shape, small.dtype)]
        + results,
        in_specs=[hbm] * 4 + [vmem] + [hbm] * len(carried),
        out_specs=[hbm] * 4 + [vmem] + [hbm] * len(results),
        scratch_shapes=[pltpu.VMEM(array.shape, array.dtype) for array in own]
        + [
            dma((4,)),
            dma((4,)),
            dma((plan.shards - 1,)),
            dma((plan.shards - 1,)),
            dma((4, plan.chips, 2, plan.orders)),
            dma((4, plan.chips, plan.orders)),
            dma((4, gaps, plan.orders, crossing)),
            dma((4, gaps, plan.orders, crossing)),
            dma((4, plan.chips)),
            dma((4, plan.chips)),
        ]
        + [pltpu.VMEM(array.shape, array.dtype) for array in carried]
        + [pltpu.VMEM(result.shape, result.dtype) for result in results]
        + [
            pltpu.VMEM(shapes[0].shape, low),
            pltpu.VMEM((length, length), wide),
            dma((len(carried),)),
            dma,
            dma((12,)),
            pltpu.VMEM(shapes[1].shape, low),
            pltpu.VMEM((length, plan.width), wide),
            dma((3, 2 * plan.width // width)),
            pltpu.VMEM(shapes[3].shape, low),
            dma((plan.width // width,)),
            dma((4,)),
        ],
        compiler_params=pltpu.CompilerParams(
            collective_id=0, has_side_effects=True, vmem_limit_bytes=VMEM_LIMIT
        ),
        name="gather_weights",
    )(*own, small, *carried)


def back_pair(pair, query, key, value, upper, logsum, mask_bias, tables, joined_low, width):
    length = query.shape[0]
    block = min(length, 256)
    span = pl.ds(pl.multiple_of(pair * LANES, LANES), LANES)
    lane = lax.broadcasted_iota(jnp.int32, (1, LANES), 1)
    keys, values = key[:, span], value[:, span]
    query_parts = [0.0] * (length // block)
    key_total = value_total = 0.0
    for half in range(LANES // HD):
        pick = jnp.where(lane // HD == half, 1.0, 0.0).astype(jnp.bfloat16)
        scaled = pick * jnp.bfloat16(1.0 / math.sqrt(HD))
        keys_scaled = keys * scaled
        rowsum = logsum[pl.ds(pair * (LANES // HD) + half, 1), :]
        for at in range(length // block):
            rows = slice(at * block, (at + 1) * block)
            queries_scaled = query[rows, span] * scaled
            grads = upper[rows, span] * pick
            scores = product(keys, queries_scaled, 1, 1) + mask_bias[:, rows]
            probs = jnp.exp(scores - rowsum[:, rows])
            dprobs = product(values, grads, 1, 1)
            dots = jnp.sum(probs * dprobs, axis=0, keepdims=True)
            score_grad = (probs * (dprobs - dots)).astype(jnp.bfloat16)
            value_total += product(probs.astype(jnp.bfloat16), grads, 1, 0)
            key_total += product(score_grad, queries_scaled, 1, 0)
            query_parts[at] += product(score_grad, keys_scaled, 0, 0)
    cosine, before, after = tables

    def unrotate(grad, rows):
        return (
            grad * cosine[rows, :]
            - pltpu.roll(grad, LANES - HD // 2, 1) * before[rows, :]
            - pltpu.roll(grad, HD // 2, 1) * after[rows, :]
        ).astype(jnp.bfloat16)

    for at, part in enumerate(query_parts):
        rows = slice(at * block, (at + 1) * block)
        joined_low[rows, span] = unrotate(part, rows)
    everything = slice(0, length)
    joined_low[:, pl.ds(pl.multiple_of(width + pair * LANES, LANES), LANES)] = unrotate(
        key_total, everything
    )
    joined_low[:, pl.ds(pl.multiple_of(2 * width + pair * LANES, LANES), LANES)] = (
        value_total.astype(jnp.bfloat16)
    )


def sum_kernel(plan, *refs):
    (gate_far, up_far, active_far, gate_weight, up_weight, down_weight, attention) = refs[:7]
    carried = refs[7:23]
    outs, small_out, input_grad = refs[23:27], refs[27], refs[28]
    (pool, mate_in, rep_in, z_in, final, small_in, out_sem, small_sem, mate_send, mate_recv,
     rep_send, rep_recv, z_send, z_recv, last_send, last_recv) = refs[29:45]
    here = refs[45:61]
    (weight, joined_low, mask_bias, across, branch, upper, small, gate_low, upward_low, active,
     fetch_sem, tile_sem, weight_sem, result_sem) = refs[61:]
    (query, key, value, attended, logsum, marks, segment_across, cosine, before, after, tokens,
     inner_resid, grad, result_grad, normed_low, sums) = here
    rep, shard = lax.axis_index("rep"), lax.axis_index("shard")
    chips, piece, levels = plan.chips, plan.piece, plan.levels
    place, core = lax.div(shard, 2), lax.rem(shard, 2)
    mate = place * 2 + (1 - core)
    rows = pool.shape[2]
    total = plan.replicas * plan.shards
    early = 3 * chips
    count = 4 * chips
    length, width = query.shape
    pairs = width // LANES
    groups = plan.width // width
    tile = width // 2
    low_type, wide_type = jnp.bfloat16, jnp.float32
    gaps = list(range(1, chips)) + [0]
    held = pool

    def slab_at(gap, which):
        return lax.rem(place + gap, chips) * 2 + which

    def stage(turn):
        return 4 + turn % 3

    def scatter(turn, slab, span, block):
        gap = lax.rem(lax.div(slab, 2) - place + chips, chips)
        other = lax.rem(slab + core, 2)
        pool[turn + other * (stage(turn) - turn), gap, :, span] = block.astype(low_type)

    def give(turn, gap):
        remote(
            pool.at[stage(turn), gap], mate_in.at[turn, gap],
            mate_send.at[turn, gap], mate_recv.at[turn, gap], rep, mate,
        ).start()

    fetches = [
        pltpu.make_async_copy(far, near, fetch_sem.at[at])
        for at, (far, near) in enumerate(zip(carried, here))
    ]
    late = fetches[:11]
    soon = fetches[11:]
    for fetch in soon + late:
        fetch.start()

    quarter = max(chips // groups, 1)
    home = lax.rem(lax.div(place, quarter), groups)

    def tile_start(at):
        group = lax.rem(home + 1 + lax.div(at, 2), groups)
        return group * width + lax.rem(at, 2) * tile

    def slot_columns(left, slot):
        return pl.ds(pl.multiple_of(left + slot * tile, LANES), tile)

    def slot_rows(slot):
        return pl.ds(pl.multiple_of(slot * tile, LANES), tile)

    tail = pl.ds(4 * tile, width)

    def tile_copies(at):
        slot = lax.rem(at, 2)
        span = pl.ds(pl.multiple_of(tile_start(at), LANES), tile)
        pairs_of = (
            (gate_far.at[:, span], gate_low.at[slot]),
            (up_far.at[:, span], upward_low.at[slot]),
            (active_far.at[:, span], active.at[slot]),
            (gate_weight.at[:, span], weight.at[:, slot_columns(0, slot)]),
            (up_weight.at[:, span], weight.at[:, slot_columns(2 * tile, slot)]),
            (down_weight.at[span, :], weight.at[slot_rows(slot), tail]),
        )
        return [
            pltpu.make_async_copy(far, near, tile_sem.at[number, slot])
            for number, (far, near) in enumerate(pairs_of)
        ]

    for copy in tile_copies(0):
        copy.start()
    greet_all(plan, rep, shard)
    for fetch in soon:
        fetch.wait()
    across[...] = normed_low[...].T

    def small_go(step, carry):
        other = lax.rem(rep * plan.shards + shard + step, total)
        other_rep, other_shard = lax.div(other, plan.shards), lax.rem(other, plan.shards)
        remote(
            small.at[other_shard], small_in.at[step - 1], small_sem.at[0], small_sem.at[1],
            other_rep, other_shard,
        ).start()
        return carry

    def whole_mate(turn, gap):
        return remote(
            mate_in.at[turn, gap], mate_in.at[turn, gap],
            mate_send.at[turn, gap], mate_recv.at[turn, gap], rep, mate,
        )

    def cross(turn, gap, order, step):
        far = plan.flip(rep, plan.ways[order][step])
        at = plan.halve_at(step)
        copies = [
            remote(
                held.at[turn, gap, :, pl.ds(plan.column(section, order), piece)],
                rep_in.at[turn, gap, order, at + number],
                rep_send.at[turn, gap, order, at + number],
                rep_recv.at[turn, gap, order, at + number],
                far, shard,
            )
            for number, section in enumerate(plan.halve(far, order, step))
        ]
        return copies, [plan.column(section, order) for section in plan.halve(rep, order, step)]

    wide_piece = plan.orders * piece
    own_columns = pl.ds(pl.multiple_of(rep * wide_piece, LANES), wide_piece)

    def z_copy(turn, gap):
        return remote(
            held.at[turn, gap, :, own_columns],
            z_in.at[turn, gap - 1],
            z_send.at[turn, gap - 1], z_recv.at[turn, gap - 1],
            rep, slab_at(gap, core),
        )

    def item_of(number):
        return lax.div(number, chips), lax.rem(lax.rem(number, chips) + 1, chips)

    def advance(number, step):
        turn, gap = item_of(number)
        if step == 0:
            whole_mate(turn, gap).wait_recv()

            def add(at, carry):
                span = pl.ds(pl.multiple_of(at * piece, LANES), piece)
                held[turn, gap, :, span] = (
                    held[turn, gap, :, span].astype(jnp.float32)
                    + mate_in[turn, gap, :, span].astype(jnp.float32)
                ).astype(jnp.bfloat16)
                return carry

            lax.fori_loop(0, plan.width // piece, add, 0)
        else:
            for order in range(plan.orders):
                copies, columns = cross(turn, gap, order, step - 1)
                at = plan.halve_at(step - 1)
                for index, (copy, column) in enumerate(zip(copies, columns)):
                    copy.wait_recv()
                    span = pl.ds(column, piece)
                    held[turn, gap, :, span] = (
                        held[turn, gap, :, span].astype(jnp.float32)
                        + rep_in[turn, gap, order, at + index].astype(jnp.float32)
                    ).astype(jnp.bfloat16)
        if step < levels:
            for order in range(plan.orders):
                for copy in cross(turn, gap, order, step)[0]:
                    copy.start()
        else:
            @pl.when(gap > 0)
            def _():
                z_copy(turn, gap).start()

    def spread(turn, order, step):
        far = plan.flip(rep, plan.ways[order][step])
        at = plan.grow_at(step)
        return [
            remote(
                final.at[turn, :, pl.ds(plan.column(section, order), piece)],
                final.at[turn, :, pl.ds(plan.column(section, order), piece)],
                last_send.at[turn, order, at + number],
                last_recv.at[turn, order, at + number],
                far, shard,
            )
            for number, section in enumerate(plan.grow(rep, order, step))
        ]

    def await_spread(turn, order, step):
        far = plan.flip(rep, plan.ways[order][step])
        at = plan.grow_at(step)
        for number, section in enumerate(plan.grow(far, order, step)):
            there = final.at[turn, :, pl.ds(plan.column(section, order), piece)]
            remote(
                there, there,
                last_send.at[turn, order, at + number],
                last_recv.at[turn, order, at + number],
                far, shard,
            ).wait_recv()

    def finish(turn, step):
        if step == 0:
            for gap in range(1, chips):
                z_copy(turn, gap).wait_recv()
            for order in range(plan.orders):
                span = pl.ds(plan.column(rep, order), piece)
                part = pl.ds(order * piece, piece)
                amount = held[turn, 0, :, span].astype(jnp.float32)
                for gap in range(1, chips):
                    amount = amount + z_in[turn, gap - 1, :, part].astype(jnp.float32)
                final[turn, :, span] = amount.astype(jnp.bfloat16)
        else:
            for order in range(plan.orders):
                await_spread(turn, order, step - 1)
        if step < levels:
            for order in range(plan.orders):
                for copy in spread(turn, order, step):
                    copy.start()

    def tick(now):
        for step in reversed(range(levels + 1)):
            behind = now - (SLACK * (levels + step + 1) + chips - 1)

            @pl.when((behind >= 0) & (lax.rem(behind + chips, chips) == 0) & (behind < count))
            def _(behind=behind, step=step):
                finish(lax.div(behind, chips), step)

        for step in reversed(range(levels + 1)):
            number = now - SLACK * step

            @pl.when((number >= 0) & (number < count))
            def _(number=number, step=step):
                advance(number, step)

    block = min(length, 256)

    def hidden(at, carry):
        slot = lax.rem(at, 2)
        for copy in tile_copies(at):
            copy.wait()

        @pl.when(at + 1 < 2 * groups)
        def _():
            for copy in tile_copies(at + 1):
                copy.start()

        start = tile_start(at)
        span = pl.ds(pl.multiple_of(start, LANES), tile)
        gate_tile = weight[:, slot_columns(0, slot)]
        up_tile = weight[:, slot_columns(2 * tile, slot)]
        down_tile = weight[slot_rows(slot), tail]

        def some(number, carry):
            some_rows = pl.ds(pl.multiple_of(number * block, block), block)
            active_grad = product(result_grad[some_rows, :], down_tile, 1, 1)
            gate = gate_low[slot, some_rows, :].astype(wide_type)
            upward = upward_low[slot, some_rows, :].astype(wide_type)
            sigmoid = 1.0 / (1.0 + jnp.exp(-gate))
            gate_part = (
                active_grad * upward * sigmoid * (1.0 + gate * (1.0 - sigmoid))
            ).astype(low_type)
            upward_part = (active_grad * (gate * sigmoid)).astype(low_type)
            gate_low[slot, some_rows, :] = gate_part
            upward_low[slot, some_rows, :] = upward_part
            grad[some_rows, :] += product(gate_part, gate_tile, 1, 1) + product(
                upward_part, up_tile, 1, 1
            )
            return carry

        lax.fori_loop(0, length // block, some, 0)
        down_part = product(active[slot], result_grad[...], 0, 0)
        per = plan.width // width
        for number in range(tile // rows):
            chunk = lax.div(start, rows) + number
            left = pl.multiple_of(lax.rem(chunk, per) * width, LANES)
            scatter(
                0, lax.div(chunk, per), pl.ds(left, width),
                down_part[number * rows : (number + 1) * rows, :],
            )
        for turn, low in ((1, gate_low), (2, upward_low)):
            for some_half in range(2):
                top = some_half * (width // 2)
                part = product(across[top : top + width // 2, :], low[slot], 1, 0)
                for number in range(width // 2 // rows):
                    scatter(
                        turn, top // rows + number, span,
                        part[number * rows : (number + 1) * rows, :],
                    )
        if chips == groups:
            @pl.when(lax.rem(at, 2) == 1)
            def _():
                number = lax.div(at, 2)
                give(0, lax.rem(number + 1, chips))

                @pl.when(number > 0)
                def _():
                    tick(number - 1)
        return carry

    lax.fori_loop(0, 2 * groups, hidden, 0)
    done = chips - 1 if chips == groups else 0
    for gap in gaps:
        if chips != groups:
            give(0, gap)
    for turn in (1, 2):
        for gap in gaps:
            give(turn, gap)
    weight_load = pltpu.make_async_copy(attention, weight, weight_sem)
    weight_load.start()
    for fetch in late:
        fetch.wait()
    mask_bias[...] = jnp.where(marks[:, 0:1] == segment_across[0:1, :], 0.0, NEG_LARGE)

    def norm_back():
        gain = sums[4:5, :]
        step_rows = min(length, 128)

        def some(number, carry):
            gain_sum, shift_sum = carry
            some_rows = pl.ds(pl.multiple_of(number * step_rows, step_rows), step_rows)
            centred = inner_resid[some_rows, :]
            centred = centred - jnp.mean(centred, axis=1, keepdims=True)
            inverse = lax.rsqrt(jnp.mean(centred * centred, axis=1, keepdims=True) + EPSILON)
            normalized = centred * inverse
            upstream = grad[some_rows, :]
            gain_sum += jnp.sum(upstream * normalized, axis=0, keepdims=True)
            shift_sum += jnp.sum(upstream, axis=0, keepdims=True)
            scaled = upstream * gain
            back = inverse * (
                scaled
                - jnp.mean(scaled, axis=1, keepdims=True)
                - normalized * jnp.mean(scaled * normalized, axis=1, keepdims=True)
            )
            grad[some_rows, :] = back
            branch[some_rows, :] = back.astype(low_type)
            return gain_sum, shift_sum

        nothing = jnp.zeros((1, width), wide_type)
        gain_sum, shift_sum = lax.fori_loop(0, length // step_rows, some, (nothing, nothing))
        sums[0:1, :] = gain_sum
        sums[1:2, :] = shift_sum
        vectors = sums[...]
        for number in range(plan.shards):
            small[number] = pltpu.roll(vectors, (width - rows * number) % width, 1)[:, :LANES]

    def columns_loop(number, work):
        def one(at, carry):
            work(at)
            return carry

        lax.fori_loop(0, number, one, 0)

    def raise_up():
        weight_load.wait()

        def one(at):
            span = pl.ds(pl.multiple_of(at * 256, 256), 256)
            upper[:, span] = product(
                branch[...], weight[span, 3 * width : 4 * width], 1, 1
            ).astype(low_type)

        columns_loop(width // 256, one)

    def weigh(left, right, lefts):
        def one(at):
            span = pl.ds(pl.multiple_of(left + at * tile, LANES), tile)
            source = pl.ds(pl.multiple_of(at * tile, LANES), tile)
            for some_half in range(2):
                top = some_half * (width // 2)
                part = product(across[top : top + width // 2, :], right[:, source], 1, 0)
                for number in range(width // 2 // rows):
                    scatter(
                        3, top // rows + number, span, part[number * rows : (number + 1) * rows, :]
                    )

        columns_loop(lefts, one)

    def middle(at, carry):
        @pl.when(at == 0)
        def _():
            norm_back()
            lax.fori_loop(1, total, small_go, 0)
            raise_up()

        @pl.when((at >= 1) & (at < pairs + 1))
        def _():
            back_pair(
                at - 1, query, key, value, upper, logsum, mask_bias, (cosine, before, after),
                joined_low, width,
            )

        @pl.when(at + done < early)
        def _():
            tick(at + done)
        return carry

    lax.fori_loop(0, max(pairs + 1, early - done), middle, 0)
    for gap in gaps:
        whole_mate(0, gap).wait_send()
    across[...] = attended[...].T
    weigh(3 * width, branch, width // tile)
    across[...] = tokens[...].T
    weigh(0, joined_low, 3 * width // tile)
    for gap in gaps:
        give(3, gap)

    def back(at):
        low = pl.ds(pl.multiple_of(at * 256, 256), 256)
        result_grad[:, low] = (
            grad[:, low] + product(joined_low[...], weight[low, 0 : 3 * width], 1, 1)
        ).astype(jnp.bfloat16)

    columns_loop(width // 256, back)
    result_copy = pltpu.make_async_copy(result_grad, input_grad, result_sem)
    result_copy.start()

    def late_tick(now, carry):
        tick(now)
        return carry

    lax.fori_loop(early, count + SLACK * (2 * levels + 1), late_tick, 0)

    everything = remote(small_in, small_in, small_sem.at[0], small_sem.at[1], rep, mate)
    everything.wait_recv()

    def gain_of(at, amount):
        return amount + small_in[at]

    small_out[...] = lax.fori_loop(0, total - 1, gain_of, small[shard])
    everything.wait_send()
    for turn in range(4):
        pltpu.make_async_copy(final.at[turn], outs[turn], out_sem.at[turn]).start()

    def drain(number, carry):
        turn, gap = item_of(number)

        @pl.when(turn > 0)
        def _():
            whole_mate(turn, gap).wait_send()
        for order in range(plan.orders):
            for step in range(levels):
                for copy in cross(turn, gap, order, step)[0]:
                    copy.wait_send()

        @pl.when(gap > 0)
        def _():
            z_copy(turn, gap).wait_send()
        return carry

    lax.fori_loop(0, count, drain, 0)
    for turn in range(4):
        for order in range(plan.orders):
            for step in range(levels):
                for copy in spread(turn, order, step):
                    copy.wait_send()
        pltpu.make_async_copy(final.at[turn], outs[turn], out_sem.at[turn]).wait()
    result_copy.wait()


def sum_grads(plan, streamed, carried):
    hbm = pl.BlockSpec(memory_space=pl.ANY)
    vmem = pl.BlockSpec(memory_space=pltpu.VMEM)
    dma = pltpu.SemaphoreType.DMA
    chips, gaps, crossing = plan.chips, plan.chips - 1, plan.replicas - 1
    length, width = carried[0].shape
    rows = width // plan.shards
    low, wide = jnp.bfloat16, jnp.float32
    total = plan.replicas * plan.shards
    return pl.pallas_call(
        functools.partial(sum_kernel, plan),
        out_shape=[jax.ShapeDtypeStruct((rows, plan.width), low)] * 4
        + [
            jax.ShapeDtypeStruct((8, LANES), wide),
            jax.ShapeDtypeStruct((length, width), low),
        ],
        in_specs=[hbm] * (len(streamed) + len(carried)),
        out_specs=[hbm] * 4 + [vmem, hbm],
        scratch_shapes=[
            pltpu.VMEM((7, chips, rows, plan.width), low),
            pltpu.VMEM((4, chips, rows, plan.width), low),
            pltpu.VMEM((4, chips, plan.orders, crossing, rows, plan.piece), low),
            pltpu.VMEM((4, gaps, rows, plan.orders * plan.piece), low),
            pltpu.VMEM((4, rows, plan.width), low),
            pltpu.VMEM((total - 1, 8, LANES), wide),
            dma((4,)),
            dma((2,)),
            dma((4, chips)),
            dma((4, chips)),
            dma((4, chips, plan.orders, crossing)),
            dma((4, chips, plan.orders, crossing)),
            dma((4, gaps)),
            dma((4, gaps)),
            dma((4, plan.orders, crossing)),
            dma((4, plan.orders, crossing)),
        ]
        + [pltpu.VMEM(array.shape, array.dtype) for array in carried]
        + [
            pltpu.VMEM((width, 4 * width), low),
            pltpu.VMEM((length, 3 * width), low),
            pltpu.VMEM((length, length), wide),
            pltpu.VMEM((width, length), low),
            pltpu.VMEM((length, width), low),
            pltpu.VMEM((length, width), low),
            pltpu.VMEM((plan.shards, 8, LANES), wide),
            pltpu.VMEM((2, length, width // 2), low),
            pltpu.VMEM((2, length, width // 2), low),
            pltpu.VMEM((2, length, width // 2), low),
            dma((len(carried),)),
            dma((6, 2)),
            dma,
            dma,
        ],
        compiler_params=pltpu.CompilerParams(
            collective_id=1, has_side_effects=True, vmem_limit_bytes=VMEM_MOST
        ),
        name="sum_grads",
    )(*streamed, *carried)


def on_device(
    tokens,
    joined_weight,
    mixing_weight,
    gate_weight,
    up_weight,
    down_weight,
    inner_gain,
    inner_shift,
    outer_gain,
    outer_shift,
    segments,
    positions,
    cotangent,
):
    replicas, shards = lax.axis_size("rep"), lax.axis_size("shard")
    plan = Plan(gate_weight.shape[1], replicas, shards)
    part_rows = joined_weight.shape[0]
    own_vectors = jnp.stack([inner_gain, inner_shift, outer_gain, outer_shift]).astype(jnp.float32)
    own_vectors = jnp.pad(own_vectors, ((0, 4), (0, LANES - part_rows)))
    length, model_width = tokens.shape
    halves = np.arange(LANES) % (HD // 2)
    rates = np.float32(1000.0) ** (-(2.0 * halves.astype(np.float32)) / np.float32(HD))
    marks = jnp.where(
        jnp.arange(LANES)[None, :] == 0, segments[0][:, None], positions[0][:, None]
    )
    (
        attention_full,
        gate_full,
        upward_full,
        down_full,
        _,
        query_low,
        key_low,
        value_low,
        attended_low,
        logsum,
        inner_resid,
        cosine_wide,
        before,
        after,
        _,
        normed_low,
        _,
        gate_low,
        upward_low,
        active_low,
        outer_grad,
        result_grad,
        layer_output,
        sums,
    ) = gather_weights(
        plan,
        (
            jnp.concatenate([joined_weight, mixing_weight], axis=1),
            gate_weight,
            up_weight,
            down_weight,
        ),
        own_vectors,
        (tokens, marks, segments, jnp.asarray(np.tile(rates[None, :], (8, 1))), cotangent),
    )
    down_sum, gate_sum, up_sum, attention_sum, small_sum, input_grad = sum_grads(
        plan,
        (
            gate_low,
            upward_low,
            active_low,
            gate_full,
            upward_full,
            down_full,
            attention_full,
        ),
        (
            query_low,
            key_low,
            value_low,
            attended_low,
            logsum,
            marks,
            segments,
            cosine_wide,
            before,
            after,
            tokens,
            inner_resid,
            outer_grad,
            result_grad,
            normed_low,
            sums,
        ),
    )
    down_sum = down_sum.reshape(part_rows, -1, model_width).transpose(1, 0, 2)
    full = jnp.float32
    return (
        layer_output,
        input_grad,
        attention_sum[:, : joined_weight.shape[1]].astype(full),
        attention_sum[:, joined_weight.shape[1] :].astype(full),
        gate_sum.astype(full),
        up_sum.astype(full),
        down_sum.reshape(down_weight.shape).astype(full),
        small_sum[0, :part_rows],
        small_sum[1, :part_rows],
        small_sum[2, :part_rows],
        small_sum[3, :part_rows],
    )


def solution(mesh):
    placed = (
        P(("rep", "shard"), None),
        P("shard", None),
        P("shard", None),
        P("shard", None),
        P("shard", None),
        P("shard", None),
        P("shard"),
        P("shard"),
        P("shard"),
        P("shard"),
        P(("rep", "shard"), None),
        P(("rep", "shard"), None),
        P(("rep", "shard"), None),
    )
    return jax.shard_map(
        on_device,
        mesh=mesh,
        in_specs=placed,
        out_specs=(
            P(("rep", "shard"), None),
            P(("rep", "shard"), None),
            P("shard", None),
            P("shard", None),
            P("shard", None),
            P("shard", None),
            P("shard", None),
            P("shard"),
            P("shard"),
            P("shard"),
            P("shard"),
        ),
        check_vma=False,
    )
```

```python
import functools
import math

import jax
import jax.numpy as jnp
import numpy as np
from jax import lax
from jax.experimental import pallas as pl
from jax.experimental.pallas import tpu as pltpu
from jax.sharding import PartitionSpec as P

H = 12
HD = 64

EPSILON = 1e-12
NEG_LARGE = -1e30
LANES = 128
MESH = pl.DeviceIdType.MESH
VMEM_LIMIT = 62 * 1024 * 1024
SLACK = 2
VMEM_MOST = 67043328
LIFTS = 2
AHEAD = 3


class Plan:
    def __init__(self, width, replicas, shards):
        self.replicas, self.shards = replicas, shards
        self.chips = shards // 2
        self.levels = replicas.bit_length() - 1
        self.orders = 2 if self.levels > 1 and width % (2 * replicas * LANES) == 0 else 1
        self.ways = (tuple(range(self.levels)), tuple(reversed(range(self.levels))))[: self.orders]
        self.piece = width // (replicas * self.orders)
        self.width = width

    def flip(self, rep, bit):
        return rep + (1 << bit) * (1 - 2 * lax.rem(lax.div(rep, 1 << bit), 2))

    def with_bits(self, rep, bits, number):
        for at, bit in enumerate(bits):
            had = lax.rem(lax.div(rep, 1 << bit), 2)
            rep = rep + (1 << bit) * (((number >> at) & 1) - had)
        return rep

    def column(self, rep, order):
        return pl.multiple_of((rep * self.orders + order) * self.piece, LANES)

    def grow(self, rep, order, step):
        bits = self.ways[order][:step]
        return [self.with_bits(rep, bits, number) for number in range(1 << step)]

    def grow_at(self, step):
        return (1 << step) - 1

    def halve(self, rep, order, step):
        bits = self.ways[order][step + 1 :]
        return [self.with_bits(rep, bits, number) for number in range(1 << len(bits))]

    def halve_at(self, step):
        return sum(1 << (self.levels - 1 - at) for at in range(step))


def peer(rep, shard):
    return {"rep": rep, "shard": shard}


def remote(src, dst, send, recv, rep, shard):
    return pltpu.make_async_remote_copy(
        src_ref=src,
        dst_ref=dst,
        send_sem=send,
        recv_sem=recv,
        device_id=peer(rep, shard),
        device_id_type=MESH,
    )


def greet_all(plan, rep, shard):
    barrier = pltpu.get_barrier_semaphore()
    total = plan.replicas * plan.shards

    def hello(step, carry):
        other = lax.rem(rep * plan.shards + shard + step, total)
        pl.semaphore_signal(
            barrier,
            inc=1,
            device_id=peer(lax.div(other, plan.shards), lax.rem(other, plan.shards)),
            device_id_type=MESH,
        )
        return carry

    lax.fori_loop(1, total, hello, 0)
    pl.semaphore_wait(barrier, total - 1)


def greet_near(plan, rep, shard):
    barrier = pltpu.get_barrier_semaphore()
    for step in range(1, plan.shards):
        pl.semaphore_signal(
            barrier,
            inc=1,
            device_id=peer(rep, lax.rem(shard + step, plan.shards)),
            device_id_type=MESH,
        )
    for bit in range(plan.levels):
        pl.semaphore_signal(
            barrier, inc=1, device_id=peer(plan.flip(rep, bit), shard), device_id_type=MESH
        )
    pl.semaphore_wait(barrier, plan.shards - 1 + plan.levels)


def product(left, right, left_axis, right_axis):
    return lax.dot_general(
        left, right, (((left_axis,), (right_axis,)), ((), ())), preferred_element_type=jnp.float32
    )


def forward_pair(pair, query, key, value, mask_bias, attended, logsum):
    length = query.shape[0]
    block = min(length, 256)
    span = pl.ds(pl.multiple_of(pair * LANES, LANES), LANES)
    lane = lax.broadcasted_iota(jnp.int32, (1, LANES), 1)
    keys, values = key[:, span], value[:, span]
    parts = [0.0] * (length // block)
    for half in range(LANES // HD):
        pick = jnp.where(lane // HD == half, 1.0, 0.0).astype(jnp.bfloat16)
        scaled = pick * jnp.bfloat16(1.0 / math.sqrt(HD))
        picked = values * pick
        for at in range(length // block):
            rows = slice(at * block, (at + 1) * block)
            scores = product(keys, query[rows, span] * scaled, 1, 1) + mask_bias[:, rows]
            highest = jnp.max(scores, axis=0, keepdims=True)
            shifted = jnp.exp(scores - highest)
            denominator = jnp.sum(shifted, axis=0, keepdims=True)
            logsum[pl.ds(pair * (LANES // HD) + half, 1), rows] = highest + jnp.log(denominator)
            probs = (shifted * (1.0 / denominator)).astype(jnp.bfloat16)
            parts[at] += product(probs, picked, 0, 0)
    for at, part in enumerate(parts):
        attended[at * block : (at + 1) * block, span] = part.astype(jnp.bfloat16)


def gather_kernel(plan, *refs):
    own, small = refs[:4], refs[4]
    carried = refs[5:10]
    full, small_all = refs[10:14], refs[14]
    results = refs[15:34]
    stages = refs[34:38]
    (load_sem, store_sem, small_send, small_recv, z_send, z_recv, rep_send, rep_recv, core_send,
     core_recv) = refs[38:48]
    tokens, marks, segment_across, rates, cotangent = refs[48:53]
    near = refs[53:72]
    (query, key, value, attended, logsum, inner_resid, cosine, before, after, normed, normed_low,
     vectors) = near[:12]
    hidden_near, hidden_far = near[12:15], results[12:15]
    gate_low, upward_low, active = hidden_near
    outer_grad, result_grad, layer_output, sums = near[15:]
    weight, mask_bias, fetch_sem, weight_sem, result_sem = refs[72:77]
    hidden_weight, gate_rows, hidden_sem, down_near, down_sem, outer_sem = refs[77:]
    rep, shard = lax.axis_index("rep"), lax.axis_index("shard")
    chips, piece = plan.chips, plan.piece
    place, core = lax.div(shard, 2), lax.rem(shard, 2)
    mate = place * 2 + (1 - core)
    rows = own[0].shape[0]
    length, width = tokens.shape
    pairs = width // LANES

    def part(ref, mat, top, section_rep, order):
        if mat < 3:
            return ref.at[
                pl.ds(pl.multiple_of(top, 8), rows),
                pl.ds(plan.column(section_rep, order), piece),
            ]
        per = own[3].shape[1] // piece
        section = section_rep * plan.orders + order
        return ref.at[
            pl.ds(pl.multiple_of(top + lax.div(section, per) * rows, 8), rows),
            pl.ds(pl.multiple_of(lax.rem(section, per) * piece, LANES), piece),
        ]

    def slab_part(mat, slab, section_rep, order):
        return part(full[mat], mat, slab * own[mat].shape[0], section_rep, order)

    def slab_of(mat, slab):
        deep = own[mat].shape[0]
        return full[mat].at[pl.ds(pl.multiple_of(slab * deep, 8), deep), :]

    sent = []

    def launch(copy):
        copy.start()
        sent.append(copy)

    loads = [pltpu.make_async_copy(own[mat], stages[mat], load_sem.at[mat]) for mat in range(4)]
    for load in loads:
        load.start()
    fetches = [
        pltpu.make_async_copy(far, here, fetch_sem.at[at])
        for at, (far, here) in enumerate(zip(carried, refs[48:53]))
    ]
    for fetch in fetches:
        fetch.start()
    small_all[shard] = small[...]
    greet_near(plan, rep, shard)

    def small_copy(step):
        return remote(
            small, small_all.at[shard], small_send.at[step - 1], small_recv.at[step - 1],
            rep, lax.rem(shard + step, plan.shards),
        )

    fewest = jnp.minimum(place, chips - 1 - place)
    longer_above = jnp.where(2 * place < chips - 1, 1, 0)

    def nearest(number):
        inside = number <= 2 * fewest
        above = jnp.where(inside, number % 2, longer_above)
        distance = jnp.where(inside, (number + 1) // 2, number - fewest)
        return place + distance * (2 * above - 1), above

    def hop(mat, origin, down, order, source):
        return remote(
            source,
            slab_part(mat, origin * 2 + core, rep, order),
            z_send.at[mat, origin, down, order],
            z_recv.at[mat, origin, order],
            rep, (place + 1 - 2 * down) * 2 + core,
        )

    def own_hop(mat, down, order):
        return hop(mat, place, down, order, part(own[mat], mat, 0, rep, order))

    def next_hop(mat, number, order):
        origin, above = nearest(number)
        there = slab_part(mat, origin * 2 + core, rep, order)
        return hop(mat, origin, above, order, there)

    def leads(down):
        return (place > 0) if down else (place < chips - 1)

    def goes_on(number):
        _, above = nearest(number)
        onward = place + 1 - 2 * above
        return (onward >= 0) & (onward < chips)

    def along(mat, act):
        for down in range(2):
            @pl.when(leads(down))
            def _(down=down):
                for order in range(plan.orders):
                    act(own_hop(mat, down, order))

    def on(mat, number, act):
        @pl.when(goes_on(number))
        def _():
            for order in range(plan.orders):
                act(next_hop(mat, number, order))

    def give(mat):
        launch(remote(
            own[mat], slab_of(mat, shard), core_send.at[mat, 0], core_recv.at[mat, 0], rep, mate
        ))

    for mat in range(2):
        along(mat, lambda copy: copy.start())
    give(0)
    for step in range(1, plan.shards):
        launch(small_copy(step))
    for mat in range(1, 4):
        give(mat)
    stores = []
    for mat in range(4):
        loads[mat].wait()
        store = pltpu.make_async_copy(stages[mat], slab_of(mat, shard), store_sem.at[mat])
        store.start()
        stores.append(store)

    for fetch in fetches:
        fetch.wait()
    mask_bias[...] = jnp.where(marks[:, 0:1] == segment_across[0:1, :], 0.0, NEG_LARGE)
    angles = marks[:, 1:2].astype(jnp.float32) * rates[0:1, :]
    first = lax.broadcasted_iota(jnp.int32, (1, LANES), 1) % HD < HD // 2
    cosine[...] = jnp.cos(angles)
    sine = jnp.sin(angles)
    before[...] = jnp.where(first, -sine, 0.0)
    after[...] = jnp.where(first, 0.0, sine)

    def source(number):
        return nearest(number)[0] * 2 + core

    def exchange(mat, number, order, step):
        slab = source(number)
        far = plan.flip(rep, plan.ways[order][step])
        at = plan.grow_at(step)
        return [
            remote(
                slab_part(mat, slab, section, order),
                slab_part(mat, slab, section, order),
                rep_send.at[mat, number - 1, order, at + index],
                rep_recv.at[mat, number - 1, order, at + index],
                far, shard,
            )
            for index, section in enumerate(plan.grow(rep, order, step))
        ]

    def await_exchange(mat, number, order, step):
        slab = source(number)
        far = plan.flip(rep, plan.ways[order][step])
        at = plan.grow_at(step)
        for index, section in enumerate(plan.grow(far, order, step)):
            there = slab_part(mat, slab, section, order)
            remote(
                there, there,
                rep_send.at[mat, number - 1, order, at + index],
                rep_recv.at[mat, number - 1, order, at + index],
                far, shard,
            ).wait_recv()

    def relay(mat, number, step):
        for order in range(plan.orders):
            if step == 0:
                origin, _ = nearest(number)
                there = slab_part(mat, origin * 2 + core, rep, order)
                remote(
                    there, there, z_send.at[mat, origin, 0, order], z_recv.at[mat, origin, order],
                    rep, mate,
                ).wait_recv()
            else:
                await_exchange(mat, number, order, step - 1)
            if step < plan.levels:
                for copy in exchange(mat, number, order, step):
                    launch(copy)
        if step == 0:
            on(mat, number, lambda copy: copy.start())
            if number == 1 and mat + 2 < 4:
                along(mat + 2, lambda copy: copy.start())
        if step == plan.levels:
            there = slab_of(mat, source(number))
            launch(remote(
                there, there, core_send.at[mat, number], core_recv.at[mat, number], rep, mate
            ))

    def await_core(mat):
        stores[mat].wait()
        for number in range(chips):
            slab = (place if number == 0 else nearest(number)[0]) * 2 + (1 - core)
            there = slab_of(mat, slab)
            remote(
                there, there, core_send.at[mat, number], core_recv.at[mat, number], rep, mate
            ).wait_recv()

    weight_load = pltpu.make_async_copy(full[0], weight, weight_sem)

    def fetch_weight():
        await_core(0)
        weight_load.start()

    def project():
        weight_load.wait()
        tile = width // 2

        def columns(at):
            span = pl.ds(pl.multiple_of(at * tile, LANES), tile)
            return product(tokens[...], weight[:, span], 1, 0)

        def turned(at, carry):
            joined = columns(at)
            for down in range(tile // LANES):
                vector = joined[:, down * LANES : (down + 1) * LANES]
                spot = pl.ds(pl.multiple_of(lax.rem(at, 2) * tile + down * LANES, LANES), LANES)
                low = (
                    vector * cosine[...]
                    + pltpu.roll(vector, LANES - HD // 2, 1) * before[...]
                    + pltpu.roll(vector, HD // 2, 1) * after[...]
                ).astype(jnp.bfloat16)

                @pl.when(at < 2)
                def _():
                    query[:, spot] = low

                @pl.when(at >= 2)
                def _():
                    key[:, spot] = low
            return carry

        lax.fori_loop(0, 4, turned, 0)

        def plain(at, carry):
            value[:, pl.ds(pl.multiple_of(at * tile, LANES), tile)] = columns(at + 4).astype(
                jnp.bfloat16
            )
            return carry

        lax.fori_loop(0, 2, plain, 0)

    def attend(low, high):
        def one(pair, carry):
            forward_pair(pair, query, key, value, mask_bias, attended, logsum)
            return carry

        lax.fori_loop(low, high, one, 0)

    copies = [
        pltpu.make_async_copy(here, far, result_sem.at[at])
        for at, (here, far) in enumerate(zip(near[:12], results[:12]))
    ]

    def mix():
        def one(at, carry):
            span = pl.ds(pl.multiple_of(at * 256, 256), 256)
            across = pl.ds(pl.multiple_of(3 * width + at * 256, 256), 256)
            inner_resid[:, span] = tokens[:, span].astype(jnp.float32) + product(
                attended[...], weight[:, across], 1, 0
            )
            return carry

        lax.fori_loop(0, width // 256, one, 0)

    def normalize():
        for step in range(1, plan.shards):
            small_copy(step).wait_recv()
        rest = jnp.zeros((8, width - LANES), jnp.float32)
        whole = jnp.zeros((8, width), jnp.float32)
        for number in range(plan.shards):
            wide = jnp.concatenate([small_all[number], rest], axis=1)
            whole = whole + pltpu.roll(wide, number * rows, 1)
        vectors[...] = whole
        step_rows = min(length, 128)

        def some(at, carry):
            some_rows = pl.ds(pl.multiple_of(at * step_rows, step_rows), step_rows)
            centred = inner_resid[some_rows, :]
            centred = centred - jnp.mean(centred, axis=1, keepdims=True)
            inverse = lax.rsqrt(jnp.mean(centred * centred, axis=1, keepdims=True) + EPSILON)
            amount = centred * inverse * vectors[0:1, :] + vectors[1:2, :]
            normed[some_rows, :] = amount
            normed_low[some_rows, :] = amount.astype(jnp.bfloat16)
            return carry

        lax.fori_loop(0, length // step_rows, some, 0)
        for copy in copies:
            copy.start()

    tiles = 2 * plan.width // width

    def hidden_load(mat):
        return pltpu.make_async_copy(full[mat], hidden_weight, weight_sem)

    def hidden_copy(which, at):
        span = pl.ds(pl.multiple_of(at * (width // 2), LANES), width // 2)
        return pltpu.make_async_copy(
            hidden_near[which].at[:, span], hidden_far[which].at[:, span], hidden_sem.at[which, at]
        )

    def fetch_hidden(mat):
        await_core(mat)
        hidden_load(mat).start()

    def open_gate():
        hidden_load(1).wait()

        def one(at, carry):
            span = pl.ds(pl.multiple_of(at * (width // 2), LANES), width // 2)
            rows_of = product(normed_low[...], hidden_weight[:, span], 1, 0)
            gate_rows[:, span] = rows_of
            gate_low[:, span] = rows_of.astype(jnp.bfloat16)
            hidden_copy(0, at).start()
            return carry

        lax.fori_loop(0, tiles, one, 0)

    def activate():
        hidden_load(2).wait()

        def one(at, carry):
            span = pl.ds(pl.multiple_of(at * (width // 2), LANES), width // 2)
            upward = product(normed_low[...], hidden_weight[:, span], 1, 0)
            gate = gate_rows[:, span]
            upward_low[:, span] = upward.astype(jnp.bfloat16)
            active[:, span] = (gate / (1.0 + jnp.exp(-gate)) * upward).astype(jnp.bfloat16)
            hidden_copy(1, at).start()
            hidden_copy(2, at).start()
            return carry

        lax.fori_loop(0, tiles, one, 0)

    outer_copies = [
        pltpu.make_async_copy(here, far, outer_sem.at[at])
        for at, (here, far) in enumerate(zip(near[15:], results[15:]))
    ]

    def close():
        depth = plan.width // width
        loads = [
            pltpu.make_async_copy(
                full[3].at[pl.ds(at * width, width), :],
                down_near.at[pl.ds(at * width, width), :],
                down_sem.at[at],
            )
            for at in range(depth)
        ]
        for load in loads:
            load.start()
        block = min(length, 256)
        for at in range(depth):
            loads[at].wait()

            def some(number, carry, at=at):
                some_rows = pl.ds(pl.multiple_of(number * block, block), block)
                base = normed if at == 0 else outer_grad
                outer_grad[some_rows, :] = base[some_rows, :] + product(
                    active[some_rows, at * width : (at + 1) * width],
                    down_near[at * width : (at + 1) * width, :], 1, 0,
                )
                return carry

            lax.fori_loop(0, length // block, some, 0)
        gain, shift = vectors[2:3, :], vectors[3:4, :]
        step_rows = min(length, 128)

        def both(at, carry):
            gain_sum, shift_sum = carry
            some_rows = pl.ds(pl.multiple_of(at * step_rows, step_rows), step_rows)
            centred = outer_grad[some_rows, :]
            centred = centred - jnp.mean(centred, axis=1, keepdims=True)
            inverse = lax.rsqrt(jnp.mean(centred * centred, axis=1, keepdims=True) + EPSILON)
            normalized = centred * inverse
            layer_output[some_rows, :] = (normalized * gain + shift).astype(jnp.bfloat16)
            upstream = cotangent[some_rows, :].astype(jnp.float32)
            gain_sum += jnp.sum(upstream * normalized, axis=0, keepdims=True)
            shift_sum += jnp.sum(upstream, axis=0, keepdims=True)
            scaled = upstream * gain
            back = inverse * (
                scaled
                - jnp.mean(scaled, axis=1, keepdims=True)
                - normalized * jnp.mean(scaled * normalized, axis=1, keepdims=True)
            )
            outer_grad[some_rows, :] = back
            result_grad[some_rows, :] = back.astype(jnp.bfloat16)
            return gain_sum, shift_sum

        nothing = jnp.zeros((1, width), jnp.float32)
        gain_sum, shift_sum = lax.fori_loop(0, length // step_rows, both, (nothing, nothing))
        sums[...] = jnp.zeros_like(sums)
        sums[2:3, :] = gain_sum
        sums[3:4, :] = shift_sum
        sums[4:5, :] = vectors[0:1, :]
        for copy in outer_copies:
            copy.start()

    items = [(mat, number) for mat in range(4) for number in range(1, chips)]
    events = [
        (at + SLACK * step, -step, functools.partial(relay, *item, step))
        for at, item in enumerate(items)
        for step in range(plan.levels + 1)
    ]
    ready = chips - 1 + SLACK * plan.levels
    for late, work in (
        (0, fetch_weight),
        (1, project),
        (2, functools.partial(attend, 0, pairs // 2)),
        (3, functools.partial(attend, pairs // 2, pairs)),
        (4, mix),
        (4, normalize),
    ):
        events.append((ready + late, 1, work))
    ahead = chips - 1
    for due, work in (
        (ready + ahead, functools.partial(fetch_hidden, 1)),
        (max(ready + ahead, ready + 5), open_gate),
        (max(ready + 2 * ahead, ready + 5), functools.partial(fetch_hidden, 2)),
        (max(ready + 2 * ahead, ready + 5), activate),
    ):
        events.append((due, 2, work))
    for _, _, event in sorted(events, key=lambda event: event[:2]):
        event()

    await_core(3)
    close()
    for copy in sent:
        copy.wait_send()
    for mat in range(4):
        along(mat, lambda copy: copy.wait_send())
        for number in range(1, chips):
            on(mat, number, lambda copy: copy.wait_send())
    for copy in copies:
        copy.wait()
    for which in range(3):
        for at in range(tiles):
            hidden_copy(which, at).wait()
    for copy in outer_copies:
        copy.wait()


def gather_weights(plan, own, small, carried):
    hbm = pl.BlockSpec(memory_space=pl.ANY)
    vmem = pl.BlockSpec(memory_space=pltpu.VMEM)
    dma = pltpu.SemaphoreType.DMA
    shapes = [
        jax.ShapeDtypeStruct((array.shape[0] * plan.shards, array.shape[1]), array.dtype)
        for array in own
    ]
    gaps = plan.chips - 1
    crossing = plan.replicas - 1
    length, width = carried[0].shape
    wide, low = jnp.float32, jnp.bfloat16
    results = (
        [jax.ShapeDtypeStruct((length, width), low)] * 4
        + [
            jax.ShapeDtypeStruct((width // HD, length), wide),
            jax.ShapeDtypeStruct((length, width), wide),
        ]
        + [jax.ShapeDtypeStruct((length, LANES), wide)] * 3
        + [
            jax.ShapeDtypeStruct((length, width), wide),
            jax.ShapeDtypeStruct((length, width), low),
            jax.ShapeDtypeStruct((8, width), wide),
        ]
        + [jax.ShapeDtypeStruct((length, plan.width), low)] * 3
        + [
            jax.ShapeDtypeStruct((length, width), wide),
            jax.ShapeDtypeStruct((length, width), low),
            jax.ShapeDtypeStruct((length, width), low),
            jax.ShapeDtypeStruct((8, width), wide),
        ]
    )
    return pl.pallas_call(
        functools.partial(gather_kernel, plan),
        out_shape=shapes + [jax.ShapeDtypeStruct((plan.shards,) + small.shape, small.dtype)]
        + results,
        in_specs=[hbm] * 4 + [vmem] + [hbm] * len(carried),
        out_specs=[hbm] * 4 + [vmem] + [hbm] * len(results),
        scratch_shapes=[pltpu.VMEM(array.shape, array.dtype) for array in own]
        + [
            dma((4,)),
            dma((4,)),
            dma((plan.shards - 1,)),
            dma((plan.shards - 1,)),
            dma((4, plan.chips, 2, plan.orders)),
            dma((4, plan.chips, plan.orders)),
            dma((4, gaps, plan.orders, crossing)),
            dma((4, gaps, plan.orders, crossing)),
            dma((4, plan.chips)),
            dma((4, plan.chips)),
        ]
        + [pltpu.VMEM(array.shape, array.dtype) for array in carried]
        + [pltpu.VMEM(result.shape, result.dtype) for result in results]
        + [
            pltpu.VMEM(shapes[0].shape, low),
            pltpu.VMEM((length, length), wide),
            dma((len(carried),)),
            dma,
            dma((12,)),
            pltpu.VMEM(shapes[1].shape, low),
            pltpu.VMEM((length, plan.width), wide),
            dma((3, 2 * plan.width // width)),
            pltpu.VMEM(shapes[3].shape, low),
            dma((plan.width // width,)),
            dma((4,)),
        ],
        compiler_params=pltpu.CompilerParams(
            collective_id=0, has_side_effects=True, vmem_limit_bytes=VMEM_LIMIT
        ),
        name="gather_weights",
    )(*own, small, *carried)


def back_pair(pair, query, key, value, upper, logsum, mask_bias, tables, joined_low, width):
    length = query.shape[0]
    block = min(length, 256)
    span = pl.ds(pl.multiple_of(pair * LANES, LANES), LANES)
    lane = lax.broadcasted_iota(jnp.int32, (1, LANES), 1)
    keys, values = key[:, span], value[:, span]
    query_parts = [0.0] * (length // block)
    key_total = value_total = 0.0
    for half in range(LANES // HD):
        pick = jnp.where(lane // HD == half, 1.0, 0.0).astype(jnp.bfloat16)
        scaled = pick * jnp.bfloat16(1.0 / math.sqrt(HD))
        keys_scaled = keys * scaled
        rowsum = logsum[pl.ds(pair * (LANES // HD) + half, 1), :]
        for at in range(length // block):
            rows = slice(at * block, (at + 1) * block)
            queries_scaled = query[rows, span] * scaled
            grads = upper[rows, span] * pick
            scores = product(keys, queries_scaled, 1, 1) + mask_bias[:, rows]
            probs = jnp.exp(scores - rowsum[:, rows])
            dprobs = product(values, grads, 1, 1)
            dots = jnp.sum(probs * dprobs, axis=0, keepdims=True)
            score_grad = (probs * (dprobs - dots)).astype(jnp.bfloat16)
            value_total += product(probs.astype(jnp.bfloat16), grads, 1, 0)
            key_total += product(score_grad, queries_scaled, 1, 0)
            query_parts[at] += product(score_grad, keys_scaled, 0, 0)
    cosine, before, after = tables

    def unrotate(grad, rows):
        return (
            grad * cosine[rows, :]
            - pltpu.roll(grad, LANES - HD // 2, 1) * before[rows, :]
            - pltpu.roll(grad, HD // 2, 1) * after[rows, :]
        ).astype(jnp.bfloat16)

    for at, part in enumerate(query_parts):
        rows = slice(at * block, (at + 1) * block)
        joined_low[rows, span] = unrotate(part, rows)
    everything = slice(0, length)
    joined_low[:, pl.ds(pl.multiple_of(width + pair * LANES, LANES), LANES)] = unrotate(
        key_total, everything
    )
    joined_low[:, pl.ds(pl.multiple_of(2 * width + pair * LANES, LANES), LANES)] = (
        value_total.astype(jnp.bfloat16)
    )


def sum_kernel(plan, *refs):
    (gate_far, up_far, active_far, gate_weight, up_weight, down_weight, attention) = refs[:7]
    carried = refs[7:23]
    outs, small_out, input_grad = refs[23:27], refs[27], refs[28]
    (pool, mate_in, rep_in, z_in, final, small_in, out_sem, small_sem, mate_send, mate_recv,
     rep_send, rep_recv, z_send, z_recv, last_send, last_recv) = refs[29:45]
    here = refs[45:61]
    (weight, gate_low, mask_bias, across, branch, upper, small, upward_low, active, fetch_sem,
     tile_sem, weight_sem, result_sem) = refs[61:]
    (query, key, value, attended, logsum, marks, segment_across, cosine, before, after, tokens,
     inner_resid, grad, result_grad, normed_low, sums) = here
    rep, shard = lax.axis_index("rep"), lax.axis_index("shard")
    chips, piece, levels = plan.chips, plan.piece, plan.levels
    place, core = lax.div(shard, 2), lax.rem(shard, 2)
    mate = place * 2 + (1 - core)
    rows = pool.shape[2]
    total = plan.replicas * plan.shards
    early = 3 * chips
    count = 4 * chips
    length, width = query.shape
    pairs = width // LANES
    groups = plan.width // width
    tile = width // 2
    low_type, wide_type = jnp.bfloat16, jnp.float32
    gaps = list(range(1, chips)) + [0]
    held = pool
    joined_low = gate_low

    def slab_at(gap, which):
        return lax.rem(place + gap, chips) * 2 + which

    def stage(turn):
        return 4 + turn % 3

    def scatter(turn, slab, span, block):
        gap = lax.rem(lax.div(slab, 2) - place + chips, chips)
        other = lax.rem(slab + core, 2)
        pool[turn + other * (stage(turn) - turn), gap, :, span] = block.astype(low_type)

    def give(turn, gap):
        remote(
            pool.at[stage(turn), gap], mate_in.at[turn, gap],
            mate_send.at[turn, gap], mate_recv.at[turn, gap], rep, mate,
        ).start()

    fetches = [
        pltpu.make_async_copy(far, near, fetch_sem.at[at])
        for at, (far, near) in enumerate(zip(carried, here))
    ]
    late = fetches[:11]
    soon = fetches[11:]
    for fetch in soon + late:
        fetch.start()

    quarter = max(chips // groups, 1)
    home = lax.rem(lax.div(place, quarter), groups)

    def tile_start(at):
        group = lax.rem(home + 1 + lax.div(at, 2), groups)
        return group * width + lax.rem(at, 2) * tile

    def slot_columns(left, slot):
        return pl.ds(pl.multiple_of(left + slot * tile, LANES), tile)

    def slot_rows(slot):
        return pl.ds(pl.multiple_of(slot * tile, LANES), tile)

    tail = pl.ds(4 * tile, width)

    def tile_copies(at):
        slot = lax.rem(at, 2)
        span = pl.ds(pl.multiple_of(tile_start(at), LANES), tile)
        pairs_of = (
            (gate_far.at[:, span], gate_low.at[:, span]),
            (up_far.at[:, span], upward_low.at[:, span]),
            (active_far.at[:, span], active.at[slot]),
            (down_weight.at[span, :], weight.at[slot_rows(slot), tail]),
        )
        return [
            pltpu.make_async_copy(far, near, tile_sem.at[number, slot])
            for number, (far, near) in enumerate(pairs_of)
        ]

    def lift_copies(at):
        slot = lax.rem(at, 2)
        span = pl.ds(pl.multiple_of(at * tile, LANES), tile)
        pairs_of = (
            (gate_weight.at[:, span], weight.at[:, slot_columns(0, slot)]),
            (up_weight.at[:, span], weight.at[:, slot_columns(2 * tile, slot)]),
        )
        return [
            pltpu.make_async_copy(far, near, tile_sem.at[4 + number, slot])
            for number, (far, near) in enumerate(pairs_of)
        ]

    for copy in tile_copies(0):
        copy.start()
    greet_all(plan, rep, shard)
    for fetch in soon:
        fetch.wait()
    across[...] = normed_low[...].T

    def small_go(step, carry):
        other = lax.rem(rep * plan.shards + shard + step, total)
        other_rep, other_shard = lax.div(other, plan.shards), lax.rem(other, plan.shards)
        remote(
            small.at[other_shard], small_in.at[step - 1], small_sem.at[0], small_sem.at[1],
            other_rep, other_shard,
        ).start()
        return carry

    def whole_mate(turn, gap):
        return remote(
            mate_in.at[turn, gap], mate_in.at[turn, gap],
            mate_send.at[turn, gap], mate_recv.at[turn, gap], rep, mate,
        )

    def cross(turn, gap, order, step):
        far = plan.flip(rep, plan.ways[order][step])
        at = plan.halve_at(step)
        copies = [
            remote(
                held.at[turn, gap, :, pl.ds(plan.column(section, order), piece)],
                rep_in.at[turn, gap, order, at + number],
                rep_send.at[turn, gap, order, at + number],
                rep_recv.at[turn, gap, order, at + number],
                far, shard,
            )
            for number, section in enumerate(plan.halve(far, order, step))
        ]
        return copies, [plan.column(section, order) for section in plan.halve(rep, order, step)]

    wide_piece = plan.orders * piece
    own_columns = pl.ds(pl.multiple_of(rep * wide_piece, LANES), wide_piece)

    def z_copy(turn, gap):
        return remote(
            held.at[turn, gap, :, own_columns],
            z_in.at[turn, gap - 1],
            z_send.at[turn, gap - 1], z_recv.at[turn, gap - 1],
            rep, slab_at(gap, core),
        )

    def item_of(number):
        return lax.div(number, chips), lax.rem(lax.rem(number, chips) + 1, chips)

    def advance(number, step):
        turn, gap = item_of(number)
        if step == 0:
            whole_mate(turn, gap).wait_recv()

            def add(at, carry):
                span = pl.ds(pl.multiple_of(at * piece, LANES), piece)
                held[turn, gap, :, span] = (
                    held[turn, gap, :, span].astype(jnp.float32)
                    + mate_in[turn, gap, :, span].astype(jnp.float32)
                ).astype(jnp.bfloat16)
                return carry

            lax.fori_loop(0, plan.width // piece, add, 0)
        else:
            for order in range(plan.orders):
                copies, columns = cross(turn, gap, order, step - 1)
                at = plan.halve_at(step - 1)
                for index, (copy, column) in enumerate(zip(copies, columns)):
                    copy.wait_recv()
                    span = pl.ds(column, piece)
                    held[turn, gap, :, span] = (
                        held[turn, gap, :, span].astype(jnp.float32)
                        + rep_in[turn, gap, order, at + index].astype(jnp.float32)
                    ).astype(jnp.bfloat16)
        if step < levels:
            for order in range(plan.orders):
                for copy in cross(turn, gap, order, step)[0]:
                    copy.start()
        else:
            @pl.when(gap > 0)
            def _():
                z_copy(turn, gap).start()

    def spread(turn, order, step):
        far = plan.flip(rep, plan.ways[order][step])
        at = plan.grow_at(step)
        return [
            remote(
                final.at[turn, :, pl.ds(plan.column(section, order), piece)],
                final.at[turn, :, pl.ds(plan.column(section, order), piece)],
                last_send.at[turn, order, at + number],
                last_recv.at[turn, order, at + number],
                far, shard,
            )
            for number, section in enumerate(plan.grow(rep, order, step))
        ]

    def await_spread(turn, order, step):
        far = plan.flip(rep, plan.ways[order][step])
        at = plan.grow_at(step)
        for number, section in enumerate(plan.grow(far, order, step)):
            there = final.at[turn, :, pl.ds(plan.column(section, order), piece)]
            remote(
                there, there,
                last_send.at[turn, order, at + number],
                last_recv.at[turn, order, at + number],
                far, shard,
            ).wait_recv()

    def finish(turn, step):
        if step == 0:
            for gap in range(1, chips):
                z_copy(turn, gap).wait_recv()
            for order in range(plan.orders):
                span = pl.ds(plan.column(rep, order), piece)
                part = pl.ds(order * piece, piece)
                amount = held[turn, 0, :, span].astype(jnp.float32)
                for gap in range(1, chips):
                    amount = amount + z_in[turn, gap - 1, :, part].astype(jnp.float32)
                final[turn, :, span] = amount.astype(jnp.bfloat16)
        else:
            for order in range(plan.orders):
                await_spread(turn, order, step - 1)
        if step < levels:
            for order in range(plan.orders):
                for copy in spread(turn, order, step):
                    copy.start()

    def tick(now):
        for step in reversed(range(levels + 1)):
            behind = now - (SLACK * (levels + step + 1) + chips - 1)

            @pl.when((behind >= 0) & (lax.rem(behind + chips, chips) == 0) & (behind < count))
            def _(behind=behind, step=step):
                finish(lax.div(behind, chips), step)

        for step in reversed(range(levels + 1)):
            number = now - SLACK * step

            @pl.when((number >= 0) & (number < count))
            def _(number=number, step=step):
                advance(number, step)

    block = min(length, 256)

    def hidden(at, carry):
        slot = lax.rem(at, 2)
        for copy in tile_copies(at):
            copy.wait()

        @pl.when(at + 1 < 2 * groups)
        def _():
            for copy in tile_copies(at + 1):
                copy.start()

        start = tile_start(at)
        span = pl.ds(pl.multiple_of(start, LANES), tile)
        down_tile = weight[slot_rows(slot), tail]

        def some(number, carry):
            some_rows = pl.ds(pl.multiple_of(number * block, block), block)
            active_grad = product(result_grad[some_rows, :], down_tile, 1, 1)
            gate = gate_low[some_rows, span].astype(wide_type)
            upward = upward_low[some_rows, span].astype(wide_type)
            sigmoid = 1.0 / (1.0 + jnp.exp(-gate))
            gate_low[some_rows, span] = (
                active_grad * upward * sigmoid * (1.0 + gate * (1.0 - sigmoid))
            ).astype(low_type)
            upward_low[some_rows, span] = (active_grad * (gate * sigmoid)).astype(low_type)
            return carry

        lax.fori_loop(0, length // block, some, 0)
        down_part = product(active[slot], result_grad[...], 0, 0)
        per = plan.width // width
        for number in range(tile // rows):
            chunk = lax.div(start, rows) + number
            left = pl.multiple_of(lax.rem(chunk, per) * width, LANES)
            scatter(
                0, lax.div(chunk, per), pl.ds(left, width),
                down_part[number * rows : (number + 1) * rows, :],
            )
        for turn, low in ((1, gate_low), (2, upward_low)):
            for some_half in range(2):
                top = some_half * (width // 2)
                part = product(across[top : top + width // 2, :], low[:, span], 1, 0)
                for number in range(width // 2 // rows):
                    scatter(
                        turn, top // rows + number, span,
                        part[number * rows : (number + 1) * rows, :],
                    )
        if chips == groups:
            @pl.when(lax.rem(at, 2) == 1)
            def _():
                number = lax.div(at, 2)
                give(0, lax.rem(number + 1, chips))

                @pl.when(number > 0)
                def _():
                    tick(number - 1)
        return carry

    lax.fori_loop(0, 2 * groups, hidden, 0)
    done = chips - 1 if chips == groups else 0
    for copy in lift_copies(0):
        copy.start()
    for gap in gaps:
        if chips != groups:
            give(0, gap)
    for turn in (1, 2):
        for gap in gaps:
            give(turn, gap)
    weight_load = pltpu.make_async_copy(attention, weight, weight_sem)
    for fetch in late:
        fetch.wait()
    mask_bias[...] = jnp.where(marks[:, 0:1] == segment_across[0:1, :], 0.0, NEG_LARGE)

    def lift(at, carry):
        slot = lax.rem(at, 2)
        for copy in lift_copies(at):
            copy.wait()

        @pl.when(at + 1 < 2 * groups)
        def _():
            for copy in lift_copies(at + 1):
                copy.start()

        span = pl.ds(pl.multiple_of(at * tile, LANES), tile)

        def some(number, carry):
            some_rows = pl.ds(pl.multiple_of(number * block, block), block)
            grad[some_rows, :] += product(
                gate_low[some_rows, span], weight[:, slot_columns(0, slot)], 1, 1
            ) + product(
                upward_low[some_rows, span], weight[:, slot_columns(2 * tile, slot)], 1, 1
            )
            return carry

        return lax.fori_loop(0, length // block, some, carry)

    def norm_back():
        gain = sums[4:5, :]
        step_rows = min(length, 128)

        def some(number, carry):
            gain_sum, shift_sum = carry
            some_rows = pl.ds(pl.multiple_of(number * step_rows, step_rows), step_rows)
            centred = inner_resid[some_rows, :]
            centred = centred - jnp.mean(centred, axis=1, keepdims=True)
            inverse = lax.rsqrt(jnp.mean(centred * centred, axis=1, keepdims=True) + EPSILON)
            normalized = centred * inverse
            upstream = grad[some_rows, :]
            gain_sum += jnp.sum(upstream * normalized, axis=0, keepdims=True)
            shift_sum += jnp.sum(upstream, axis=0, keepdims=True)
            scaled = upstream * gain
            back = inverse * (
                scaled
                - jnp.mean(scaled, axis=1, keepdims=True)
                - normalized * jnp.mean(scaled * normalized, axis=1, keepdims=True)
            )
            grad[some_rows, :] = back
            branch[some_rows, :] = back.astype(low_type)
            return gain_sum, shift_sum

        nothing = jnp.zeros((1, width), wide_type)
        gain_sum, shift_sum = lax.fori_loop(0, length // step_rows, some, (nothing, nothing))
        sums[0:1, :] = gain_sum
        sums[1:2, :] = shift_sum
        vectors = sums[...]
        for number in range(plan.shards):
            small[number] = pltpu.roll(vectors, (width - rows * number) % width, 1)[:, :LANES]

    def columns_loop(number, work):
        def one(at, carry):
            work(at)
            return carry

        lax.fori_loop(0, number, one, 0)

    def raise_up():
        weight_load.wait()

        def one(at):
            span = pl.ds(pl.multiple_of(at * 256, 256), 256)
            upper[:, span] = product(
                branch[...], weight[span, 3 * width : 4 * width], 1, 1
            ).astype(low_type)

        columns_loop(width // 256, one)

    def weigh(left, right, lefts):
        def one(at):
            span = pl.ds(pl.multiple_of(left + at * tile, LANES), tile)
            source = pl.ds(pl.multiple_of(at * tile, LANES), tile)
            for some_half in range(2):
                top = some_half * (width // 2)
                part = product(across[top : top + width // 2, :], right[:, source], 1, 0)
                for number in range(width // 2 // rows):
                    scatter(
                        3, top // rows + number, span, part[number * rows : (number + 1) * rows, :]
                    )

        columns_loop(lefts, one)

    def middle(at, carry):
        @pl.when(at < LIFTS)
        def _():
            lax.fori_loop(at * 2 * groups // LIFTS, (at + 1) * 2 * groups // LIFTS, lift, 0)

        @pl.when(at == LIFTS)
        def _():
            weight_load.start()
            norm_back()
            lax.fori_loop(1, total, small_go, 0)
            raise_up()

        @pl.when((at > LIFTS) & (at < LIFTS + 1 + pairs))
        def _():
            back_pair(
                at - LIFTS - 1, query, key, value, upper, logsum, mask_bias, (cosine, before, after),
                joined_low, width,
            )

        @pl.when(at + done < early)
        def _():
            tick(at + done)
        return carry

    lax.fori_loop(0, max(LIFTS + 1 + pairs, early - done), middle, 0)
    for gap in gaps:
        whole_mate(0, gap).wait_send()
    across[...] = attended[...].T
    weigh(3 * width, branch, width // tile)
    across[...] = tokens[...].T
    weigh(0, joined_low, 3 * width // tile)
    for gap in gaps:
        give(3, gap)

    def back(at):
        low = pl.ds(pl.multiple_of(at * 256, 256), 256)
        result_grad[:, low] = (
            grad[:, low] + product(joined_low[:, 0 : 3 * width], weight[low, 0 : 3 * width], 1, 1)
        ).astype(jnp.bfloat16)

    columns_loop(width // 256, back)
    result_copy = pltpu.make_async_copy(result_grad, input_grad, result_sem)
    result_copy.start()

    def late_tick(now, carry):
        tick(now)
        return carry

    lax.fori_loop(early, count + SLACK * (2 * levels + 1), late_tick, 0)

    everything = remote(small_in, small_in, small_sem.at[0], small_sem.at[1], rep, mate)
    everything.wait_recv()

    def gain_of(at, amount):
        return amount + small_in[at]

    small_out[...] = lax.fori_loop(0, total - 1, gain_of, small[shard])
    everything.wait_send()
    for turn in range(4):
        pltpu.make_async_copy(final.at[turn], outs[turn], out_sem.at[turn]).start()

    def drain(number, carry):
        turn, gap = item_of(number)

        @pl.when(turn > 0)
        def _():
            whole_mate(turn, gap).wait_send()
        for order in range(plan.orders):
            for step in range(levels):
                for copy in cross(turn, gap, order, step)[0]:
                    copy.wait_send()

        @pl.when(gap > 0)
        def _():
            z_copy(turn, gap).wait_send()
        return carry

    lax.fori_loop(0, count, drain, 0)
    for turn in range(4):
        for order in range(plan.orders):
            for step in range(levels):
                for copy in spread(turn, order, step):
                    copy.wait_send()
        pltpu.make_async_copy(final.at[turn], outs[turn], out_sem.at[turn]).wait()
    result_copy.wait()


def sum_grads(plan, streamed, carried):
    hbm = pl.BlockSpec(memory_space=pl.ANY)
    vmem = pl.BlockSpec(memory_space=pltpu.VMEM)
    dma = pltpu.SemaphoreType.DMA
    chips, gaps, crossing = plan.chips, plan.chips - 1, plan.replicas - 1
    length, width = carried[0].shape
    rows = width // plan.shards
    low, wide = jnp.bfloat16, jnp.float32
    total = plan.replicas * plan.shards
    return pl.pallas_call(
        functools.partial(sum_kernel, plan),
        out_shape=[jax.ShapeDtypeStruct((rows, plan.width), low)] * 4
        + [
            jax.ShapeDtypeStruct((8, LANES), wide),
            jax.ShapeDtypeStruct((length, width), low),
        ],
        in_specs=[hbm] * (len(streamed) + len(carried)),
        out_specs=[hbm] * 4 + [vmem, hbm],
        scratch_shapes=[
            pltpu.VMEM((7, chips, rows, plan.width), low),
            pltpu.VMEM((4, chips, rows, plan.width), low),
            pltpu.VMEM((4, chips, plan.orders, crossing, rows, plan.piece), low),
            pltpu.VMEM((4, gaps, rows, plan.orders * plan.piece), low),
            pltpu.VMEM((4, rows, plan.width), low),
            pltpu.VMEM((total - 1, 8, LANES), wide),
            dma((4,)),
            dma((2,)),
            dma((4, chips)),
            dma((4, chips)),
            dma((4, chips, plan.orders, crossing)),
            dma((4, chips, plan.orders, crossing)),
            dma((4, gaps)),
            dma((4, gaps)),
            dma((4, plan.orders, crossing)),
            dma((4, plan.orders, crossing)),
        ]
        + [pltpu.VMEM(array.shape, array.dtype) for array in carried]
        + [
            pltpu.VMEM((width, 4 * width), low),
            pltpu.VMEM((length, plan.width), low),
            pltpu.VMEM((length, length), wide),
            pltpu.VMEM((width, length), low),
            pltpu.VMEM((length, width), low),
            pltpu.VMEM((length, width), low),
            pltpu.VMEM((plan.shards, 8, LANES), wide),
            pltpu.VMEM((length, plan.width), low),
            pltpu.VMEM((2, length, width // 2), low),
            dma((len(carried),)),
            dma((6, 2)),
            dma,
            dma,
        ],
        compiler_params=pltpu.CompilerParams(
            collective_id=1, has_side_effects=True, vmem_limit_bytes=VMEM_MOST
        ),
        name="sum_grads",
    )(*streamed, *carried)


def on_device(
    tokens,
    joined_weight,
    mixing_weight,
    gate_weight,
    up_weight,
    down_weight,
    inner_gain,
    inner_shift,
    outer_gain,
    outer_shift,
    segments,
    positions,
    cotangent,
):
    replicas, shards = lax.axis_size("rep"), lax.axis_size("shard")
    plan = Plan(gate_weight.shape[1], replicas, shards)
    part_rows = joined_weight.shape[0]
    own_vectors = jnp.stack([inner_gain, inner_shift, outer_gain, outer_shift]).astype(jnp.float32)
    own_vectors = jnp.pad(own_vectors, ((0, 4), (0, LANES - part_rows)))
    length, model_width = tokens.shape
    halves = np.arange(LANES) % (HD // 2)
    rates = np.float32(1000.0) ** (-(2.0 * halves.astype(np.float32)) / np.float32(HD))
    marks = jnp.where(
        jnp.arange(LANES)[None, :] == 0, segments[0][:, None], positions[0][:, None]
    )
    (
        attention_full,
        gate_full,
        upward_full,
        down_full,
        _,
        query_low,
        key_low,
        value_low,
        attended_low,
        logsum,
        inner_resid,
        cosine_wide,
        before,
        after,
        _,
        normed_low,
        _,
        gate_low,
        upward_low,
        active_low,
        outer_grad,
        result_grad,
        layer_output,
        sums,
    ) = gather_weights(
        plan,
        (
            jnp.concatenate([joined_weight, mixing_weight], axis=1),
            gate_weight,
            up_weight,
            down_weight,
        ),
        own_vectors,
        (tokens, marks, segments, jnp.asarray(np.tile(rates[None, :], (8, 1))), cotangent),
    )
    down_sum, gate_sum, up_sum, attention_sum, small_sum, input_grad = sum_grads(
        plan,
        (
            gate_low,
            upward_low,
            active_low,
            gate_full,
            upward_full,
            down_full,
            attention_full,
        ),
        (
            query_low,
            key_low,
            value_low,
            attended_low,
            logsum,
            marks,
            segments,
            cosine_wide,
            before,
            after,
            tokens,
            inner_resid,
            outer_grad,
            result_grad,
            normed_low,
            sums,
        ),
    )
    down_sum = down_sum.reshape(part_rows, -1, model_width).transpose(1, 0, 2)
    full = jnp.float32
    return (
        layer_output,
        input_grad,
        attention_sum[:, : joined_weight.shape[1]].astype(full),
        attention_sum[:, joined_weight.shape[1] :].astype(full),
        gate_sum.astype(full),
        up_sum.astype(full),
        down_sum.reshape(down_weight.shape).astype(full),
        small_sum[0, :part_rows],
        small_sum[1, :part_rows],
        small_sum[2, :part_rows],
        small_sum[3, :part_rows],
    )


def solution(mesh):
    placed = (
        P(("rep", "shard"), None),
        P("shard", None),
        P("shard", None),
        P("shard", None),
        P("shard", None),
        P("shard", None),
        P("shard"),
        P("shard"),
        P("shard"),
        P("shard"),
        P(("rep", "shard"), None),
        P(("rep", "shard"), None),
        P(("rep", "shard"), None),
    )
    return jax.shard_map(
        on_device,
        mesh=mesh,
        in_specs=placed,
        out_specs=(
            P(("rep", "shard"), None),
            P(("rep", "shard"), None),
            P("shard", None),
            P("shard", None),
            P("shard", None),
            P("shard", None),
            P("shard", None),
            P("shard"),
            P("shard"),
            P("shard"),
            P("shard"),
        ),
        check_vma=False,
    )
```

```python
import functools
import math

import jax
import jax.numpy as jnp
import numpy as np
from jax import lax
from jax.experimental import pallas as pl
from jax.experimental.pallas import tpu as pltpu
from jax.sharding import PartitionSpec as P

H = 12
HD = 64

EPSILON = 1e-12
NEG_LARGE = -1e30
LANES = 128
MESH = pl.DeviceIdType.MESH
VMEM_LIMIT = 62 * 1024 * 1024
SLACK = 2
VMEM_MOST = 67043328
LIFTS = 2
AHEAD = 3


class Plan:
    def __init__(self, width, replicas, shards):
        self.replicas, self.shards = replicas, shards
        self.chips = shards // 2
        self.levels = replicas.bit_length() - 1
        self.orders = 2 if self.levels > 1 and width % (2 * replicas * LANES) == 0 else 1
        self.ways = (tuple(range(self.levels)), tuple(reversed(range(self.levels))))[: self.orders]
        self.piece = width // (replicas * self.orders)
        self.width = width

    def flip(self, rep, bit):
        return rep + (1 << bit) * (1 - 2 * lax.rem(lax.div(rep, 1 << bit), 2))

    def with_bits(self, rep, bits, number):
        for at, bit in enumerate(bits):
            had = lax.rem(lax.div(rep, 1 << bit), 2)
            rep = rep + (1 << bit) * (((number >> at) & 1) - had)
        return rep

    def column(self, rep, order):
        return pl.multiple_of((rep * self.orders + order) * self.piece, LANES)

    def grow(self, rep, order, step):
        bits = self.ways[order][:step]
        return [self.with_bits(rep, bits, number) for number in range(1 << step)]

    def grow_at(self, step):
        return (1 << step) - 1

    def halve(self, rep, order, step):
        bits = self.ways[order][step + 1 :]
        return [self.with_bits(rep, bits, number) for number in range(1 << len(bits))]

    def halve_at(self, step):
        return sum(1 << (self.levels - 1 - at) for at in range(step))


def peer(rep, shard):
    return {"rep": rep, "shard": shard}


def remote(src, dst, send, recv, rep, shard):
    return pltpu.make_async_remote_copy(
        src_ref=src,
        dst_ref=dst,
        send_sem=send,
        recv_sem=recv,
        device_id=peer(rep, shard),
        device_id_type=MESH,
    )


def greet_all(plan, rep, shard):
    barrier = pltpu.get_barrier_semaphore()
    total = plan.replicas * plan.shards

    def hello(step, carry):
        other = lax.rem(rep * plan.shards + shard + step, total)
        pl.semaphore_signal(
            barrier,
            inc=1,
            device_id=peer(lax.div(other, plan.shards), lax.rem(other, plan.shards)),
            device_id_type=MESH,
        )
        return carry

    lax.fori_loop(1, total, hello, 0)
    pl.semaphore_wait(barrier, total - 1)


def greet_near(plan, rep, shard):
    barrier = pltpu.get_barrier_semaphore()
    for step in range(1, plan.shards):
        pl.semaphore_signal(
            barrier,
            inc=1,
            device_id=peer(rep, lax.rem(shard + step, plan.shards)),
            device_id_type=MESH,
        )
    for bit in range(plan.levels):
        pl.semaphore_signal(
            barrier, inc=1, device_id=peer(plan.flip(rep, bit), shard), device_id_type=MESH
        )
    pl.semaphore_wait(barrier, plan.shards - 1 + plan.levels)


def product(left, right, left_axis, right_axis):
    return lax.dot_general(
        left, right, (((left_axis,), (right_axis,)), ((), ())), preferred_element_type=jnp.float32
    )


def forward_pair(pair, query, key, value, mask_bias, attended, logsum):
    length = query.shape[0]
    block = min(length, 256)
    span = pl.ds(pl.multiple_of(pair * LANES, LANES), LANES)
    lane = lax.broadcasted_iota(jnp.int32, (1, LANES), 1)
    keys, values = key[:, span], value[:, span]
    parts = [0.0] * (length // block)
    for half in range(LANES // HD):
        pick = jnp.where(lane // HD == half, 1.0, 0.0).astype(jnp.bfloat16)
        scaled = pick * jnp.bfloat16(1.0 / math.sqrt(HD))
        picked = values * pick
        for at in range(length // block):
            rows = slice(at * block, (at + 1) * block)
            scores = product(keys, query[rows, span] * scaled, 1, 1) + mask_bias[:, rows]
            highest = jnp.max(scores, axis=0, keepdims=True)
            shifted = jnp.exp(scores - highest)
            denominator = jnp.sum(shifted, axis=0, keepdims=True)
            logsum[pl.ds(pair * (LANES // HD) + half, 1), rows] = highest + jnp.log(denominator)
            probs = (shifted * (1.0 / denominator)).astype(jnp.bfloat16)
            parts[at] += product(probs, picked, 0, 0)
    for at, part in enumerate(parts):
        attended[at * block : (at + 1) * block, span] = part.astype(jnp.bfloat16)


def gather_kernel(plan, mixing_own, *refs):
    own, small = refs[:4], refs[4]
    carried = refs[5:10]
    full, small_all = refs[10:14], refs[14]
    results = refs[15:34]
    stages = refs[34:38]
    (load_sem, store_sem, small_send, small_recv, z_send, z_recv, rep_send, rep_recv, core_send,
     core_recv) = refs[38:48]
    tokens, marks, segment_across, rates, cotangent = refs[48:53]
    near = refs[53:72]
    (query, key, value, attended, logsum, inner_resid, cosine, before, after, normed, normed_low,
     vectors) = near[:12]
    hidden_near, hidden_far = near[12:15], results[12:15]
    gate_low, upward_low, active = hidden_near
    outer_grad, result_grad, layer_output, sums = near[15:]
    weight, mask_bias, fetch_sem, weight_sem, result_sem = refs[72:77]
    hidden_weight, gate_rows, hidden_sem, down_near, down_sem, outer_sem = refs[77:]
    rep, shard = lax.axis_index("rep"), lax.axis_index("shard")
    chips, piece = plan.chips, plan.piece
    place, core = lax.div(shard, 2), lax.rem(shard, 2)
    mate = place * 2 + (1 - core)
    rows = own[0].shape[0]
    length, width = tokens.shape
    pairs = width // LANES

    def part(ref, mat, top, section_rep, order):
        if mat < 3:
            return ref.at[
                pl.ds(pl.multiple_of(top, 8), rows),
                pl.ds(plan.column(section_rep, order), piece),
            ]
        per = own[3].shape[1] // piece
        section = section_rep * plan.orders + order
        return ref.at[
            pl.ds(pl.multiple_of(top + lax.div(section, per) * rows, 8), rows),
            pl.ds(pl.multiple_of(lax.rem(section, per) * piece, LANES), piece),
        ]

    def slab_part(mat, slab, section_rep, order):
        return part(full[mat], mat, slab * own[mat].shape[0], section_rep, order)

    def slab_of(mat, slab):
        deep = own[mat].shape[0]
        return full[mat].at[pl.ds(pl.multiple_of(slab * deep, 8), deep), :]

    sent = []

    def launch(copy):
        copy.start()
        sent.append(copy)

    mine = (stages[0],) + tuple(own[1:])
    joined_own = own[0].shape[1]
    loads = [
        pltpu.make_async_copy(own[0], stages[0].at[:, pl.ds(0, joined_own)], load_sem.at[0])
    ]
    loads += [pltpu.make_async_copy(own[mat], stages[mat], load_sem.at[mat]) for mat in range(1, 4)]
    loads.append(
        pltpu.make_async_copy(
            mixing_own, stages[0].at[:, pl.ds(joined_own, mixing_own.shape[1])], load_sem.at[4]
        )
    )
    for load in loads:
        load.start()
    fetches = [
        pltpu.make_async_copy(far, here, fetch_sem.at[at])
        for at, (far, here) in enumerate(zip(carried, refs[48:53]))
    ]
    for fetch in fetches:
        fetch.start()
    small_all[shard] = small[...]
    greet_near(plan, rep, shard)

    def small_copy(step):
        return remote(
            small, small_all.at[shard], small_send.at[step - 1], small_recv.at[step - 1],
            rep, lax.rem(shard + step, plan.shards),
        )

    fewest = jnp.minimum(place, chips - 1 - place)
    longer_above = jnp.where(2 * place < chips - 1, 1, 0)

    def nearest(number):
        inside = number <= 2 * fewest
        above = jnp.where(inside, number % 2, longer_above)
        distance = jnp.where(inside, (number + 1) // 2, number - fewest)
        return place + distance * (2 * above - 1), above

    def hop(mat, origin, down, order, source):
        return remote(
            source,
            slab_part(mat, origin * 2 + core, rep, order),
            z_send.at[mat, origin, down, order],
            z_recv.at[mat, origin, order],
            rep, (place + 1 - 2 * down) * 2 + core,
        )

    def own_hop(mat, down, order):
        return hop(mat, place, down, order, part(mine[mat], mat, 0, rep, order))

    def next_hop(mat, number, order):
        origin, above = nearest(number)
        there = slab_part(mat, origin * 2 + core, rep, order)
        return hop(mat, origin, above, order, there)

    def leads(down):
        return (place > 0) if down else (place < chips - 1)

    def goes_on(number):
        _, above = nearest(number)
        onward = place + 1 - 2 * above
        return (onward >= 0) & (onward < chips)

    def along(mat, act):
        for down in range(2):
            @pl.when(leads(down))
            def _(down=down):
                for order in range(plan.orders):
                    act(own_hop(mat, down, order))

    def on(mat, number, act):
        @pl.when(goes_on(number))
        def _():
            for order in range(plan.orders):
                act(next_hop(mat, number, order))

    def give(mat):
        launch(remote(
            mine[mat], slab_of(mat, shard), core_send.at[mat, 0], core_recv.at[mat, 0], rep, mate
        ))

    for load in (loads[0], loads[4]):
        load.wait()
    along(0, lambda copy: copy.start())
    give(0)
    for step in range(1, plan.shards):
        launch(small_copy(step))
    for mat in range(1, 4):
        give(mat)
    stores = []
    for mat in range(4):
        if mat > 0:
            loads[mat].wait()
        store = pltpu.make_async_copy(stages[mat], slab_of(mat, shard), store_sem.at[mat])
        store.start()
        stores.append(store)

    for fetch in fetches:
        fetch.wait()
    mask_bias[...] = jnp.where(marks[:, 0:1] == segment_across[0:1, :], 0.0, NEG_LARGE)
    angles = marks[:, 1:2].astype(jnp.float32) * rates[0:1, :]
    first = lax.broadcasted_iota(jnp.int32, (1, LANES), 1) % HD < HD // 2
    cosine[...] = jnp.cos(angles)
    sine = jnp.sin(angles)
    before[...] = jnp.where(first, -sine, 0.0)
    after[...] = jnp.where(first, 0.0, sine)

    def source(number):
        return nearest(number)[0] * 2 + core

    def exchange(mat, number, order, step):
        slab = source(number)
        far = plan.flip(rep, plan.ways[order][step])
        at = plan.grow_at(step)
        return [
            remote(
                slab_part(mat, slab, section, order),
                slab_part(mat, slab, section, order),
                rep_send.at[mat, number - 1, order, at + index],
                rep_recv.at[mat, number - 1, order, at + index],
                far, shard,
            )
            for index, section in enumerate(plan.grow(rep, order, step))
        ]

    def await_exchange(mat, number, order, step):
        slab = source(number)
        far = plan.flip(rep, plan.ways[order][step])
        at = plan.grow_at(step)
        for index, section in enumerate(plan.grow(far, order, step)):
            there = slab_part(mat, slab, section, order)
            remote(
                there, there,
                rep_send.at[mat, number - 1, order, at + index],
                rep_recv.at[mat, number - 1, order, at + index],
                far, shard,
            ).wait_recv()

    def relay(mat, number, step):
        for order in range(plan.orders):
            if step == 0:
                origin, _ = nearest(number)
                there = slab_part(mat, origin * 2 + core, rep, order)
                remote(
                    there, there, z_send.at[mat, origin, 0, order], z_recv.at[mat, origin, order],
                    rep, mate,
                ).wait_recv()
            else:
                await_exchange(mat, number, order, step - 1)
            if step < plan.levels:
                for copy in exchange(mat, number, order, step):
                    launch(copy)
        if step == 0:
            on(mat, number, lambda copy: copy.start())
            if number == 1 and mat + 1 < 4:
                along(mat + 1, lambda copy: copy.start())
        if step == plan.levels:
            there = slab_of(mat, source(number))
            launch(remote(
                there, there, core_send.at[mat, number], core_recv.at[mat, number], rep, mate
            ))

    def await_core(mat):
        stores[mat].wait()
        for number in range(chips):
            slab = (place if number == 0 else nearest(number)[0]) * 2 + (1 - core)
            there = slab_of(mat, slab)
            remote(
                there, there, core_send.at[mat, number], core_recv.at[mat, number], rep, mate
            ).wait_recv()

    weight_load = pltpu.make_async_copy(full[0], weight, weight_sem)

    def fetch_weight():
        await_core(0)
        weight_load.start()

    def project():
        weight_load.wait()
        tile = width // 2

        def columns(at):
            span = pl.ds(pl.multiple_of(at * tile, LANES), tile)
            return product(tokens[...], weight[:, span], 1, 0)

        def turned(at, carry):
            joined = columns(at)
            for down in range(tile // LANES):
                vector = joined[:, down * LANES : (down + 1) * LANES]
                spot = pl.ds(pl.multiple_of(lax.rem(at, 2) * tile + down * LANES, LANES), LANES)
                low = (
                    vector * cosine[...]
                    + pltpu.roll(vector, LANES - HD // 2, 1) * before[...]
                    + pltpu.roll(vector, HD // 2, 1) * after[...]
                ).astype(jnp.bfloat16)

                @pl.when(at < 2)
                def _():
                    query[:, spot] = low

                @pl.when(at >= 2)
                def _():
                    key[:, spot] = low
            return carry

        lax.fori_loop(0, 4, turned, 0)

        def plain(at, carry):
            value[:, pl.ds(pl.multiple_of(at * tile, LANES), tile)] = columns(at + 4).astype(
                jnp.bfloat16
            )
            return carry

        lax.fori_loop(0, 2, plain, 0)

    def attend(low, high):
        def one(pair, carry):
            forward_pair(pair, query, key, value, mask_bias, attended, logsum)
            return carry

        lax.fori_loop(low, high, one, 0)

    copies = [
        pltpu.make_async_copy(here, far, result_sem.at[at])
        for at, (here, far) in enumerate(zip(near[:12], results[:12]))
    ]

    def mix():
        def one(at, carry):
            span = pl.ds(pl.multiple_of(at * 256, 256), 256)
            across = pl.ds(pl.multiple_of(3 * width + at * 256, 256), 256)
            inner_resid[:, span] = tokens[:, span].astype(jnp.float32) + product(
                attended[...], weight[:, across], 1, 0
            )
            return carry

        lax.fori_loop(0, width // 256, one, 0)

    def normalize():
        for step in range(1, plan.shards):
            small_copy(step).wait_recv()
        rest = jnp.zeros((8, width - LANES), jnp.float32)
        whole = jnp.zeros((8, width), jnp.float32)
        for number in range(plan.shards):
            wide = jnp.concatenate([small_all[number], rest], axis=1)
            whole = whole + pltpu.roll(wide, number * rows, 1)
        vectors[...] = whole
        step_rows = min(length, 128)

        def some(at, carry):
            some_rows = pl.ds(pl.multiple_of(at * step_rows, step_rows), step_rows)
            centred = inner_resid[some_rows, :]
            centred = centred - jnp.mean(centred, axis=1, keepdims=True)
            inverse = lax.rsqrt(jnp.mean(centred * centred, axis=1, keepdims=True) + EPSILON)
            amount = centred * inverse * vectors[0:1, :] + vectors[1:2, :]
            normed[some_rows, :] = amount
            normed_low[some_rows, :] = amount.astype(jnp.bfloat16)
            return carry

        lax.fori_loop(0, length // step_rows, some, 0)
        for copy in copies:
            copy.start()

    tiles = 2 * plan.width // width

    def hidden_load(mat):
        return pltpu.make_async_copy(full[mat], hidden_weight, weight_sem)

    def hidden_copy(which, at):
        span = pl.ds(pl.multiple_of(at * (width // 2), LANES), width // 2)
        return pltpu.make_async_copy(
            hidden_near[which].at[:, span], hidden_far[which].at[:, span], hidden_sem.at[which, at]
        )

    def fetch_hidden(mat):
        await_core(mat)
        hidden_load(mat).start()

    def open_gate():
        hidden_load(1).wait()

        def one(at, carry):
            span = pl.ds(pl.multiple_of(at * (width // 2), LANES), width // 2)
            rows_of = product(normed_low[...], hidden_weight[:, span], 1, 0)
            gate_rows[:, span] = rows_of
            gate_low[:, span] = rows_of.astype(jnp.bfloat16)
            hidden_copy(0, at).start()
            return carry

        lax.fori_loop(0, tiles, one, 0)

    def activate():
        hidden_load(2).wait()

        def one(at, carry):
            span = pl.ds(pl.multiple_of(at * (width // 2), LANES), width // 2)
            upward = product(normed_low[...], hidden_weight[:, span], 1, 0)
            gate = gate_rows[:, span]
            upward_low[:, span] = upward.astype(jnp.bfloat16)
            active[:, span] = (gate / (1.0 + jnp.exp(-gate)) * upward).astype(jnp.bfloat16)
            hidden_copy(1, at).start()
            hidden_copy(2, at).start()
            return carry

        lax.fori_loop(0, tiles, one, 0)

    outer_copies = [
        pltpu.make_async_copy(here, far, outer_sem.at[at])
        for at, (here, far) in enumerate(zip(near[15:], results[15:]))
    ]

    def close():
        depth = plan.width // width
        loads = [
            pltpu.make_async_copy(
                full[3].at[pl.ds(at * width, width), :],
                down_near.at[pl.ds(at * width, width), :],
                down_sem.at[at],
            )
            for at in range(depth)
        ]
        for load in loads:
            load.start()
        block = min(length, 256)
        for at in range(depth):
            loads[at].wait()

            def some(number, carry, at=at):
                some_rows = pl.ds(pl.multiple_of(number * block, block), block)
                base = normed if at == 0 else outer_grad
                outer_grad[some_rows, :] = base[some_rows, :] + product(
                    active[some_rows, at * width : (at + 1) * width],
                    down_near[at * width : (at + 1) * width, :], 1, 0,
                )
                return carry

            lax.fori_loop(0, length // block, some, 0)
        gain, shift = vectors[2:3, :], vectors[3:4, :]
        step_rows = min(length, 128)

        def both(at, carry):
            gain_sum, shift_sum = carry
            some_rows = pl.ds(pl.multiple_of(at * step_rows, step_rows), step_rows)
            centred = outer_grad[some_rows, :]
            centred = centred - jnp.mean(centred, axis=1, keepdims=True)
            inverse = lax.rsqrt(jnp.mean(centred * centred, axis=1, keepdims=True) + EPSILON)
            normalized = centred * inverse
            layer_output[some_rows, :] = (normalized * gain + shift).astype(jnp.bfloat16)
            upstream = cotangent[some_rows, :].astype(jnp.float32)
            gain_sum += jnp.sum(upstream * normalized, axis=0, keepdims=True)
            shift_sum += jnp.sum(upstream, axis=0, keepdims=True)
            scaled = upstream * gain
            back = inverse * (
                scaled
                - jnp.mean(scaled, axis=1, keepdims=True)
                - normalized * jnp.mean(scaled * normalized, axis=1, keepdims=True)
            )
            outer_grad[some_rows, :] = back
            result_grad[some_rows, :] = back.astype(jnp.bfloat16)
            return gain_sum, shift_sum

        nothing = jnp.zeros((1, width), jnp.float32)
        gain_sum, shift_sum = lax.fori_loop(0, length // step_rows, both, (nothing, nothing))
        sums[...] = jnp.zeros_like(sums)
        sums[2:3, :] = gain_sum
        sums[3:4, :] = shift_sum
        sums[4:5, :] = vectors[0:1, :]
        for copy in outer_copies:
            copy.start()

    items = [(mat, number) for mat in range(4) for number in range(1, chips)]
    events = [
        (at + SLACK * step, -step, functools.partial(relay, *item, step))
        for at, item in enumerate(items)
        for step in range(plan.levels + 1)
    ]
    ready = chips - 1 + SLACK * plan.levels
    for late, work in (
        (0, fetch_weight),
        (1, project),
        (2, functools.partial(attend, 0, pairs // 2)),
        (3, functools.partial(attend, pairs // 2, pairs)),
        (4, mix),
        (4, normalize),
    ):
        events.append((ready + late, 1, work))
    ahead = chips - 1
    for due, work in (
        (ready + ahead, functools.partial(fetch_hidden, 1)),
        (max(ready + ahead, ready + 5), open_gate),
        (max(ready + 2 * ahead, ready + 5), functools.partial(fetch_hidden, 2)),
        (max(ready + 2 * ahead, ready + 5), activate),
    ):
        events.append((due, 2, work))
    for _, _, event in sorted(events, key=lambda event: event[:2]):
        event()

    await_core(3)
    close()
    for copy in sent:
        copy.wait_send()
    for mat in range(4):
        along(mat, lambda copy: copy.wait_send())
        for number in range(1, chips):
            on(mat, number, lambda copy: copy.wait_send())
    for copy in copies:
        copy.wait()
    for which in range(3):
        for at in range(tiles):
            hidden_copy(which, at).wait()
    for copy in outer_copies:
        copy.wait()


def gather_weights(plan, own, small, carried):
    hbm = pl.BlockSpec(memory_space=pl.ANY)
    vmem = pl.BlockSpec(memory_space=pltpu.VMEM)
    dma = pltpu.SemaphoreType.DMA
    pieces = [jax.ShapeDtypeStruct((own[1].shape[0], plan.width), own[1].dtype)] + [
        jax.ShapeDtypeStruct(array.shape, array.dtype) for array in own[2:]
    ]
    shapes = [
        jax.ShapeDtypeStruct((array.shape[0] * plan.shards, array.shape[1]), array.dtype)
        for array in pieces
    ]
    gaps = plan.chips - 1
    crossing = plan.replicas - 1
    length, width = carried[0].shape
    wide, low = jnp.float32, jnp.bfloat16
    results = (
        [jax.ShapeDtypeStruct((length, width), low)] * 4
        + [
            jax.ShapeDtypeStruct((width // HD, length), wide),
            jax.ShapeDtypeStruct((length, width), wide),
        ]
        + [jax.ShapeDtypeStruct((length, LANES), wide)] * 3
        + [
            jax.ShapeDtypeStruct((length, width), wide),
            jax.ShapeDtypeStruct((length, width), low),
            jax.ShapeDtypeStruct((8, width), wide),
        ]
        + [jax.ShapeDtypeStruct((length, plan.width), low)] * 3
        + [
            jax.ShapeDtypeStruct((length, width), wide),
            jax.ShapeDtypeStruct((length, width), low),
            jax.ShapeDtypeStruct((length, width), low),
            jax.ShapeDtypeStruct((8, width), wide),
        ]
    )
    return pl.pallas_call(
        functools.partial(gather_kernel, plan),
        out_shape=shapes + [jax.ShapeDtypeStruct((plan.shards,) + small.shape, small.dtype)]
        + results,
        in_specs=[hbm] * 5 + [vmem] + [hbm] * len(carried),
        out_specs=[hbm] * 4 + [vmem] + [hbm] * len(results),
        scratch_shapes=[pltpu.VMEM(array.shape, array.dtype) for array in pieces]
        + [
            dma((5,)),
            dma((4,)),
            dma((plan.shards - 1,)),
            dma((plan.shards - 1,)),
            dma((4, plan.chips, 2, plan.orders)),
            dma((4, plan.chips, plan.orders)),
            dma((4, gaps, plan.orders, crossing)),
            dma((4, gaps, plan.orders, crossing)),
            dma((4, plan.chips)),
            dma((4, plan.chips)),
        ]
        + [pltpu.VMEM(array.shape, array.dtype) for array in carried]
        + [pltpu.VMEM(result.shape, result.dtype) for result in results]
        + [
            pltpu.VMEM(shapes[0].shape, low),
            pltpu.VMEM((length, length), wide),
            dma((len(carried),)),
            dma,
            dma((12,)),
            pltpu.VMEM(shapes[1].shape, low),
            pltpu.VMEM((length, plan.width), wide),
            dma((3, 2 * plan.width // width)),
            pltpu.VMEM(shapes[3].shape, low),
            dma((plan.width // width,)),
            dma((4,)),
        ],
        compiler_params=pltpu.CompilerParams(
            collective_id=0, has_side_effects=True, vmem_limit_bytes=VMEM_LIMIT
        ),
        name="gather_weights",
    )(*own, small, *carried)


def back_pair(pair, query, key, value, upper, logsum, mask_bias, tables, joined_low, width):
    length = query.shape[0]
    block = min(length, 256)
    span = pl.ds(pl.multiple_of(pair * LANES, LANES), LANES)
    lane = lax.broadcasted_iota(jnp.int32, (1, LANES), 1)
    keys, values = key[:, span], value[:, span]
    query_parts = [0.0] * (length // block)
    key_total = value_total = 0.0
    for half in range(LANES // HD):
        pick = jnp.where(lane // HD == half, 1.0, 0.0).astype(jnp.bfloat16)
        scaled = pick * jnp.bfloat16(1.0 / math.sqrt(HD))
        keys_scaled = keys * scaled
        rowsum = logsum[pl.ds(pair * (LANES // HD) + half, 1), :]
        for at in range(length // block):
            rows = slice(at * block, (at + 1) * block)
            queries_scaled = query[rows, span] * scaled
            grads = upper[rows, span] * pick
            scores = product(keys, queries_scaled, 1, 1) + mask_bias[:, rows]
            probs = jnp.exp(scores - rowsum[:, rows])
            dprobs = product(values, grads, 1, 1)
            dots = jnp.sum(probs * dprobs, axis=0, keepdims=True)
            score_grad = (probs * (dprobs - dots)).astype(jnp.bfloat16)
            value_total += product(probs.astype(jnp.bfloat16), grads, 1, 0)
            key_total += product(score_grad, queries_scaled, 1, 0)
            query_parts[at] += product(score_grad, keys_scaled, 0, 0)
    cosine, before, after = tables

    def unrotate(grad, rows):
        return (
            grad * cosine[rows, :]
            - pltpu.roll(grad, LANES - HD // 2, 1) * before[rows, :]
            - pltpu.roll(grad, HD // 2, 1) * after[rows, :]
        ).astype(jnp.bfloat16)

    for at, part in enumerate(query_parts):
        rows = slice(at * block, (at + 1) * block)
        joined_low[rows, span] = unrotate(part, rows)
    everything = slice(0, length)
    joined_low[:, pl.ds(pl.multiple_of(width + pair * LANES, LANES), LANES)] = unrotate(
        key_total, everything
    )
    joined_low[:, pl.ds(pl.multiple_of(2 * width + pair * LANES, LANES), LANES)] = (
        value_total.astype(jnp.bfloat16)
    )


def sum_kernel(plan, *refs):
    (gate_far, up_far, active_far, gate_weight, up_weight, down_weight, attention) = refs[:7]
    carried = refs[7:23]
    outs, small_out, input_grad = refs[23:27], refs[27], refs[28]
    (pool, mate_in, rep_in, z_in, final, small_in, out_sem, small_sem, mate_send, mate_recv,
     rep_send, rep_recv, z_send, z_recv, last_send, last_recv) = refs[29:45]
    here = refs[45:61]
    (weight, gate_low, mask_bias, across, branch, upper, small, upward_low, active, fetch_sem,
     tile_sem, weight_sem, result_sem) = refs[61:]
    (query, key, value, attended, logsum, marks, segment_across, cosine, before, after, tokens,
     inner_resid, grad, result_grad, normed_low, sums) = here
    rep, shard = lax.axis_index("rep"), lax.axis_index("shard")
    chips, piece, levels = plan.chips, plan.piece, plan.levels
    place, core = lax.div(shard, 2), lax.rem(shard, 2)
    mate = place * 2 + (1 - core)
    rows = pool.shape[2]
    total = plan.replicas * plan.shards
    early = 3 * chips
    count = 4 * chips
    length, width = query.shape
    pairs = width // LANES
    groups = plan.width // width
    tile = width // 2
    low_type, wide_type = jnp.bfloat16, jnp.float32
    gaps = list(range(1, chips)) + [0]
    held = pool
    joined_low = gate_low

    def slab_at(gap, which):
        return lax.rem(place + gap, chips) * 2 + which

    def stage(turn):
        return 4 + turn % 3

    def scatter(turn, slab, span, block):
        gap = lax.rem(lax.div(slab, 2) - place + chips, chips)
        other = lax.rem(slab + core, 2)
        pool[turn + other * (stage(turn) - turn), gap, :, span] = block.astype(low_type)

    def give(turn, gap):
        remote(
            pool.at[stage(turn), gap], mate_in.at[turn, gap],
            mate_send.at[turn, gap], mate_recv.at[turn, gap], rep, mate,
        ).start()

    fetches = [
        pltpu.make_async_copy(far, near, fetch_sem.at[at])
        for at, (far, near) in enumerate(zip(carried, here))
    ]
    late = fetches[:11]
    soon = fetches[11:]
    for fetch in soon + late:
        fetch.start()

    quarter = max(chips // groups, 1)
    home = lax.rem(lax.div(place, quarter), groups)

    def tile_start(at):
        group = lax.rem(home + 1 + lax.div(at, 2), groups)
        return group * width + lax.rem(at, 2) * tile

    def slot_columns(left, slot):
        return pl.ds(pl.multiple_of(left + slot * tile, LANES), tile)

    def slot_rows(slot):
        return pl.ds(pl.multiple_of(slot * tile, LANES), tile)

    tail = pl.ds(4 * tile, width)

    def tile_copies(at):
        slot = lax.rem(at, 2)
        span = pl.ds(pl.multiple_of(tile_start(at), LANES), tile)
        pairs_of = (
            (gate_far.at[:, span], gate_low.at[:, span]),
            (up_far.at[:, span], upward_low.at[:, span]),
            (active_far.at[:, span], active.at[slot]),
            (down_weight.at[span, :], weight.at[slot_rows(slot), tail]),
        )
        return [
            pltpu.make_async_copy(far, near, tile_sem.at[number, slot])
            for number, (far, near) in enumerate(pairs_of)
        ]

    def lift_copies(at):
        slot = lax.rem(at, 2)
        span = pl.ds(pl.multiple_of(at * tile, LANES), tile)
        pairs_of = (
            (gate_weight.at[:, span], weight.at[:, slot_columns(0, slot)]),
            (up_weight.at[:, span], weight.at[:, slot_columns(2 * tile, slot)]),
        )
        return [
            pltpu.make_async_copy(far, near, tile_sem.at[4 + number, slot])
            for number, (far, near) in enumerate(pairs_of)
        ]

    for copy in tile_copies(0):
        copy.start()
    greet_all(plan, rep, shard)
    for fetch in soon:
        fetch.wait()
    across[...] = normed_low[...].T

    def small_go(step, carry):
        other = lax.rem(rep * plan.shards + shard + step, total)
        other_rep, other_shard = lax.div(other, plan.shards), lax.rem(other, plan.shards)
        remote(
            small.at[other_shard], small_in.at[step - 1], small_sem.at[0], small_sem.at[1],
            other_rep, other_shard,
        ).start()
        return carry

    def whole_mate(turn, gap):
        return remote(
            mate_in.at[turn, gap], mate_in.at[turn, gap],
            mate_send.at[turn, gap], mate_recv.at[turn, gap], rep, mate,
        )

    def cross(turn, gap, order, step):
        far = plan.flip(rep, plan.ways[order][step])
        at = plan.halve_at(step)
        copies = [
            remote(
                held.at[turn, gap, :, pl.ds(plan.column(section, order), piece)],
                rep_in.at[turn, gap, order, at + number],
                rep_send.at[turn, gap, order, at + number],
                rep_recv.at[turn, gap, order, at + number],
                far, shard,
            )
            for number, section in enumerate(plan.halve(far, order, step))
        ]
        return copies, [plan.column(section, order) for section in plan.halve(rep, order, step)]

    wide_piece = plan.orders * piece
    own_columns = pl.ds(pl.multiple_of(rep * wide_piece, LANES), wide_piece)

    def z_copy(turn, gap):
        return remote(
            held.at[turn, gap, :, own_columns],
            z_in.at[turn, gap - 1],
            z_send.at[turn, gap - 1], z_recv.at[turn, gap - 1],
            rep, slab_at(gap, core),
        )

    def item_of(number):
        return lax.div(number, chips), lax.rem(lax.rem(number, chips) + 1, chips)

    def advance(number, step):
        turn, gap = item_of(number)
        if step == 0:
            whole_mate(turn, gap).wait_recv()

            def add(at, carry):
                span = pl.ds(pl.multiple_of(at * piece, LANES), piece)
                held[turn, gap, :, span] = (
                    held[turn, gap, :, span].astype(jnp.float32)
                    + mate_in[turn, gap, :, span].astype(jnp.float32)
                ).astype(jnp.bfloat16)
                return carry

            lax.fori_loop(0, plan.width // piece, add, 0)
        else:
            for order in range(plan.orders):
                copies, columns = cross(turn, gap, order, step - 1)
                at = plan.halve_at(step - 1)
                for index, (copy, column) in enumerate(zip(copies, columns)):
                    copy.wait_recv()
                    span = pl.ds(column, piece)
                    held[turn, gap, :, span] = (
                        held[turn, gap, :, span].astype(jnp.float32)
                        + rep_in[turn, gap, order, at + index].astype(jnp.float32)
                    ).astype(jnp.bfloat16)
        if step < levels:
            for order in range(plan.orders):
                for copy in cross(turn, gap, order, step)[0]:
                    copy.start()
        else:
            @pl.when(gap > 0)
            def _():
                z_copy(turn, gap).start()

    def spread(turn, order, step):
        far = plan.flip(rep, plan.ways[order][step])
        at = plan.grow_at(step)
        return [
            remote(
                final.at[turn, :, pl.ds(plan.column(section, order), piece)],
                final.at[turn, :, pl.ds(plan.column(section, order), piece)],
                last_send.at[turn, order, at + number],
                last_recv.at[turn, order, at + number],
                far, shard,
            )
            for number, section in enumerate(plan.grow(rep, order, step))
        ]

    def await_spread(turn, order, step):
        far = plan.flip(rep, plan.ways[order][step])
        at = plan.grow_at(step)
        for number, section in enumerate(plan.grow(far, order, step)):
            there = final.at[turn, :, pl.ds(plan.column(section, order), piece)]
            remote(
                there, there,
                last_send.at[turn, order, at + number],
                last_recv.at[turn, order, at + number],
                far, shard,
            ).wait_recv()

    def finish(turn, step):
        if step == 0:
            for gap in range(1, chips):
                z_copy(turn, gap).wait_recv()
            for order in range(plan.orders):
                span = pl.ds(plan.column(rep, order), piece)
                part = pl.ds(order * piece, piece)
                amount = held[turn, 0, :, span].astype(jnp.float32)
                for gap in range(1, chips):
                    amount = amount + z_in[turn, gap - 1, :, part].astype(jnp.float32)
                final[turn, :, span] = amount.astype(jnp.bfloat16)
        else:
            for order in range(plan.orders):
                await_spread(turn, order, step - 1)
        if step < levels:
            for order in range(plan.orders):
                for copy in spread(turn, order, step):
                    copy.start()

    def tick(now):
        for step in reversed(range(levels + 1)):
            behind = now - (SLACK * (levels + step + 1) + chips - 1)

            @pl.when((behind >= 0) & (lax.rem(behind + chips, chips) == 0) & (behind < count))
            def _(behind=behind, step=step):
                finish(lax.div(behind, chips), step)

        for step in reversed(range(levels + 1)):
            number = now - SLACK * step

            @pl.when((number >= 0) & (number < count))
            def _(number=number, step=step):
                advance(number, step)

    block = min(length, 256)

    def hidden(at, carry):
        slot = lax.rem(at, 2)
        for copy in tile_copies(at):
            copy.wait()

        @pl.when(at + 1 < 2 * groups)
        def _():
            for copy in tile_copies(at + 1):
                copy.start()

        start = tile_start(at)
        span = pl.ds(pl.multiple_of(start, LANES), tile)
        down_tile = weight[slot_rows(slot), tail]

        def some(number, carry):
            some_rows = pl.ds(pl.multiple_of(number * block, block), block)
            active_grad = product(result_grad[some_rows, :], down_tile, 1, 1)
            gate = gate_low[some_rows, span].astype(wide_type)
            upward = upward_low[some_rows, span].astype(wide_type)
            sigmoid = 1.0 / (1.0 + jnp.exp(-gate))
            gate_low[some_rows, span] = (
                active_grad * upward * sigmoid * (1.0 + gate * (1.0 - sigmoid))
            ).astype(low_type)
            upward_low[some_rows, span] = (active_grad * (gate * sigmoid)).astype(low_type)
            return carry

        lax.fori_loop(0, length // block, some, 0)
        down_part = product(active[slot], result_grad[...], 0, 0)
        per = plan.width // width
        for number in range(tile // rows):
            chunk = lax.div(start, rows) + number
            left = pl.multiple_of(lax.rem(chunk, per) * width, LANES)
            scatter(
                0, lax.div(chunk, per), pl.ds(left, width),
                down_part[number * rows : (number + 1) * rows, :],
            )
        for turn, low in ((1, gate_low), (2, upward_low)):
            for some_half in range(2):
                top = some_half * (width // 2)
                part = product(across[top : top + width // 2, :], low[:, span], 1, 0)
                for number in range(width // 2 // rows):
                    scatter(
                        turn, top // rows + number, span,
                        part[number * rows : (number + 1) * rows, :],
                    )
        if chips == groups:
            @pl.when(lax.rem(at, 2) == 1)
            def _():
                number = lax.div(at, 2)
                give(0, lax.rem(number + 1, chips))

                @pl.when(number > 0)
                def _():
                    tick(number - 1)
        return carry

    lax.fori_loop(0, 2 * groups, hidden, 0)
    done = chips - 1 if chips == groups else 0
    for copy in lift_copies(0):
        copy.start()
    for gap in gaps:
        if chips != groups:
            give(0, gap)
    for turn in (1, 2):
        for gap in gaps:
            give(turn, gap)
    weight_load = pltpu.make_async_copy(attention, weight, weight_sem)
    for fetch in late:
        fetch.wait()
    mask_bias[...] = jnp.where(marks[:, 0:1] == segment_across[0:1, :], 0.0, NEG_LARGE)

    def lift(at, carry):
        slot = lax.rem(at, 2)
        for copy in lift_copies(at):
            copy.wait()

        @pl.when(at + 1 < 2 * groups)
        def _():
            for copy in lift_copies(at + 1):
                copy.start()

        span = pl.ds(pl.multiple_of(at * tile, LANES), tile)

        def some(number, carry):
            some_rows = pl.ds(pl.multiple_of(number * block, block), block)
            grad[some_rows, :] += product(
                gate_low[some_rows, span], weight[:, slot_columns(0, slot)], 1, 1
            ) + product(
                upward_low[some_rows, span], weight[:, slot_columns(2 * tile, slot)], 1, 1
            )
            return carry

        return lax.fori_loop(0, length // block, some, carry)

    def norm_back():
        gain = sums[4:5, :]
        step_rows = min(length, 128)

        def some(number, carry):
            gain_sum, shift_sum = carry
            some_rows = pl.ds(pl.multiple_of(number * step_rows, step_rows), step_rows)
            centred = inner_resid[some_rows, :]
            centred = centred - jnp.mean(centred, axis=1, keepdims=True)
            inverse = lax.rsqrt(jnp.mean(centred * centred, axis=1, keepdims=True) + EPSILON)
            normalized = centred * inverse
            upstream = grad[some_rows, :]
            gain_sum += jnp.sum(upstream * normalized, axis=0, keepdims=True)
            shift_sum += jnp.sum(upstream, axis=0, keepdims=True)
            scaled = upstream * gain
            back = inverse * (
                scaled
                - jnp.mean(scaled, axis=1, keepdims=True)
                - normalized * jnp.mean(scaled * normalized, axis=1, keepdims=True)
            )
            grad[some_rows, :] = back
            branch[some_rows, :] = back.astype(low_type)
            return gain_sum, shift_sum

        nothing = jnp.zeros((1, width), wide_type)
        gain_sum, shift_sum = lax.fori_loop(0, length // step_rows, some, (nothing, nothing))
        sums[0:1, :] = gain_sum
        sums[1:2, :] = shift_sum
        vectors = sums[...]
        for number in range(plan.shards):
            small[number] = pltpu.roll(vectors, (width - rows * number) % width, 1)[:, :LANES]

    def columns_loop(number, work):
        def one(at, carry):
            work(at)
            return carry

        lax.fori_loop(0, number, one, 0)

    def raise_up():
        weight_load.wait()

        def one(at):
            span = pl.ds(pl.multiple_of(at * 256, 256), 256)
            upper[:, span] = product(
                branch[...], weight[span, 3 * width : 4 * width], 1, 1
            ).astype(low_type)

        columns_loop(width // 256, one)

    def weigh(left, right, lefts):
        def one(at):
            span = pl.ds(pl.multiple_of(left + at * tile, LANES), tile)
            source = pl.ds(pl.multiple_of(at * tile, LANES), tile)
            for some_half in range(2):
                top = some_half * (width // 2)
                part = product(across[top : top + width // 2, :], right[:, source], 1, 0)
                for number in range(width // 2 // rows):
                    scatter(
                        3, top // rows + number, span, part[number * rows : (number + 1) * rows, :]
                    )

        columns_loop(lefts, one)

    def middle(at, carry):
        @pl.when(at < LIFTS)
        def _():
            lax.fori_loop(at * 2 * groups // LIFTS, (at + 1) * 2 * groups // LIFTS, lift, 0)

        @pl.when(at == LIFTS)
        def _():
            weight_load.start()
            norm_back()
            lax.fori_loop(1, total, small_go, 0)
            raise_up()

        @pl.when((at > LIFTS) & (at < LIFTS + 1 + pairs))
        def _():
            back_pair(
                at - LIFTS - 1, query, key, value, upper, logsum, mask_bias, (cosine, before, after),
                joined_low, width,
            )

        @pl.when(at + done < early)
        def _():
            tick(at + done)
        return carry

    lax.fori_loop(0, max(LIFTS + 1 + pairs, early - done), middle, 0)
    for gap in gaps:
        whole_mate(0, gap).wait_send()
    across[...] = attended[...].T
    weigh(3 * width, branch, width // tile)
    across[...] = tokens[...].T
    weigh(0, joined_low, 3 * width // tile)
    for gap in gaps:
        give(3, gap)

    def back(at):
        low = pl.ds(pl.multiple_of(at * 256, 256), 256)
        result_grad[:, low] = (
            grad[:, low] + product(joined_low[:, 0 : 3 * width], weight[low, 0 : 3 * width], 1, 1)
        ).astype(jnp.bfloat16)

    columns_loop(width // 256, back)
    result_copy = pltpu.make_async_copy(result_grad, input_grad, result_sem)
    result_copy.start()

    def late_tick(now, carry):
        tick(now)
        return carry

    lax.fori_loop(early, count + SLACK * (2 * levels + 1), late_tick, 0)

    everything = remote(small_in, small_in, small_sem.at[0], small_sem.at[1], rep, mate)
    everything.wait_recv()

    def gain_of(at, amount):
        return amount + small_in[at]

    small_out[...] = lax.fori_loop(0, total - 1, gain_of, small[shard])
    everything.wait_send()
    for turn in range(4):
        pltpu.make_async_copy(final.at[turn], outs[turn], out_sem.at[turn]).start()

    def drain(number, carry):
        turn, gap = item_of(number)

        @pl.when(turn > 0)
        def _():
            whole_mate(turn, gap).wait_send()
        for order in range(plan.orders):
            for step in range(levels):
                for copy in cross(turn, gap, order, step)[0]:
                    copy.wait_send()

        @pl.when(gap > 0)
        def _():
            z_copy(turn, gap).wait_send()
        return carry

    lax.fori_loop(0, count, drain, 0)
    for turn in range(4):
        for order in range(plan.orders):
            for step in range(levels):
                for copy in spread(turn, order, step):
                    copy.wait_send()
        pltpu.make_async_copy(final.at[turn], outs[turn], out_sem.at[turn]).wait()
    result_copy.wait()


def sum_grads(plan, streamed, carried):
    hbm = pl.BlockSpec(memory_space=pl.ANY)
    vmem = pl.BlockSpec(memory_space=pltpu.VMEM)
    dma = pltpu.SemaphoreType.DMA
    chips, gaps, crossing = plan.chips, plan.chips - 1, plan.replicas - 1
    length, width = carried[0].shape
    rows = width // plan.shards
    low, wide = jnp.bfloat16, jnp.float32
    total = plan.replicas * plan.shards
    return pl.pallas_call(
        functools.partial(sum_kernel, plan),
        out_shape=[jax.ShapeDtypeStruct((rows, plan.width), low)] * 4
        + [
            jax.ShapeDtypeStruct((8, LANES), wide),
            jax.ShapeDtypeStruct((length, width), low),
        ],
        in_specs=[hbm] * (len(streamed) + len(carried)),
        out_specs=[hbm] * 4 + [vmem, hbm],
        scratch_shapes=[
            pltpu.VMEM((7, chips, rows, plan.width), low),
            pltpu.VMEM((4, chips, rows, plan.width), low),
            pltpu.VMEM((4, chips, plan.orders, crossing, rows, plan.piece), low),
            pltpu.VMEM((4, gaps, rows, plan.orders * plan.piece), low),
            pltpu.VMEM((4, rows, plan.width), low),
            pltpu.VMEM((total - 1, 8, LANES), wide),
            dma((4,)),
            dma((2,)),
            dma((4, chips)),
            dma((4, chips)),
            dma((4, chips, plan.orders, crossing)),
            dma((4, chips, plan.orders, crossing)),
            dma((4, gaps)),
            dma((4, gaps)),
            dma((4, plan.orders, crossing)),
            dma((4, plan.orders, crossing)),
        ]
        + [pltpu.VMEM(array.shape, array.dtype) for array in carried]
        + [
            pltpu.VMEM((width, 4 * width), low),
            pltpu.VMEM((length, plan.width), low),
            pltpu.VMEM((length, length), wide),
            pltpu.VMEM((width, length), low),
            pltpu.VMEM((length, width), low),
            pltpu.VMEM((length, width), low),
            pltpu.VMEM((plan.shards, 8, LANES), wide),
            pltpu.VMEM((length, plan.width), low),
            pltpu.VMEM((2, length, width // 2), low),
            dma((len(carried),)),
            dma((6, 2)),
            dma,
            dma,
        ],
        compiler_params=pltpu.CompilerParams(
            collective_id=1, has_side_effects=True, vmem_limit_bytes=VMEM_MOST
        ),
        name="sum_grads",
    )(*streamed, *carried)


def on_device(
    tokens,
    joined_weight,
    mixing_weight,
    gate_weight,
    up_weight,
    down_weight,
    inner_gain,
    inner_shift,
    outer_gain,
    outer_shift,
    segments,
    positions,
    cotangent,
):
    replicas, shards = lax.axis_size("rep"), lax.axis_size("shard")
    plan = Plan(gate_weight.shape[1], replicas, shards)
    part_rows = joined_weight.shape[0]
    own_vectors = jnp.stack([inner_gain, inner_shift, outer_gain, outer_shift]).astype(jnp.float32)
    own_vectors = jnp.pad(own_vectors, ((0, 4), (0, LANES - part_rows)))
    length, model_width = tokens.shape
    halves = np.arange(LANES) % (HD // 2)
    rates = np.float32(1000.0) ** (-(2.0 * halves.astype(np.float32)) / np.float32(HD))
    marks = jnp.where(
        jnp.arange(LANES)[None, :] == 0, segments[0][:, None], positions[0][:, None]
    )
    (
        attention_full,
        gate_full,
        upward_full,
        down_full,
        _,
        query_low,
        key_low,
        value_low,
        attended_low,
        logsum,
        inner_resid,
        cosine_wide,
        before,
        after,
        _,
        normed_low,
        _,
        gate_low,
        upward_low,
        active_low,
        outer_grad,
        result_grad,
        layer_output,
        sums,
    ) = gather_weights(
        plan,
        (
            mixing_weight,
            joined_weight,
            gate_weight,
            up_weight,
            down_weight,
        ),
        own_vectors,
        (tokens, marks, segments, jnp.asarray(np.tile(rates[None, :], (8, 1))), cotangent),
    )
    down_sum, gate_sum, up_sum, attention_sum, small_sum, input_grad = sum_grads(
        plan,
        (
            gate_low,
            upward_low,
            active_low,
            gate_full,
            upward_full,
            down_full,
            attention_full,
        ),
        (
            query_low,
            key_low,
            value_low,
            attended_low,
            logsum,
            marks,
            segments,
            cosine_wide,
            before,
            after,
            tokens,
            inner_resid,
            outer_grad,
            result_grad,
            normed_low,
            sums,
        ),
    )
    down_sum = down_sum.reshape(part_rows, -1, model_width).transpose(1, 0, 2)
    full = jnp.float32
    return (
        layer_output,
        input_grad,
        attention_sum[:, : joined_weight.shape[1]].astype(full),
        attention_sum[:, joined_weight.shape[1] :].astype(full),
        gate_sum.astype(full),
        up_sum.astype(full),
        down_sum.reshape(down_weight.shape).astype(full),
        small_sum[0, :part_rows],
        small_sum[1, :part_rows],
        small_sum[2, :part_rows],
        small_sum[3, :part_rows],
    )


def solution(mesh):
    placed = (
        P(("rep", "shard"), None),
        P("shard", None),
        P("shard", None),
        P("shard", None),
        P("shard", None),
        P("shard", None),
        P("shard"),
        P("shard"),
        P("shard"),
        P("shard"),
        P(("rep", "shard"), None),
        P(("rep", "shard"), None),
        P(("rep", "shard"), None),
    )
    return jax.shard_map(
        on_device,
        mesh=mesh,
        in_specs=placed,
        out_specs=(
            P(("rep", "shard"), None),
            P(("rep", "shard"), None),
            P("shard", None),
            P("shard", None),
            P("shard", None),
            P("shard", None),
            P("shard", None),
            P("shard"),
            P("shard"),
            P("shard"),
            P("shard"),
        ),
        check_vma=False,
    )
```
